256 devices in a mesh: chan: 4 (over z_lo, core), bl: 64 (over x, y, z_hi).
Axes of the slice: x: 4, y: 4, z: 8 (z_hi: 4, z_lo: 2; z = z_hi * 2 + z_lo), core: 2. Of those that a mesh axis runs over, the one named last changes fastest.
Arguments:
- vis_value: bfloat16 [4, 64, 2, 2048], P('chan', 'bl'), may hold values from -6 to 6
- vis_weight: bfloat16 [4, 64, 2048], P('chan', 'bl'), may hold values from 0.19921875 to 5
- kernel: bfloat16 [4, 64, 64, 2048], P('chan', 'bl'), may hold values from 0.049804688 to 1
- tile_index: int32 [4, 64, 2048], P('chan', 'bl'), may hold values from 0 to 262143
- plane_index: int32 [4, 64, 2048], P('chan', 'bl'), may hold values from 0 to 7
- chan_index: int32 [4, 64, 2048], P('chan', 'bl'), may hold values from 0 to 15
- chan_offset: float32 [4, 16], P('chan'), may hold values from -0.4 to 0.4
- counts: int32 [4, 64], P('chan', 'bl'), may hold values from 256 to 2048, as said below
Outputs:
- taylor_coeffs: float32 [3, 32768], P(None, ('chan', 'bl'))
The draws below stay inside these ranges and needn't reach their ends.
Inputs may be any that keep to these rules, and one draw needn't show every extreme that they name: `counts`: each device's number of live visibility slots; slots from that number on are ignored. In every draw some device has exactly 2048.
All inputs are finite; a program needn't handle non-finite values.
Results may differ from the reference program's by a relative error of at most 0.0003.
Values may be sent and summed in bfloat16 or wider, within the bound.
A program may use at most 128 MiB of HBM per device.

```python
import math
import jax
import jax.numpy as jnp
from jax import lax

NPIX = 4096
TILE = 8
NTILE = 512
TAYLOR = 3
MOMENTS = 5
WPLANES = 8
CH_DEV = 16
STRIP = 8
SLOTS = 2048
BLK = 256
N_CHAN = 4
N_BL = 64


def draw_counts(key, part):
    raw = jax.random.randint(jax.random.fold_in(key, 11), (N_CHAN, N_BL), 0, 1000)
    spread = raw * raw // 1000 * (SLOTS - BLK) // 1000
    base_counts = (BLK + spread).reshape(-1)
    chosen = jax.random.randint(jax.random.fold_in(key, 12), (), 0, N_CHAN * N_BL)
    filled = jnp.where(jnp.arange(N_CHAN * N_BL) == chosen, SLOTS, base_counts)
    return filled.reshape(N_CHAN, N_BL).astype(jnp.int32)


def place_ends(values, key, least, high):
    dims = values.shape
    index_at = [jax.random.randint(jax.random.fold_in(key, axis), (), 0, dims[axis]) for axis in range(len(dims))]
    values = values.at[tuple(index_at)].set(least)
    longest = dims.index(max(dims))
    index_at[longest] = (index_at[longest] + 1) % dims[longest]
    return values.at[tuple(index_at)].set(high)


def block_levels(stream_key, dims, pieces, least, top_value):
    def one(axis_at, shards_of):
        draws = jax.random.uniform(jax.random.fold_in(jax.random.fold_in(stream_key, 6), axis_at), (shards_of,), jnp.float32, least / len(pieces), top_value / len(pieces))
        return jnp.repeat(jnp.exp(draws), dims[axis_at] // shards_of).reshape((-1,) + (1,) * (len(dims) - axis_at - 1))

    gain = one(*pieces[0])
    for cut in pieces[1:]:
        gain = gain * one(*cut)
    return gain


def scatter_about(stream_key, shape, width, limit, cuts=(), kind=jnp.bfloat16):
    result = jax.random.normal(stream_key, shape, jnp.float32) * width
    if len(cuts) > 0:
        result = block_levels(stream_key, shape, cuts, -0.22, 0.18) * result
    return jnp.clip(result, min=-limit, max=limit).astype(kind)


def setup_inputs(seed: int = 0) -> dict:
    arg_keys = jax.random.split(jax.random.key(seed), 9)
    vis_value = scatter_about(arg_keys[0], (N_CHAN, N_BL, 2, SLOTS), 1.0, 6.0, ((0, 4), (1, 64)))
    vis_weight = jnp.clip(jnp.exp(math.log(5.0) - 3.2227897 * jax.random.uniform(arg_keys[1], (N_CHAN, N_BL, SLOTS), jnp.float32) ** block_levels(arg_keys[1], (N_CHAN, N_BL, SLOTS), ((0, 4), (1, 64)), -0.2, 0.2)), 0.19921875, 5.0).astype(jnp.bfloat16)
    kernel = jnp.clip(0.049804688 + 0.9501953 * jax.random.uniform(arg_keys[2], (N_CHAN, N_BL, TILE * TILE, SLOTS), jnp.float32) ** block_levels(arg_keys[2], (N_CHAN, N_BL, TILE * TILE, SLOTS), ((0, 4), (1, 64)), -0.2, 0.2), 0.049804688, 1.0).astype(jnp.bfloat16)
    tile_index = place_ends(jax.random.randint(arg_keys[3], (N_CHAN, N_BL, SLOTS), 0, NTILE * NTILE), jax.random.fold_in(arg_keys[3], 1), 0, (NTILE * NTILE) - 1).astype(jnp.int32)
    plane_index = place_ends(jax.random.randint(arg_keys[4], (N_CHAN, N_BL, SLOTS), 0, WPLANES), jax.random.fold_in(arg_keys[4], 1), 0, WPLANES - 1).astype(jnp.int32)
    chan_index = place_ends(jax.random.randint(arg_keys[5], (N_CHAN, N_BL, SLOTS), 0, CH_DEV), jax.random.fold_in(arg_keys[5], 1), 0, CH_DEV - 1).astype(jnp.int32)
    chan_offset = jnp.clip(jax.random.uniform(arg_keys[6], (N_CHAN, CH_DEV), jnp.float32, -0.4, 0.4) * block_levels(arg_keys[6], (N_CHAN, CH_DEV), ((0, 4),), -0.4, 0.0), -0.4, 0.4)
    counts = draw_counts(jax.random.fold_in(arg_keys[8], 71), 0)
    return dict(vis_value=vis_value, vis_weight=vis_weight, kernel=kernel, tile_index=tile_index, plane_index=plane_index, chan_index=chan_index, chan_offset=chan_offset, counts=counts)


two_pi = 6.283185307179586
w_step = 40.0

def device_terms(values, weights, kernel, tiles, planes, chans, offsets, live_count):
    slot_count = weights.shape[0]
    ntiles = NPIX // TILE
    live_mask = jnp.arange(slot_count, dtype=jnp.int32) < live_count
    channel_ids = jnp.arange(CH_DEV, dtype=jnp.int32)
    taylor_coord = lax.optimization_barrier(jnp.sum(jnp.where(chans[:, None] == channel_ids[None, :], offsets[None, :], 0.0), axis=1))
    live_weight = jnp.where(live_mask, weights.astype(jnp.float32), 0.0)
    kernel_taps = kernel.astype(jnp.float32).reshape(TILE, TILE, slot_count)
    strip_rows = jnp.arange(STRIP, dtype=jnp.int32) - STRIP // 2
    grid_cols = (tiles // ntiles)[:, None] * TILE + jnp.arange(TILE, dtype=jnp.int32)[None, :] - NPIX // 2
    phase_index = grid_cols[:, :, None] * strip_rows[None, None, :] % NPIX
    phase_angle = phase_index.astype(jnp.float32) * (two_pi / NPIX)
    tile_real = jnp.einsum('abj,jal->jlb', kernel_taps, jnp.cos(phase_angle), precision=lax.Precision.HIGHEST)
    tile_imag = jnp.einsum('abj,jal->jlb', kernel_taps, jnp.sin(phase_angle), precision=lax.Precision.HIGHEST)
    base_real = live_weight * values[0].astype(jnp.float32)
    base_imag = live_weight * values[1].astype(jnp.float32)
    power_list = [jnp.ones_like(taylor_coord)]
    for power_id in range(MOMENTS - 1):
        power_list.append(power_list[power_id] * taylor_coord)
    power_stack = jnp.stack(power_list[:TAYLOR], axis=1)
    coeff_real = base_real[:, None] * power_stack
    coeff_imag = base_imag[:, None] * power_stack
    part_real = coeff_real[:, :, None, None] * tile_real[:, None] - coeff_imag[:, :, None, None] * tile_imag[:, None]
    part_imag = coeff_real[:, :, None, None] * tile_imag[:, None] + coeff_imag[:, :, None, None] * tile_real[:, None]
    updates = jnp.stack([part_real, part_imag], axis=-1).reshape(slot_count, TAYLOR * STRIP * TILE * 2)
    target_rows = planes * ntiles + tiles % ntiles
    tap_sums = lax.optimization_barrier(jnp.sum(kernel_taps, axis=(0, 1)))
    weighted_taps = live_weight * tap_sums
    moment_add = jnp.stack([jnp.sum(weighted_taps * power_list[moment_id]) for moment_id in range(MOMENTS)])
    return (updates, target_rows, moment_add)

def screen_angle(plane_ids, column_ids):
    cell_size = 0.5 / NPIX
    strip_rows = jnp.arange(STRIP, dtype=jnp.int32) - STRIP // 2
    xcoord = strip_rows.astype(jnp.float32) * cell_size
    ycoord = (column_ids - NPIX // 2).astype(jnp.float32) * cell_size
    radius = xcoord[:, None] * xcoord[:, None] + ycoord[None, :] * ycoord[None, :]
    lowered = -radius / (1.0 + jnp.sqrt(1.0 - radius))
    w_value = w_step * (plane_ids.astype(jnp.float32) - 0.5 * (WPLANES - 1))
    return two_pi * w_value[:, None, None] * lowered[None]

def solve_taylor(moments, images):
    entry_00, entry_01, entry_02 = (moments[0], moments[1], moments[2])
    entry_11, entry_12, entry_22 = (moments[2], moments[3], moments[4])
    minor_00 = entry_11 * entry_22 - entry_12 * entry_12
    minor_01 = entry_02 * entry_12 - entry_01 * entry_22
    minor_02 = entry_01 * entry_12 - entry_02 * entry_11
    minor_11 = entry_00 * entry_22 - entry_02 * entry_02
    minor_12 = entry_01 * entry_02 - entry_00 * entry_12
    minor_22 = entry_00 * entry_11 - entry_01 * entry_01
    determinant = entry_00 * minor_00 + entry_01 * minor_01 + entry_02 * minor_02
    first = (minor_00 * images[0] + minor_01 * images[1] + minor_02 * images[2]) / determinant
    second = (minor_01 * images[0] + minor_11 * images[1] + minor_12 * images[2]) / determinant
    third = (minor_02 * images[0] + minor_12 * images[1] + minor_22 * images[2]) / determinant
    return jnp.stack([first, second, third])

def reference(vis_value, vis_weight, kernel, tile_index, plane_index, chan_index, chan_offset, counts):
    device_total = N_CHAN * N_BL
    slot_count = vis_weight.shape[-1]
    ntiles = NPIX // TILE
    offsets_all = jnp.repeat(chan_offset, N_BL, axis=0)
    inputs = (vis_value.reshape(device_total, 2, slot_count), vis_weight.reshape(device_total, slot_count), kernel.reshape(device_total, TILE * TILE, slot_count), tile_index.reshape(device_total, slot_count), plane_index.reshape(device_total, slot_count), chan_index.reshape(device_total, slot_count), offsets_all, counts.reshape(device_total))

    def accumulate(state_pair, sliced):
        uv_grid, moments = state_pair
        updates, target_rows, moment_add = device_terms(*sliced)
        return ((uv_grid.at[target_rows].add(updates), moments + moment_add), None)
    initial = (jnp.zeros((WPLANES * ntiles, TAYLOR * STRIP * TILE * 2), jnp.float32), jnp.zeros((MOMENTS,), jnp.float32))
    (uv_grid, moments), unused = lax.scan(accumulate, initial, inputs)
    cube = uv_grid.reshape(WPLANES, ntiles, TAYLOR, STRIP, TILE, 2)
    cube = jnp.transpose(cube, (0, 2, 3, 1, 4, 5)).reshape(WPLANES, TAYLOR, STRIP, NPIX, 2)
    column_ids = jnp.arange(NPIX, dtype=jnp.int32)
    parity = 1.0 - 2.0 * (column_ids % 2).astype(jnp.float32)
    spectrum = (cube[..., 0] + 1j * cube[..., 1]) * parity
    transformed = jnp.fft.ifft(spectrum, axis=-1) * NPIX
    angles = screen_angle(jnp.arange(WPLANES, dtype=jnp.int32), column_ids)
    image = lax.optimization_barrier(jnp.sum(parity * (jnp.real(transformed) * jnp.cos(angles)[:, None] - jnp.imag(transformed) * jnp.sin(angles)[:, None]), axis=0))
    return solve_taylor(moments, image.reshape(TAYLOR, STRIP * NPIX))
```

```python
import functools
import math

import jax
import jax.numpy as jnp
import numpy as np
from jax import lax
from jax.experimental import pallas as pl
from jax.experimental.pallas import tpu as pltpu
from jax.sharding import Mesh
from jax.sharding import PartitionSpec as P

NPIX = 4096
TILE = 8
TAYLOR = 3
MOMENTS = 5
STRIP = 8
SLOTS = 2048
HALF_PLANES = 4
WIDE = TILE + 1
ROWS = TAYLOR * WIDE * 2 * STRIP
CELLS = HALF_PLANES * NPIX // TILE
BLOCKS = 32
LANES = 128
CHUNK = 256
CHAN_BL = ("chan_0", "chan_1", "bl_0", "bl_1", "bl_2")
CHAN = ("chan_0", "chan_1")
BL = ("bl_0", "bl_1", "bl_2")
f32 = jnp.float32
bf16 = jnp.bfloat16


def split_pair(table):
    high = table.astype(np.float32).astype(bf16)
    low = (table - high.astype(np.float64)).astype(np.float32).astype(bf16)
    return high, low


def tap_table():
    a = np.arange(TILE)[None, :]
    l = np.arange(STRIP)[:, None] - STRIP // 2
    angle = 2.0 * math.pi * ((a - NPIX // 2) * l % NPIX) / NPIX
    table = np.zeros((2, TILE, STRIP, TILE, TILE))
    for e in range(TILE):
        table[0, e, :, :, e] = np.cos(angle)
        table[1, e, :, :, e] = np.sin(angle)
    high, low = split_pair(table.reshape(2 * TILE * STRIP, TILE * TILE))
    ones = np.zeros((16, TILE * TILE), np.float32)
    ones[0] = 1.0
    return np.concatenate([high, low, ones.astype(bf16)], axis=0)


def line_table():
    n = np.arange(LANES)
    angle = 2.0 * math.pi * (n[:, None] * n[None, :] % LANES) / LANES
    sign = 1.0 - 2.0 * (n % 2)
    c, s = np.cos(angle) * sign, np.sin(angle) * sign
    return np.concatenate(split_pair(np.block([[c, s], [-s, c]])), axis=0)


def twist_table():
    mq = np.arange(LANES)
    rows = [2.0 * math.pi * 8 * vb * mq / NPIX for vb in range(4)]
    for e in range(TILE):
        for mr in range(4):
            rows.append(2.0 * math.pi * e * (mq + LANES * mr) / NPIX + math.pi * e)
    angle = np.stack(rows)
    return np.concatenate([np.cos(angle), np.sin(angle)], axis=0).astype(np.float32)


def screen_table():
    cell = 0.5 / NPIX
    l = np.arange(STRIP)[None, :, None] - STRIP // 2
    m = (np.arange(BLOCKS)[:, None, None] - BLOCKS // 2) * LANES + np.arange(LANES)[None, None, :]
    radius = (l * cell) ** 2 + (m * cell) ** 2
    s = -radius / (1.0 + np.sqrt(1.0 - radius))
    angle = 2.0 * math.pi * 20.0 * s
    return np.stack([np.cos(angle), np.sin(angle)]).astype(np.float32)


def unit_circle(index):
    quarter = ((index + 64) >> 7) & 3
    x = (((index + 64) & 127) - 64).astype(f32) * (2.0 * math.pi / 512.0)
    x2 = x * x
    s = x * (1.0 + x2 * (-1.0 / 6 + x2 * (1.0 / 120 + x2 * (-1.0 / 5040 + x2 * (1.0 / 362880)))))
    c = 1.0 + x2 * (-0.5 + x2 * (1.0 / 24 + x2 * (-1.0 / 720 + x2 * (1.0 / 40320))))
    odd = (quarter & 1) == 1
    cos = jnp.where(odd, s, c)
    sin = jnp.where(odd, c, s)
    cos = jnp.where((quarter == 1) | (quarter == 2), -cos, cos)
    sin = jnp.where(quarter >= 2, -sin, sin)
    return cos, sin


def cmul(a, b):
    return a[0] * b[0] - a[1] * b[1], a[0] * b[1] + a[1] * b[0]


def cadd(a, b):
    return a[0] + b[0], a[1] + b[1]


def csub(a, b):
    return a[0] - b[0], a[1] - b[1]


def turn(a):
    return -a[1], a[0]


def four_point(x):
    a, b = cadd(x[0], x[2]), csub(x[0], x[2])
    c, d = cadd(x[1], x[3]), turn(csub(x[1], x[3]))
    return [cadd(a, c), cadd(b, d), csub(a, c), csub(b, d)]


def eight_point(x):
    even, odd = four_point(x[0::2]), four_point(x[1::2])
    r = math.sqrt(0.5)
    odd = [
        odd[0],
        ((odd[1][0] - odd[1][1]) * r, (odd[1][0] + odd[1][1]) * r),
        turn(odd[2]),
        ((-odd[3][0] - odd[3][1]) * r, (odd[3][0] - odd[3][1]) * r),
    ]
    return [cadd(e, o) for e, o in zip(even, odd)] + [csub(e, o) for e, o in zip(even, odd)]


def image_kernel(
    count_ref, offset_ref, vis_ref, weight_ref, kernel_ref, tile_ref, plane_ref, chan_ref,
    tap_ref, line_ref, twist_ref, screen_ref, out_ref, taps, updates, cell_of, grid, lines, screens, image,
):
    taps[...] = jnp.dot(tap_ref[...], kernel_ref[...], preferred_element_type=f32)
    count = count_ref[0, 0]

    def one_chunk(step, sums):
        at = pl.ds(pl.multiple_of(step * CHUNK, CHUNK), CHUNK)
        slot = step * CHUNK + lax.broadcasted_iota(jnp.int32, (1, CHUNK), 1)
        weight = jnp.where(slot < count, weight_ref[:, at].astype(f32), 0.0)
        chan = chan_ref[:, at]
        coord = jnp.zeros((1, CHUNK), f32)
        for c in range(16):
            coord = jnp.where(chan == c, offset_ref[0, c], coord)
        tile = tile_ref[:, at]
        plane = plane_ref[:, at]
        direct = plane >= HALF_PLANES
        tile_v = tile & 511
        tile_v = jnp.where(direct, tile_v, 511 - tile_v)
        half = jnp.where(direct, plane - HALF_PLANES, HALF_PLANES - 1 - plane)
        cell = half * 512 + (tile_v & 3) * LANES + (tile_v >> 2)
        cell_of[at, :] = jnp.transpose(jnp.broadcast_to(cell.astype(f32), (LANES, CHUNK)))
        weighted = weight * taps[256:257, at]
        new_sums = []
        power = weighted
        for m in range(MOMENTS):
            new_sums.append(sums[m] + power)
            power = power * coord
        vis = vis_ref[:, at].astype(f32)
        base = (weight * vis[0:1], weight * vis[1:2])
        row = lax.broadcasted_iota(jnp.int32, (STRIP, CHUNK), 0) - STRIP // 2
        phase = unit_circle(((tile >> 9) * row) & 511)
        turned = cmul(phase, base)
        mirror = jnp.where(direct, 1.0, -1.0)
        flipped = (turned[0] * mirror, turned[1] * mirror)
        direct_rows = jnp.broadcast_to(direct, (STRIP, CHUNK))
        coord_rows = jnp.broadcast_to(coord, (STRIP, CHUNK))
        parts = []
        for e in range(TILE):
            r = slice(e * STRIP, (e + 1) * STRIP)
            i = slice(64 + e * STRIP, 64 + (e + 1) * STRIP)
            tap_r = taps[r, at] + taps[128 + r.start:128 + r.stop, at]
            tap_i = taps[i, at] + taps[128 + i.start:128 + i.stop, at]
            parts.append(
                (turned[0] * tap_r - turned[1] * tap_i, flipped[0] * tap_i + flipped[1] * tap_r)
            )
        zero = jnp.zeros((STRIP, CHUNK), f32)
        for e in range(WIDE):
            there = parts[e] if e < TILE else (zero, zero)
            back = parts[TILE - e] if e > 0 else (zero, zero)
            both = jnp.concatenate(
                [jnp.where(direct_rows, there[0], back[0]), jnp.where(direct_rows, there[1], back[1])], axis=0
            )
            for k in range(TAYLOR):
                if k > 0:
                    both = both * jnp.concatenate([coord_rows, coord_rows], axis=0)
                high = both.astype(bf16)
                low = (both - high.astype(f32)).astype(bf16)
                first = (k * WIDE + e) * 16
                updates[first:first + 16, at] = high
                updates[ROWS + first:ROWS + first + 16, at] = low
        return tuple(new_sums)

    sums = lax.fori_loop(
        0, SLOTS // CHUNK, one_chunk, tuple(jnp.zeros((1, CHUNK), f32) for _ in range(MOMENTS))
    )
    lane = lax.broadcasted_iota(jnp.int32, (STRIP, LANES), 1)
    moment_row = jnp.zeros((STRIP, LANES), f32)
    for m in range(MOMENTS):
        total = jnp.sum(sums[m], axis=1, keepdims=True)
        moment_row = jnp.where(lane == m, jnp.broadcast_to(total, (STRIP, LANES)), moment_row)

    def one_stretch(step, carry):
        first = step * CHUNK
        cells = cell_of[...]
        pos = lax.broadcasted_iota(jnp.int32, (1, LANES), 1) + first
        hot = jnp.concatenate(
            [
                jnp.where(cells == (pos + half * LANES).astype(f32), 1.0, 0.0).astype(bf16)
                for half in range(CHUNK // LANES)
            ],
            axis=1,
        )
        both = jnp.dot(updates[...], hot, preferred_element_type=f32)
        grid[:, pl.ds(pl.multiple_of(first, CHUNK), CHUNK)] = both[:ROWS] + both[ROWS:]
        return carry

    lax.fori_loop(0, CELLS // CHUNK, one_stretch, 0)

    for b in range(BLOCKS):
        one = (screen_ref[0, b], screen_ref[1, b])
        two = cmul(one, one)
        for q in range(HALF_PLANES):
            screens[q, 0, b] = one[0]
            screens[q, 1, b] = one[1]
            if q < HALF_PLANES - 1:
                one = cmul(one, two)

    def piece(k, e, part, q, vb):
        first = ((k * WIDE + e) * 2 + part) * STRIP
        at = pl.ds(pl.multiple_of(q * 512 + vb * LANES, LANES), LANES)
        return grid[first:first + STRIP, at]

    def one_plane(q, carry):
        for k in range(TAYLOR):
            residues = []
            for vb in range(4):
                halves = []
                for part in range(2):
                    spill = piece(k, TILE, part, q, (vb - 1) % 4)
                    if vb == 0:
                        spill = pltpu.roll(spill, 1, 1)
                    column = [piece(k, 0, part, q, vb) + spill]
                    column += [piece(k, e, part, q, vb) for e in range(1, TILE)]
                    halves.append(jnp.concatenate(column, axis=0))
                residues.append(jnp.concatenate(halves, axis=1))
            whole = jnp.concatenate(residues, axis=0)
            high = whole.astype(bf16)
            low = (whole - high.astype(f32)).astype(bf16)
            lines[...] = (
                jnp.dot(high, line_ref[0:256], preferred_element_type=f32)
                + jnp.dot(low, line_ref[0:256], preferred_element_type=f32)
                + jnp.dot(high, line_ref[256:512], preferred_element_type=f32)
            )
            quarters = [[], [], [], []]
            for e in range(TILE):
                x = []
                for vb in range(4):
                    first = (vb * TILE + e) * STRIP
                    value = (lines[first:first + STRIP, 0:LANES], lines[first:first + STRIP, LANES:2 * LANES])
                    if vb > 0:
                        value = cmul(value, (twist_ref[vb:vb + 1], twist_ref[36 + vb:37 + vb]))
                    x.append(value)
                for mr, value in enumerate(four_point(x)):
                    if e > 0:
                        t = 4 + e * 4 + mr
                        value = cmul(value, (twist_ref[t:t + 1], twist_ref[36 + t:37 + t]))
                    quarters[mr].append(value)
            for mr in range(4):
                for mh, value in enumerate(eight_point(quarters[mr])):
                    b = 4 * mh + mr
                    add = value[0] * screens[q, 0, b] - value[1] * screens[q, 1, b]
                    image[k, b] = image[k, b] + add
        return carry

    image[...] = jnp.zeros_like(image)
    lax.fori_loop(0, HALF_PLANES, one_plane, 0)
    for b in range(BLOCKS):
        for k in range(TAYLOR):
            out_ref[pl.ds(b * 4 + k, STRIP, stride=LANES), :] = image[k, b]
        out_ref[pl.ds(b * 4 + TAYLOR, STRIP, stride=LANES), :] = moment_row


def device_image(counts, offsets, vis, weight, kernel, tile, plane, chan):
    smem = pl.BlockSpec(memory_space=pltpu.SMEM)
    vmem = pl.BlockSpec(memory_space=pltpu.VMEM)
    return pl.pallas_call(
        image_kernel,
        out_shape=jax.ShapeDtypeStruct((STRIP * BLOCKS * 4, LANES), f32),
        in_specs=[smem, smem] + [vmem] * 10,
        out_specs=vmem,
        scratch_shapes=[
            pltpu.VMEM((272, SLOTS), f32),
            pltpu.VMEM((2 * ROWS, SLOTS), bf16),
            pltpu.VMEM((SLOTS, LANES), f32),
            pltpu.VMEM((ROWS, CELLS), f32),
            pltpu.VMEM((256, 256), f32),
            pltpu.VMEM((HALF_PLANES, 2, BLOCKS, STRIP, LANES), f32),
            pltpu.VMEM((TAYLOR, BLOCKS, STRIP, LANES), f32),
        ],
        compiler_params=pltpu.CompilerParams(vmem_limit_bytes=56 * 1024 * 1024),
        name="strip_image",
    )(
        counts, offsets, vis, weight, kernel, tile, plane, chan,
        jnp.asarray(tap_table()), jnp.asarray(line_table()), jnp.asarray(twist_table()), jnp.asarray(screen_table()),
    )


def solve_taylor(moments, images):
    entry_00, entry_01, entry_02 = (moments[0], moments[1], moments[2])
    entry_11, entry_12, entry_22 = (moments[2], moments[3], moments[4])
    minor_00 = entry_11 * entry_22 - entry_12 * entry_12
    minor_01 = entry_02 * entry_12 - entry_01 * entry_22
    minor_02 = entry_01 * entry_12 - entry_02 * entry_11
    minor_11 = entry_00 * entry_22 - entry_02 * entry_02
    minor_12 = entry_01 * entry_02 - entry_00 * entry_12
    minor_22 = entry_00 * entry_11 - entry_01 * entry_01
    determinant = entry_00 * minor_00 + entry_01 * minor_01 + entry_02 * minor_02
    first = (minor_00 * images[0] + minor_01 * images[1] + minor_02 * images[2]) / determinant
    second = (minor_01 * images[0] + minor_11 * images[1] + minor_12 * images[2]) / determinant
    third = (minor_02 * images[0] + minor_12 * images[1] + minor_22 * images[2]) / determinant
    return jnp.stack([first, second, third])


def body(vis_value, vis_weight, kernel, tile_index, plane_index, chan_index, chan_offset, counts):
    pieces = device_image(
        counts, chan_offset, vis_value[0, 0], vis_weight[0], kernel[0, 0],
        tile_index[0], plane_index[0], chan_index[0],
    )
    pieces = pieces.reshape(4, 64 * 4, LANES)
    pieces = lax.all_to_all(pieces, CHAN, split_axis=0, concat_axis=0, tiled=True).sum(axis=0)
    pieces = pieces.reshape(64, 4, LANES)
    pieces = lax.all_to_all(pieces, BL, split_axis=0, concat_axis=0, tiled=True).sum(axis=0)
    return solve_taylor(pieces[TAYLOR, :MOMENTS], pieces[:TAYLOR])


def solution(mesh):
    split = Mesh(mesh.devices.reshape(2, 2, 4, 4, 4), ("chan_0", "chan_1", "bl_0", "bl_1", "bl_2"))
    return jax.shard_map(
        body,
        mesh=split,
        in_specs=(
            P(CHAN, BL, None, None),
            P(CHAN, BL, None),
            P(CHAN, BL, None, None),
            P(CHAN, BL, None),
            P(CHAN, BL, None),
            P(CHAN, BL, None),
            P(CHAN, None),
            P(CHAN, BL),
        ),
        out_specs=P(None, CHAN_BL),
        check_vma=False,
    )
```

```python
import functools
import math

import jax
import jax.numpy as jnp
import numpy as np
from jax import lax
from jax.experimental import pallas as pl
from jax.experimental.pallas import tpu as pltpu
from jax.sharding import Mesh
from jax.sharding import PartitionSpec as P

NPIX = 4096
TILE = 8
TAYLOR = 3
MOMENTS = 5
STRIP = 8
SLOTS = 2048
HALF_PLANES = 4
WIDE = TILE + 1
ROWS = TAYLOR * WIDE * 2 * STRIP
CELLS = HALF_PLANES * NPIX // TILE
BLOCKS = 32
LANES = 128
CHUNK = 256
CHAN_BL = ("chan_0", "chan_1", "bl_0", "bl_1", "bl_2")
CHAN = ("chan_0", "chan_1")
BL = ("bl_0", "bl_1", "bl_2")
f32 = jnp.float32
bf16 = jnp.bfloat16


def split_pair(table):
    high = table.astype(np.float32).astype(bf16)
    low = (table - high.astype(np.float64)).astype(np.float32).astype(bf16)
    return high, low


def tap_table():
    a = np.arange(TILE)[None, :]
    l = np.arange(STRIP)[:, None] - STRIP // 2
    angle = 2.0 * math.pi * ((a - NPIX // 2) * l % NPIX) / NPIX
    table = np.zeros((2, TILE, STRIP, TILE, TILE))
    for e in range(TILE):
        table[0, e, :, :, e] = np.cos(angle)
        table[1, e, :, :, e] = np.sin(angle)
    high, low = split_pair(table.reshape(2 * TILE * STRIP, TILE * TILE))
    ones = np.zeros((16, TILE * TILE), np.float32)
    ones[0] = 1.0
    return np.concatenate([high, low, ones.astype(bf16)], axis=0)


def line_table():
    n = np.arange(LANES)
    angle = 2.0 * math.pi * (n[:, None] * n[None, :] % LANES) / LANES
    sign = 1.0 - 2.0 * (n % 2)
    c, s = np.cos(angle) * sign, np.sin(angle) * sign
    return np.concatenate(split_pair(np.block([[c, s], [-s, c]])), axis=0)


def twist_table():
    mq = np.arange(LANES)
    rows = [2.0 * math.pi * 8 * vb * mq / NPIX for vb in range(4)]
    for e in range(TILE):
        for mr in range(4):
            rows.append(2.0 * math.pi * e * (mq + LANES * mr) / NPIX + math.pi * e)
    angle = np.stack(rows)
    return np.concatenate([np.cos(angle), np.sin(angle)], axis=0).astype(np.float32)


def screen_table():
    cell = 0.5 / NPIX
    l = np.arange(STRIP)[None, :, None] - STRIP // 2
    m = (np.arange(BLOCKS)[:, None, None] - BLOCKS // 2) * LANES + np.arange(LANES)[None, None, :]
    radius = (l * cell) ** 2 + (m * cell) ** 2
    s = -radius / (1.0 + np.sqrt(1.0 - radius))
    angle = 2.0 * math.pi * 20.0 * s
    return np.stack([np.cos(angle), np.sin(angle)]).astype(np.float32)


def unit_circle(index):
    quarter = ((index + 64) >> 7) & 3
    x = (((index + 64) & 127) - 64).astype(f32) * (2.0 * math.pi / 512.0)
    x2 = x * x
    s = x * (1.0 + x2 * (-1.0 / 6 + x2 * (1.0 / 120 + x2 * (-1.0 / 5040 + x2 * (1.0 / 362880)))))
    c = 1.0 + x2 * (-0.5 + x2 * (1.0 / 24 + x2 * (-1.0 / 720 + x2 * (1.0 / 40320))))
    odd = (quarter & 1) == 1
    cos = jnp.where(odd, s, c)
    sin = jnp.where(odd, c, s)
    cos = jnp.where((quarter == 1) | (quarter == 2), -cos, cos)
    sin = jnp.where(quarter >= 2, -sin, sin)
    return cos, sin


def cmul(a, b):
    return a[0] * b[0] - a[1] * b[1], a[0] * b[1] + a[1] * b[0]


def cadd(a, b):
    return a[0] + b[0], a[1] + b[1]


def csub(a, b):
    return a[0] - b[0], a[1] - b[1]


def turn(a):
    return -a[1], a[0]


def four_point(x):
    a, b = cadd(x[0], x[2]), csub(x[0], x[2])
    c, d = cadd(x[1], x[3]), turn(csub(x[1], x[3]))
    return [cadd(a, c), cadd(b, d), csub(a, c), csub(b, d)]


def eight_point(x):
    even, odd = four_point(x[0::2]), four_point(x[1::2])
    r = math.sqrt(0.5)
    odd = [
        odd[0],
        ((odd[1][0] - odd[1][1]) * r, (odd[1][0] + odd[1][1]) * r),
        turn(odd[2]),
        ((-odd[3][0] - odd[3][1]) * r, (odd[3][0] - odd[3][1]) * r),
    ]
    return [cadd(e, o) for e, o in zip(even, odd)] + [csub(e, o) for e, o in zip(even, odd)]


def image_kernel(
    count_ref, offset_ref, vis_ref, weight_ref, kernel_ref, tile_ref, plane_ref, chan_ref,
    tap_ref, line_ref, twist_ref, screen_ref, out_ref, taps, updates, cell_of, grid, lines, screens, image,
):
    taps[...] = jnp.dot(tap_ref[...], kernel_ref[...], preferred_element_type=f32)
    count = count_ref[0, 0]

    def one_chunk(step, sums):
        at = pl.ds(pl.multiple_of(step * CHUNK, CHUNK), CHUNK)
        slot = step * CHUNK + lax.broadcasted_iota(jnp.int32, (1, CHUNK), 1)
        weight = jnp.where(slot < count, weight_ref[:, at].astype(f32), 0.0)
        chan = chan_ref[:, at]
        coord = jnp.zeros((1, CHUNK), f32)
        for c in range(16):
            coord = jnp.where(chan == c, offset_ref[0, c], coord)
        tile = tile_ref[:, at]
        plane = plane_ref[:, at]
        direct = plane >= HALF_PLANES
        tile_v = tile & 511
        tile_v = jnp.where(direct, tile_v, 511 - tile_v)
        half = jnp.where(direct, plane - HALF_PLANES, HALF_PLANES - 1 - plane)
        cell = half * 512 + (tile_v & 3) * LANES + (tile_v >> 2)
        cell_of[at, :] = jnp.transpose(jnp.broadcast_to(cell.astype(f32), (LANES, CHUNK)))
        weighted = weight * taps[256:257, at]
        new_sums = []
        power = weighted
        for m in range(MOMENTS):
            new_sums.append(sums[m] + power)
            power = power * coord
        vis = vis_ref[:, at].astype(f32)
        base = (weight * vis[0:1], weight * vis[1:2])
        row = lax.broadcasted_iota(jnp.int32, (STRIP, CHUNK), 0) - STRIP // 2
        phase = unit_circle(((tile >> 9) * row) & 511)
        turned = cmul(phase, base)
        mirror = jnp.where(direct, 1.0, -1.0)
        flipped = (turned[0] * mirror, turned[1] * mirror)
        direct_rows = jnp.broadcast_to(direct, (STRIP, CHUNK))
        coord_rows = jnp.broadcast_to(coord, (STRIP, CHUNK))
        parts = []
        for e in range(TILE):
            r = slice(e * STRIP, (e + 1) * STRIP)
            i = slice(64 + e * STRIP, 64 + (e + 1) * STRIP)
            tap_r = taps[r, at] + taps[128 + r.start:128 + r.stop, at]
            tap_i = taps[i, at] + taps[128 + i.start:128 + i.stop, at]
            parts.append(
                (turned[0] * tap_r - turned[1] * tap_i, flipped[0] * tap_i + flipped[1] * tap_r)
            )
        zero = jnp.zeros((STRIP, CHUNK), f32)
        for e in range(WIDE):
            there = parts[e] if e < TILE else (zero, zero)
            back = parts[TILE - e] if e > 0 else (zero, zero)
            both = jnp.concatenate(
                [jnp.where(direct_rows, there[0], back[0]), jnp.where(direct_rows, there[1], back[1])], axis=0
            )
            for k in range(TAYLOR):
                if k > 0:
                    both = both * jnp.concatenate([coord_rows, coord_rows], axis=0)
                high = both.astype(bf16)
                low = (both - high.astype(f32)).astype(bf16)
                first = (k * WIDE + e) * 16
                updates[first:first + 16, at] = high
                updates[ROWS + first:ROWS + first + 16, at] = low
        return tuple(new_sums)

    sums = lax.fori_loop(
        0, SLOTS // CHUNK, one_chunk, tuple(jnp.zeros((1, CHUNK), f32) for _ in range(MOMENTS))
    )
    lane = lax.broadcasted_iota(jnp.int32, (STRIP, LANES), 1)
    moment_row = jnp.zeros((STRIP, LANES), f32)
    for m in range(MOMENTS):
        total = jnp.sum(sums[m], axis=1, keepdims=True)
        moment_row = jnp.where(lane == m, jnp.broadcast_to(total, (STRIP, LANES)), moment_row)

    def one_stretch(step, carry):
        first = step * CHUNK
        cells = cell_of[...]
        pos = lax.broadcasted_iota(jnp.int32, (1, LANES), 1) + first
        hot = jnp.concatenate(
            [
                jnp.where(cells == (pos + half * LANES).astype(f32), 1.0, 0.0).astype(bf16)
                for half in range(CHUNK // LANES)
            ],
            axis=1,
        )
        both = jnp.dot(updates[...], hot, preferred_element_type=f32)
        grid[:, pl.ds(pl.multiple_of(first, CHUNK), CHUNK)] = both[:ROWS] + both[ROWS:]
        return carry

    lax.fori_loop(0, CELLS // CHUNK, one_stretch, 0)

    for b in range(BLOCKS):
        one = (screen_ref[0, b], screen_ref[1, b])
        two = cmul(one, one)
        for q in range(HALF_PLANES):
            screens[q, 0, b] = one[0]
            screens[q, 1, b] = one[1]
            if q < HALF_PLANES - 1:
                one = cmul(one, two)

    def piece(k, e, part, q, vb):
        first = ((k * WIDE + e) * 2 + part) * STRIP
        at = pl.ds(pl.multiple_of(q * 512 + vb * LANES, LANES), LANES)
        return grid[first:first + STRIP, at]

    def one_plane(q, carry):
        for k in range(TAYLOR):
            residues = []
            for vb in range(4):
                halves = []
                for part in range(2):
                    spill = piece(k, TILE, part, q, (vb - 1) % 4)
                    if vb == 0:
                        spill = pltpu.roll(spill, 1, 1)
                    column = [piece(k, 0, part, q, vb) + spill]
                    column += [piece(k, e, part, q, vb) for e in range(1, TILE)]
                    halves.append(jnp.concatenate(column, axis=0))
                residues.append(jnp.concatenate(halves, axis=1))
            whole = jnp.concatenate(residues, axis=0)
            high = whole.astype(bf16)
            low = (whole - high.astype(f32)).astype(bf16)
            lines[...] = (
                jnp.dot(high, line_ref[0:256], preferred_element_type=f32)
                + jnp.dot(low, line_ref[0:256], preferred_element_type=f32)
                + jnp.dot(high, line_ref[256:512], preferred_element_type=f32)
            )
            quarters = [[], [], [], []]
            for e in range(TILE):
                x = []
                for vb in range(4):
                    first = (vb * TILE + e) * STRIP
                    value = (lines[first:first + STRIP, 0:LANES], lines[first:first + STRIP, LANES:2 * LANES])
                    if vb > 0:
                        value = cmul(value, (twist_ref[vb:vb + 1], twist_ref[36 + vb:37 + vb]))
                    x.append(value)
                for mr, value in enumerate(four_point(x)):
                    if e > 0:
                        t = 4 + e * 4 + mr
                        value = cmul(value, (twist_ref[t:t + 1], twist_ref[36 + t:37 + t]))
                    quarters[mr].append(value)
            for mr in range(4):
                for mh, value in enumerate(eight_point(quarters[mr])):
                    b = 4 * mh + mr
                    add = value[0] * screens[q, 0, b] - value[1] * screens[q, 1, b]
                    image[k, b] = image[k, b] + add
        return carry

    image[...] = jnp.zeros_like(image)
    lax.fori_loop(0, HALF_PLANES, one_plane, 0)
    for b in range(BLOCKS):
        for k in range(TAYLOR):
            out_ref[pl.ds(b * 4 + k, STRIP, stride=LANES), :] = image[k, b]
        out_ref[pl.ds(b * 4 + TAYLOR, STRIP, stride=LANES), :] = moment_row


def device_image(counts, offsets, vis, weight, kernel, tile, plane, chan):
    smem = pl.BlockSpec(memory_space=pltpu.SMEM)
    vmem = pl.BlockSpec(memory_space=pltpu.VMEM)
    return pl.pallas_call(
        image_kernel,
        out_shape=jax.ShapeDtypeStruct((STRIP * BLOCKS * 4, LANES), f32),
        in_specs=[smem, smem] + [vmem] * 10,
        out_specs=vmem,
        scratch_shapes=[
            pltpu.VMEM((272, SLOTS), f32),
            pltpu.VMEM((2 * ROWS, SLOTS), bf16),
            pltpu.VMEM((SLOTS, LANES), f32),
            pltpu.VMEM((ROWS, CELLS), f32),
            pltpu.VMEM((256, 256), f32),
            pltpu.VMEM((HALF_PLANES, 2, BLOCKS, STRIP, LANES), f32),
            pltpu.VMEM((TAYLOR, BLOCKS, STRIP, LANES), f32),
        ],
        compiler_params=pltpu.CompilerParams(vmem_limit_bytes=56 * 1024 * 1024),
        name="strip_image",
    )(
        counts, offsets, vis, weight, kernel, tile, plane, chan,
        jnp.asarray(tap_table()), jnp.asarray(line_table()), jnp.asarray(twist_table()), jnp.asarray(screen_table()),
    )


def solve_taylor(moments, images):
    entry_00, entry_01, entry_02 = (moments[0], moments[1], moments[2])
    entry_11, entry_12, entry_22 = (moments[2], moments[3], moments[4])
    minor_00 = entry_11 * entry_22 - entry_12 * entry_12
    minor_01 = entry_02 * entry_12 - entry_01 * entry_22
    minor_02 = entry_01 * entry_12 - entry_02 * entry_11
    minor_11 = entry_00 * entry_22 - entry_02 * entry_02
    minor_12 = entry_01 * entry_02 - entry_00 * entry_12
    minor_22 = entry_00 * entry_11 - entry_01 * entry_01
    determinant = entry_00 * minor_00 + entry_01 * minor_01 + entry_02 * minor_02
    first = (minor_00 * images[0] + minor_01 * images[1] + minor_02 * images[2]) / determinant
    second = (minor_01 * images[0] + minor_11 * images[1] + minor_12 * images[2]) / determinant
    third = (minor_02 * images[0] + minor_12 * images[1] + minor_22 * images[2]) / determinant
    return first, second, third


MESH_ID = pl.DeviceIdType.MESH


def sum_kernel(
    own_ref, out_ref, pair_in, pair_sum, plane_in, plane_sum, line_in,
    pair_send, pair_recv, plane_send, plane_recv, line_send, line_recv,
):
    low = lax.axis_index("chan_0")
    core = lax.axis_index("chan_1")
    flat = lax.axis_index("bl_0") * 4 + lax.axis_index("bl_1")
    deep = lax.axis_index("bl_2") * 2 + low
    partner = {"chan_1": 1 - core}

    def plane_peer(j):
        there = (flat + j) % 16
        return there, {"bl_0": there // 4, "bl_1": there % 4}

    def line_peer(j):
        there = (deep + j) % 8
        return there, {"bl_2": there // 2, "chan_0": there % 2}

    barrier = pltpu.get_barrier_semaphore()
    pl.semaphore_signal(barrier, inc=1, device_id=partner, device_id_type=MESH_ID)
    for j in range(1, 16):
        pl.semaphore_signal(barrier, inc=1, device_id=plane_peer(j)[1], device_id_type=MESH_ID)
    for j in range(1, 8):
        pl.semaphore_signal(barrier, inc=1, device_id=line_peer(j)[1], device_id_type=MESH_ID)
    pl.semaphore_wait(barrier, 23)

    pair = pltpu.make_async_remote_copy(
        src_ref=own_ref.at[:, 1 - core], dst_ref=pair_in, send_sem=pair_send, recv_sem=pair_recv,
        device_id=partner, device_id_type=MESH_ID,
    )
    pair.start()
    pair.wait()
    for z in range(2):
        pair_sum[:, z] = own_ref[z, core] + pair_in[z]

    copies = []
    for j in range(1, 16):
        there, where = plane_peer(j)
        copies.append(
            pltpu.make_async_remote_copy(
                src_ref=pair_sum.at[there], dst_ref=plane_in.at[j], send_sem=plane_send.at[j],
                recv_sem=plane_recv.at[j], device_id=where, device_id_type=MESH_ID,
            )
        )
        copies[-1].start()
    total = pair_sum[flat]
    for j, copy in enumerate(copies):
        copy.wait()
        total = total + plane_in[j + 1]
    plane_sum[...] = total

    copies = []
    for j in range(1, 8):
        there, where = line_peer(j)
        copies.append(
            pltpu.make_async_remote_copy(
                src_ref=plane_sum.at[there % 2, there // 2], dst_ref=line_in.at[j], send_sem=line_send.at[j],
                recv_sem=line_recv.at[j], device_id=where, device_id_type=MESH_ID,
            )
        )
        copies[-1].start()
    total = plane_sum[low, deep // 2]
    for j, copy in enumerate(copies):
        copy.wait()
        total = total + line_in[j + 1]
    moments = [total[TAYLOR:TAYLOR + 1, m:m + 1] for m in range(MOMENTS)]
    images = [total[k:k + 1] for k in range(TAYLOR)]
    for k, row in enumerate(solve_taylor(moments, images)):
        out_ref[k:k + 1] = row


def summed(pieces):
    dma = pltpu.SemaphoreType.DMA
    return pl.pallas_call(
        sum_kernel,
        out_shape=jax.ShapeDtypeStruct((TAYLOR, LANES), f32),
        in_specs=[pl.BlockSpec(memory_space=pltpu.VMEM)],
        out_specs=pl.BlockSpec(memory_space=pltpu.VMEM),
        scratch_shapes=[
            pltpu.VMEM((2, 16, 4, 4, LANES), f32),
            pltpu.VMEM((16, 2, 4, 4, LANES), f32),
            pltpu.VMEM((16, 2, 4, 4, LANES), f32),
            pltpu.VMEM((2, 4, 4, LANES), f32),
            pltpu.VMEM((8, 4, LANES), f32),
            dma, dma, dma((16,)), dma((16,)), dma((8,)), dma((8,)),
        ],
        compiler_params=pltpu.CompilerParams(collective_id=0, has_side_effects=True),
        name="sum_and_solve",
    )(pieces.reshape(2, 2, 16, 4, 4, LANES))


def body(vis_value, vis_weight, kernel, tile_index, plane_index, chan_index, chan_offset, counts):
    pieces = device_image(
        counts, chan_offset, vis_value[0, 0], vis_weight[0], kernel[0, 0],
        tile_index[0], plane_index[0], chan_index[0],
    )
    return summed(pieces)


def solution(mesh):
    split = Mesh(mesh.devices.reshape(2, 2, 4, 4, 4), ("chan_0", "chan_1", "bl_0", "bl_1", "bl_2"))
    return jax.shard_map(
        body,
        mesh=split,
        in_specs=(
            P(CHAN, BL, None, None),
            P(CHAN, BL, None),
            P(CHAN, BL, None, None),
            P(CHAN, BL, None),
            P(CHAN, BL, None),
            P(CHAN, BL, None),
            P(CHAN, None),
            P(CHAN, BL),
        ),
        out_specs=P(None, CHAN_BL),
        check_vma=False,
    )
```

```python
import functools
import math

import jax
import jax.numpy as jnp
import numpy as np
from jax import lax
from jax.experimental import pallas as pl
from jax.experimental.pallas import tpu as pltpu
from jax.sharding import Mesh
from jax.sharding import PartitionSpec as P

NPIX = 4096
TILE = 8
TAYLOR = 3
MOMENTS = 5
STRIP = 8
SLOTS = 2048
HALF_PLANES = 4
WIDE = TILE + 1
ROWS = TAYLOR * WIDE * 2 * STRIP
CELLS = HALF_PLANES * NPIX // TILE
BLOCKS = 32
LANES = 128
CHUNK = 256
CHAN_BL = ("chan_0", "chan_1", "bl_0", "bl_1", "bl_2")
CHAN = ("chan_0", "chan_1")
BL = ("bl_0", "bl_1", "bl_2")
f32 = jnp.float32
bf16 = jnp.bfloat16


def split_pair(table):
    high = table.astype(np.float32).astype(bf16)
    low = (table - high.astype(np.float64)).astype(np.float32).astype(bf16)
    return high, low


def tap_table():
    a = np.arange(TILE)[None, :]
    l = np.arange(STRIP)[:, None] - STRIP // 2
    angle = 2.0 * math.pi * ((a - NPIX // 2) * l % NPIX) / NPIX
    table = np.zeros((2, TILE, STRIP, TILE, TILE))
    for e in range(TILE):
        table[0, e, :, :, e] = np.cos(angle)
        table[1, e, :, :, e] = np.sin(angle)
    high, low = split_pair(table.reshape(2 * TILE * STRIP, TILE * TILE))
    ones = np.zeros((16, TILE * TILE), np.float32)
    ones[0] = 1.0
    return np.concatenate([high, low, ones.astype(bf16)], axis=0)


def line_table():
    n = np.arange(LANES)
    angle = 2.0 * math.pi * (n[:, None] * n[None, :] % LANES) / LANES
    sign = 1.0 - 2.0 * (n % 2)
    c, s = np.cos(angle) * sign, np.sin(angle) * sign
    return np.concatenate(split_pair(np.block([[c, s], [-s, c]])), axis=0)


def twist_table():
    mq = np.arange(LANES)
    rows = [2.0 * math.pi * 8 * vb * mq / NPIX for vb in range(4)]
    for e in range(TILE):
        for mr in range(4):
            rows.append(2.0 * math.pi * e * (mq + LANES * mr) / NPIX + math.pi * e)
    angle = np.stack(rows)
    return np.concatenate([np.cos(angle), np.sin(angle)], axis=0).astype(np.float32)


def screen_table():
    cell = 0.5 / NPIX
    l = np.arange(STRIP)[None, :, None] - STRIP // 2
    m = (np.arange(BLOCKS)[:, None, None] - BLOCKS // 2) * LANES + np.arange(LANES)[None, None, :]
    radius = (l * cell) ** 2 + (m * cell) ** 2
    s = -radius / (1.0 + np.sqrt(1.0 - radius))
    angle = 2.0 * math.pi * 20.0 * s
    return np.stack([np.cos(angle), np.sin(angle)]).astype(np.float32)


def unit_circle(index):
    quarter = ((index + 64) >> 7) & 3
    x = (((index + 64) & 127) - 64).astype(f32) * (2.0 * math.pi / 512.0)
    x2 = x * x
    s = x * (1.0 + x2 * (-1.0 / 6 + x2 * (1.0 / 120 + x2 * (-1.0 / 5040 + x2 * (1.0 / 362880)))))
    c = 1.0 + x2 * (-0.5 + x2 * (1.0 / 24 + x2 * (-1.0 / 720 + x2 * (1.0 / 40320))))
    odd = (quarter & 1) == 1
    cos = jnp.where(odd, s, c)
    sin = jnp.where(odd, c, s)
    cos = jnp.where((quarter == 1) | (quarter == 2), -cos, cos)
    sin = jnp.where(quarter >= 2, -sin, sin)
    return cos, sin


def cmul(a, b):
    return a[0] * b[0] - a[1] * b[1], a[0] * b[1] + a[1] * b[0]


def cadd(a, b):
    return a[0] + b[0], a[1] + b[1]


def csub(a, b):
    return a[0] - b[0], a[1] - b[1]


def turn(a):
    return -a[1], a[0]


def four_point(x):
    a, b = cadd(x[0], x[2]), csub(x[0], x[2])
    c, d = cadd(x[1], x[3]), turn(csub(x[1], x[3]))
    return [cadd(a, c), cadd(b, d), csub(a, c), csub(b, d)]


def eight_point(x):
    even, odd = four_point(x[0::2]), four_point(x[1::2])
    r = math.sqrt(0.5)
    odd = [
        odd[0],
        ((odd[1][0] - odd[1][1]) * r, (odd[1][0] + odd[1][1]) * r),
        turn(odd[2]),
        ((-odd[3][0] - odd[3][1]) * r, (odd[3][0] - odd[3][1]) * r),
    ]
    return [cadd(e, o) for e, o in zip(even, odd)] + [csub(e, o) for e, o in zip(even, odd)]


def image_kernel(
    count_ref, offset_ref, vis_ref, weight_ref, kernel_ref, tile_ref, plane_ref, chan_ref,
    tap_ref, line_ref, twist_ref, screen_ref, out_ref, taps, updates, bank_of, lane_hot, hot, grid, lines, screens, image,
    own, pair_in, pair_sum, plane_in, plane_sum, line_in, moment_own, moment_in, moment_pair,
    pair_send, pair_recv, moment_sem, plane_send, plane_recv, line_send, line_recv,
):
    barrier = pltpu.get_barrier_semaphore()
    signal = functools.partial(pl.semaphore_signal, barrier, inc=1, device_id_type=MESH_ID)
    signal(device_id={"chan_1": 1 - lax.axis_index("chan_1")})
    flat = lax.axis_index("bl_0") * 4 + lax.axis_index("bl_1")
    for j in range(1, 16):
        there = (flat + j) % 16
        signal(device_id={"bl_0": there // 4, "bl_1": there % 4})
    deep = lax.axis_index("chan_0") * 4 + lax.axis_index("bl_2")
    for j in range(1, 8):
        there = (deep + j) % 8
        signal(device_id={"bl_2": there % 4, "chan_0": there // 4})

    taps[...] = jnp.dot(tap_ref[...], kernel_ref[...], preferred_element_type=f32)
    count = count_ref[0, 0]

    def one_chunk(step, sums):
        at = pl.ds(pl.multiple_of(step * CHUNK, CHUNK), CHUNK)
        slot = step * CHUNK + lax.broadcasted_iota(jnp.int32, (1, CHUNK), 1)
        weight = jnp.where(slot < count, weight_ref[:, at].astype(f32), 0.0)
        chan = chan_ref[:, at]
        coord = jnp.zeros((1, CHUNK), f32)
        for c in range(16):
            coord = jnp.where(chan == c, offset_ref[0, c], coord)
        tile = tile_ref[:, at]
        plane = plane_ref[:, at]
        direct = plane >= HALF_PLANES
        tile_v = tile & 511
        tile_v = jnp.where(direct, tile_v, 511 - tile_v)
        half = jnp.where(direct, plane - HALF_PLANES, HALF_PLANES - 1 - plane)
        across = lambda row: jnp.transpose(jnp.broadcast_to(row.astype(f32), (LANES, CHUNK)))
        bank_of[at, :] = across(half * 4 + (tile_v & 3)).astype(bf16)
        lane = lax.broadcasted_iota(jnp.int32, (CHUNK, LANES), 1).astype(f32)
        lane_hot[at, :] = jnp.where(across(tile_v >> 2) == lane, 1.0, 0.0).astype(bf16)
        weighted = weight * taps[256:257, at]
        new_sums = []
        power = weighted
        for m in range(MOMENTS):
            new_sums.append(sums[m] + power)
            power = power * coord
        vis = vis_ref[:, at].astype(f32)
        base = (weight * vis[0:1], weight * vis[1:2])
        row = lax.broadcasted_iota(jnp.int32, (STRIP, CHUNK), 0) - STRIP // 2
        phase = unit_circle(((tile >> 9) * row) & 511)
        turned = cmul(phase, base)
        mirror = jnp.where(direct, 1.0, -1.0)
        flipped = (turned[0] * mirror, turned[1] * mirror)
        direct_rows = jnp.broadcast_to(direct, (STRIP, CHUNK))
        coord_rows = jnp.broadcast_to(coord, (STRIP, CHUNK))
        parts = []
        for e in range(TILE):
            r = slice(e * STRIP, (e + 1) * STRIP)
            i = slice(64 + e * STRIP, 64 + (e + 1) * STRIP)
            tap_r = taps[r, at] + taps[128 + r.start:128 + r.stop, at]
            tap_i = taps[i, at] + taps[128 + i.start:128 + i.stop, at]
            parts.append(
                (turned[0] * tap_r - turned[1] * tap_i, flipped[0] * tap_i + flipped[1] * tap_r)
            )
        zero = jnp.zeros((STRIP, CHUNK), f32)
        for e in range(WIDE):
            there = parts[e] if e < TILE else (zero, zero)
            back = parts[TILE - e] if e > 0 else (zero, zero)
            both = jnp.concatenate(
                [jnp.where(direct_rows, there[0], back[0]), jnp.where(direct_rows, there[1], back[1])], axis=0
            )
            for k in range(TAYLOR):
                if k > 0:
                    both = both * jnp.concatenate([coord_rows, coord_rows], axis=0)
                high = both.astype(bf16)
                low = (both - high.astype(f32)).astype(bf16)
                first = (k * WIDE + e) * 16
                updates[first:first + 16, at] = high
                updates[ROWS + first:ROWS + first + 16, at] = low
        return tuple(new_sums)

    sums = lax.fori_loop(
        0, SLOTS // CHUNK, one_chunk, tuple(jnp.zeros((1, CHUNK), f32) for _ in range(MOMENTS))
    )
    lane = lax.broadcasted_iota(jnp.int32, (STRIP, LANES), 1)
    moment_row = jnp.zeros((STRIP, LANES), f32)
    for m in range(MOMENTS):
        total = jnp.sum(sums[m], axis=1, keepdims=True)
        moment_row = jnp.where(lane == m, jnp.broadcast_to(total, (STRIP, LANES)), moment_row)
    moment_own[...] = moment_row

    def fill(step, slot):
        banks = bank_of[...]
        for half in range(CHUNK // LANES):
            bank = (step * (CHUNK // LANES) + half).astype(f32).astype(bf16)
            hot[slot, :, half * LANES:(half + 1) * LANES] = jnp.where(banks == bank, lane_hot[...], jnp.zeros((), bf16))

    def spread(step, slot):
        both = jnp.dot(updates[...], hot[slot], preferred_element_type=f32)
        grid[:, pl.ds(pl.multiple_of(step * CHUNK, CHUNK), CHUNK)] = both[:ROWS] + both[ROWS:]

    def two_stretches(turn, carry):
        step = turn * 2
        spread(step, 0)
        fill(step + 1, 1)
        spread(step + 1, 1)
        fill(step + 2, 0)
        return carry

    fill(jnp.int32(0), 0)
    lax.fori_loop(0, CELLS // CHUNK // 2, two_stretches, 0)

    for b in range(BLOCKS):
        one = (screen_ref[0, b], screen_ref[1, b])
        two = cmul(one, one)
        for q in range(HALF_PLANES):
            screens[q, 0, b] = one[0]
            screens[q, 1, b] = one[1]
            if q < HALF_PLANES - 1:
                one = cmul(one, two)

    def piece(k, e, part, q, vb):
        first = ((k * WIDE + e) * 2 + part) * STRIP
        at = pl.ds(pl.multiple_of(q * 512 + vb * LANES, LANES), LANES)
        return grid[first:first + STRIP, at]

    def one_term(k):
        for q in range(HALF_PLANES):
            residues = []
            for vb in range(4):
                halves = []
                for part in range(2):
                    spill = piece(k, TILE, part, q, (vb - 1) % 4)
                    if vb == 0:
                        spill = pltpu.roll(spill, 1, 1)
                    column = [piece(k, 0, part, q, vb) + spill]
                    column += [piece(k, e, part, q, vb) for e in range(1, TILE)]
                    halves.append(jnp.concatenate(column, axis=0))
                residues.append(jnp.concatenate(halves, axis=1))
            whole = jnp.concatenate(residues, axis=0)
            high = whole.astype(bf16)
            low = (whole - high.astype(f32)).astype(bf16)
            lines[q] = (
                jnp.dot(high, line_ref[0:256], preferred_element_type=f32)
                + jnp.dot(low, line_ref[0:256], preferred_element_type=f32)
                + jnp.dot(high, line_ref[256:512], preferred_element_type=f32)
            )
        for q in range(HALF_PLANES):
            quarters = [[], [], [], []]
            for e in range(TILE):
                x = []
                for vb in range(4):
                    first = (vb * TILE + e) * STRIP
                    value = (lines[q, first:first + STRIP, 0:LANES], lines[q, first:first + STRIP, LANES:2 * LANES])
                    if vb > 0:
                        value = cmul(value, (twist_ref[vb:vb + 1], twist_ref[36 + vb:37 + vb]))
                    x.append(value)
                for mr, value in enumerate(four_point(x)):
                    if e > 0:
                        t = 4 + e * 4 + mr
                        value = cmul(value, (twist_ref[t:t + 1], twist_ref[36 + t:37 + t]))
                    quarters[mr].append(value)
            for mr in range(4):
                for mh, value in enumerate(eight_point(quarters[mr])):
                    b = 4 * mh + mr
                    add = value[0] * screens[q, 0, b] - value[1] * screens[q, 1, b]
                    if q < HALF_PLANES - 1:
                        image[b] = image[b] + add if q > 0 else add
                    else:
                        own[k, pl.ds(b, STRIP, stride=BLOCKS), :] = image[b] + add

    low_z = lax.axis_index("chan_0")
    core = lax.axis_index("chan_1")
    flat = lax.axis_index("bl_0") * 4 + lax.axis_index("bl_1")
    deep = low_z * 4 + lax.axis_index("bl_2")

    def pair_copies(k):
        return [
            pltpu.make_async_remote_copy(
                src_ref=own.at[k, pl.ds(pl.multiple_of(z * 128 + (1 - core) * 64, 64), 64)],
                dst_ref=pair_in.at[k, pl.ds(z * 64, 64)],
                send_sem=pair_send.at[k, z], recv_sem=pair_recv.at[k, z],
                device_id={"chan_1": 1 - core}, device_id_type=MESH_ID,
            )
            for z in range(2)
        ]

    def moment_copy():
        return pltpu.make_async_remote_copy(
            src_ref=moment_own, dst_ref=moment_in, send_sem=moment_sem.at[0], recv_sem=moment_sem.at[1],
            device_id={"chan_1": 1 - core}, device_id_type=MESH_ID,
        )

    def plane_copies(k):
        copies = []
        for j in range(1, 16):
            there = (flat + j) % 16
            copies.append(
                pltpu.make_async_remote_copy(
                    src_ref=pair_sum.at[k, there] if k < TAYLOR else moment_pair,
                    dst_ref=plane_in.at[k, j], send_sem=plane_send.at[k, j], recv_sem=plane_recv.at[k, j],
                    device_id={"bl_0": there // 4, "bl_1": there % 4}, device_id_type=MESH_ID,
                )
            )
        return copies

    def join_pair(k):
        for copy in pair_copies(k):
            copy.wait()
        sums = [
            own[k, pl.ds(pl.multiple_of(z * 128 + core * 64, 64), 64)] + pair_in[k, z * 64:z * 64 + 64] for z in range(2)
        ]
        for xy in range(16):
            pair_sum[k, xy] = jnp.concatenate([sums[z][xy * 4:xy * 4 + 4] for z in range(2)], axis=0)
        for copy in plane_copies(k):
            copy.start()

    for k in range(TAYLOR):
        one_term(k)
        if k == 0:
            pl.semaphore_wait(barrier, 23)
            moment_copy().start()
        for copy in pair_copies(k):
            copy.start()
        if k == 0:
            moment_copy().wait()
            moment_pair[...] = moment_own[...] + moment_in[...]
            for copy in plane_copies(TAYLOR):
                copy.start()
        else:
            join_pair(k - 1)
    join_pair(TAYLOR - 1)

    for k in (TAYLOR, 0, 1, 2):
        total = pair_sum[k, flat] if k < TAYLOR else moment_pair[...]
        for j, copy in enumerate(plane_copies(k)):
            copy.wait()
            total = total + plane_in[k, j + 1]
        for r in range(8):
            plane_sum[r, k:k + 1] = total[r:r + 1]

    copies = []
    for j in range(1, 8):
        there = (deep + j) % 8
        copies.append(
            pltpu.make_async_remote_copy(
                src_ref=plane_sum.at[there], dst_ref=line_in.at[j], send_sem=line_send.at[j],
                recv_sem=line_recv.at[j], device_id={"bl_2": there % 4, "chan_0": there // 4}, device_id_type=MESH_ID,
            )
        )
        copies[-1].start()
    total = plane_sum[deep]
    for j, copy in enumerate(copies):
        copy.wait()
        total = total + line_in[j + 1]
    moments = [total[TAYLOR:TAYLOR + 1, m:m + 1] for m in range(MOMENTS)]
    images = [total[k:k + 1] for k in range(TAYLOR)]
    for k, row in enumerate(solve_taylor(moments, images)):
        out_ref[k:k + 1] = row


def device_image(counts, offsets, vis, weight, kernel, tile, plane, chan):
    smem = pl.BlockSpec(memory_space=pltpu.SMEM)
    vmem = pl.BlockSpec(memory_space=pltpu.VMEM)
    dma = pltpu.SemaphoreType.DMA
    return pl.pallas_call(
        image_kernel,
        out_shape=jax.ShapeDtypeStruct((TAYLOR, LANES), f32),
        in_specs=[smem, smem] + [vmem] * 10,
        out_specs=vmem,
        scratch_shapes=[
            pltpu.VMEM((272, SLOTS), f32),
            pltpu.VMEM((2 * ROWS, SLOTS), bf16),
            pltpu.VMEM((SLOTS, LANES), bf16),
            pltpu.VMEM((SLOTS, LANES), bf16),
            pltpu.VMEM((2, SLOTS, CHUNK), bf16),
            pltpu.VMEM((ROWS, CELLS), f32),
            pltpu.VMEM((HALF_PLANES, 256, 256), f32),
            pltpu.VMEM((HALF_PLANES, 2, BLOCKS, STRIP, LANES), f32),
            pltpu.VMEM((BLOCKS, STRIP, LANES), f32),
            pltpu.VMEM((TAYLOR, 256, LANES), f32),
            pltpu.VMEM((TAYLOR, 128, LANES), f32),
            pltpu.VMEM((TAYLOR, 16, 8, LANES), f32),
            pltpu.VMEM((TAYLOR + 1, 16, 8, LANES), f32),
            pltpu.VMEM((8, 4, LANES), f32),
            pltpu.VMEM((8, 4, LANES), f32),
            pltpu.VMEM((8, LANES), f32),
            pltpu.VMEM((8, LANES), f32),
            pltpu.VMEM((8, LANES), f32),
            dma((TAYLOR, 2)), dma((TAYLOR, 2)), dma((2,)), dma((4, 16)), dma((4, 16)), dma((8,)), dma((8,)),
        ],
        compiler_params=pltpu.CompilerParams(
            vmem_limit_bytes=56 * 1024 * 1024, collective_id=0, has_side_effects=True
        ),
        name="strip_image",
    )(
        counts, offsets, vis, weight, kernel, tile, plane, chan,
        jnp.asarray(tap_table()), jnp.asarray(line_table()), jnp.asarray(twist_table()), jnp.asarray(screen_table()),
    )


def solve_taylor(moments, images):
    entry_00, entry_01, entry_02 = (moments[0], moments[1], moments[2])
    entry_11, entry_12, entry_22 = (moments[2], moments[3], moments[4])
    minor_00 = entry_11 * entry_22 - entry_12 * entry_12
    minor_01 = entry_02 * entry_12 - entry_01 * entry_22
    minor_02 = entry_01 * entry_12 - entry_02 * entry_11
    minor_11 = entry_00 * entry_22 - entry_02 * entry_02
    minor_12 = entry_01 * entry_02 - entry_00 * entry_12
    minor_22 = entry_00 * entry_11 - entry_01 * entry_01
    determinant = entry_00 * minor_00 + entry_01 * minor_01 + entry_02 * minor_02
    first = (minor_00 * images[0] + minor_01 * images[1] + minor_02 * images[2]) / determinant
    second = (minor_01 * images[0] + minor_11 * images[1] + minor_12 * images[2]) / determinant
    third = (minor_02 * images[0] + minor_12 * images[1] + minor_22 * images[2]) / determinant
    return first, second, third


MESH_ID = pl.DeviceIdType.MESH


def body(vis_value, vis_weight, kernel, tile_index, plane_index, chan_index, chan_offset, counts):
    return device_image(
        counts, chan_offset, vis_value[0, 0], vis_weight[0], kernel[0, 0],
        tile_index[0], plane_index[0], chan_index[0],
    )


def solution(mesh):
    split = Mesh(mesh.devices.reshape(2, 2, 4, 4, 4), ("chan_0", "chan_1", "bl_0", "bl_1", "bl_2"))
    return jax.shard_map(
        body,
        mesh=split,
        in_specs=(
            P(CHAN, BL, None, None),
            P(CHAN, BL, None),
            P(CHAN, BL, None, None),
            P(CHAN, BL, None),
            P(CHAN, BL, None),
            P(CHAN, BL, None),
            P(CHAN, None),
            P(CHAN, BL),
        ),
        out_specs=P(None, CHAN_BL),
        check_vma=False,
    )
```

```python
import functools
import math

import jax
import jax.numpy as jnp
import numpy as np
from jax import lax
from jax.experimental import pallas as pl
from jax.experimental.pallas import tpu as pltpu
from jax.sharding import Mesh
from jax.sharding import PartitionSpec as P

NPIX = 4096
TILE = 8
TAYLOR = 3
MOMENTS = 5
STRIP = 8
SLOTS = 2048
HALF_PLANES = 4
WIDE = TILE + 1
ROWS = TAYLOR * WIDE * 2 * STRIP
CELLS = HALF_PLANES * NPIX // TILE
BLOCKS = 32
LANES = 128
CHUNK = 256
CHAN_BL = ("chan_0", "chan_1", "bl_0", "bl_1", "bl_2")
CHAN = ("chan_0", "chan_1")
BL = ("bl_0", "bl_1", "bl_2")
f32 = jnp.float32
bf16 = jnp.bfloat16


def split_pair(table):
    high = table.astype(np.float32).astype(bf16)
    low = (table - high.astype(np.float64)).astype(np.float32).astype(bf16)
    return high, low


def tap_table():
    a = np.arange(TILE)[None, :]
    l = np.arange(STRIP)[:, None] - STRIP // 2
    angle = 2.0 * math.pi * ((a - NPIX // 2) * l % NPIX) / NPIX
    table = np.zeros((2, TILE, STRIP, TILE, TILE))
    for e in range(TILE):
        table[0, e, :, :, e] = np.cos(angle)
        table[1, e, :, :, e] = np.sin(angle)
    high, low = split_pair(table.reshape(2 * TILE * STRIP, TILE * TILE))
    ones = np.zeros((16, TILE * TILE), np.float32)
    ones[0] = 1.0
    return np.concatenate([high, low, ones.astype(bf16)], axis=0)


def line_table():
    n = np.arange(LANES)
    angle = 2.0 * math.pi * (n[:, None] * n[None, :] % LANES) / LANES
    sign = 1.0 - 2.0 * (n % 2)
    c, s = np.cos(angle) * sign, np.sin(angle) * sign
    return np.concatenate(split_pair(np.block([[c, s], [-s, c]])), axis=0)


def twist_table():
    mq = np.arange(LANES)
    rows = [2.0 * math.pi * 8 * vb * mq / NPIX for vb in range(4)]
    for e in range(TILE):
        for mr in range(4):
            rows.append(2.0 * math.pi * e * (mq + LANES * mr) / NPIX + math.pi * e)
    angle = np.stack(rows)
    return np.concatenate([np.cos(angle), np.sin(angle)], axis=0).astype(np.float32)


def screen_table():
    cell = 0.5 / NPIX
    l = np.arange(STRIP)[None, :, None] - STRIP // 2
    m = (np.arange(BLOCKS)[:, None, None] - BLOCKS // 2) * LANES + np.arange(LANES)[None, None, :]
    radius = (l * cell) ** 2 + (m * cell) ** 2
    s = -radius / (1.0 + np.sqrt(1.0 - radius))
    angle = 2.0 * math.pi * 20.0 * s
    return np.stack([np.cos(angle), np.sin(angle)]).astype(np.float32)


def unit_circle(index):
    quarter = ((index + 64) >> 7) & 3
    x = (((index + 64) & 127) - 64).astype(f32) * (2.0 * math.pi / 512.0)
    x2 = x * x
    s = x * (1.0 + x2 * (-1.0 / 6 + x2 * (1.0 / 120 + x2 * (-1.0 / 5040 + x2 * (1.0 / 362880)))))
    c = 1.0 + x2 * (-0.5 + x2 * (1.0 / 24 + x2 * (-1.0 / 720 + x2 * (1.0 / 40320))))
    odd = (quarter & 1) == 1
    cos = jnp.where(odd, s, c)
    sin = jnp.where(odd, c, s)
    cos = jnp.where((quarter == 1) | (quarter == 2), -cos, cos)
    sin = jnp.where(quarter >= 2, -sin, sin)
    return cos, sin


def cmul(a, b):
    return a[0] * b[0] - a[1] * b[1], a[0] * b[1] + a[1] * b[0]


def cadd(a, b):
    return a[0] + b[0], a[1] + b[1]


def csub(a, b):
    return a[0] - b[0], a[1] - b[1]


def turn(a):
    return -a[1], a[0]


def four_point(x):
    a, b = cadd(x[0], x[2]), csub(x[0], x[2])
    c, d = cadd(x[1], x[3]), turn(csub(x[1], x[3]))
    return [cadd(a, c), cadd(b, d), csub(a, c), csub(b, d)]


def eight_point(x):
    even, odd = four_point(x[0::2]), four_point(x[1::2])
    r = math.sqrt(0.5)
    odd = [
        odd[0],
        ((odd[1][0] - odd[1][1]) * r, (odd[1][0] + odd[1][1]) * r),
        turn(odd[2]),
        ((-odd[3][0] - odd[3][1]) * r, (odd[3][0] - odd[3][1]) * r),
    ]
    return [cadd(e, o) for e, o in zip(even, odd)] + [csub(e, o) for e, o in zip(even, odd)]


def image_kernel(
    count_ref, offset_ref, vis_ref, weight_ref, kernel_ref, tile_ref, plane_ref, chan_ref,
    tap_ref, line_ref, twist_ref, screen_ref, out_ref, taps, updates, bank_of, lane_hot, grid, lines, screens, image,
    own, pair_in, pair_sum, plane_in, plane_sum, line_in, moment_own, moment_in, moment_pair,
    pair_send, pair_recv, moment_sem, plane_send, plane_recv, line_send, line_recv,
):
    barrier = pltpu.get_barrier_semaphore()
    signal = functools.partial(pl.semaphore_signal, barrier, inc=1, device_id_type=MESH_ID)
    signal(device_id={"chan_1": 1 - lax.axis_index("chan_1")})
    flat = lax.axis_index("bl_0") * 4 + lax.axis_index("bl_1")
    for j in range(1, 16):
        there = (flat + j) % 16
        signal(device_id={"bl_0": there // 4, "bl_1": there % 4})
    deep = lax.axis_index("chan_0") * 4 + lax.axis_index("bl_2")
    for j in range(1, 8):
        there = (deep + j) % 8
        signal(device_id={"bl_2": there % 4, "chan_0": there // 4})

    taps[...] = jnp.dot(tap_ref[...], kernel_ref[...], preferred_element_type=f32)
    count = jnp.broadcast_to(count_ref[0:1, 0:1], (1, CHUNK))
    offsets = [jnp.broadcast_to(offset_ref[0:1, c:c + 1], (1, CHUNK)) for c in range(16)]

    def one_chunk(step, sums):
        at = pl.ds(pl.multiple_of(step * CHUNK, CHUNK), CHUNK)
        slot = step * CHUNK + lax.broadcasted_iota(jnp.int32, (1, CHUNK), 1)
        weight = jnp.where(slot < count, weight_ref[:, at].astype(f32), 0.0)
        chan = chan_ref[:, at]
        coord = jnp.zeros((1, CHUNK), f32)
        for c in range(16):
            coord = jnp.where(chan == c, offsets[c], coord)
        tile = tile_ref[:, at]
        plane = plane_ref[:, at]
        direct = plane >= HALF_PLANES
        tile_v = tile & 511
        tile_v = jnp.where(direct, tile_v, 511 - tile_v)
        half = jnp.where(direct, plane - HALF_PLANES, HALF_PLANES - 1 - plane)
        across = lambda row: jnp.transpose(jnp.broadcast_to(row.astype(f32), (LANES, CHUNK)))
        bank_of[at, :] = across(half * 4 + (tile_v & 3)).astype(bf16)
        lane = lax.broadcasted_iota(jnp.int32, (CHUNK, LANES), 1).astype(f32)
        lane_hot[at, :] = jnp.where(across(tile_v >> 2) == lane, 1.0, 0.0).astype(bf16)
        weighted = weight * taps[256:257, at]
        new_sums = []
        power = weighted
        for m in range(MOMENTS):
            new_sums.append(sums[m] + power)
            power = power * coord
        vis = vis_ref[:, at].astype(f32)
        base = (weight * vis[0:1], weight * vis[1:2])
        row = lax.broadcasted_iota(jnp.int32, (STRIP, CHUNK), 0) - STRIP // 2
        phase = unit_circle(((tile >> 9) * row) & 511)
        turned = cmul(phase, base)
        mirror = jnp.where(direct, 1.0, -1.0)
        flipped = (turned[0] * mirror, turned[1] * mirror)
        direct_rows = jnp.broadcast_to(direct, (STRIP, CHUNK))
        coord_rows = jnp.broadcast_to(coord, (STRIP, CHUNK))
        parts = []
        for e in range(TILE):
            r = slice(e * STRIP, (e + 1) * STRIP)
            i = slice(64 + e * STRIP, 64 + (e + 1) * STRIP)
            tap_r = taps[r, at] + taps[128 + r.start:128 + r.stop, at]
            tap_i = taps[i, at] + taps[128 + i.start:128 + i.stop, at]
            parts.append(
                (turned[0] * tap_r - turned[1] * tap_i, flipped[0] * tap_i + flipped[1] * tap_r)
            )
        zero = jnp.zeros((STRIP, CHUNK), f32)
        for e in range(WIDE):
            there = parts[e] if e < TILE else (zero, zero)
            back = parts[TILE - e] if e > 0 else (zero, zero)
            both = jnp.concatenate(
                [jnp.where(direct_rows, there[0], back[0]), jnp.where(direct_rows, there[1], back[1])], axis=0
            )
            for k in range(TAYLOR):
                if k > 0:
                    both = both * jnp.concatenate([coord_rows, coord_rows], axis=0)
                high = both.astype(bf16)
                low = (both - high.astype(f32)).astype(bf16)
                first = (k * WIDE + e) * 16
                updates[first:first + 16, at] = high
                updates[ROWS + first:ROWS + first + 16, at] = low
        return tuple(new_sums)

    sums = lax.fori_loop(
        0, SLOTS // CHUNK, one_chunk, tuple(jnp.zeros((1, CHUNK), f32) for _ in range(MOMENTS))
    )
    lane = lax.broadcasted_iota(jnp.int32, (STRIP, LANES), 1)
    moment_row = jnp.zeros((STRIP, LANES), f32)
    for m in range(MOMENTS):
        total = jnp.sum(sums[m], axis=1, keepdims=True)
        moment_row = jnp.where(lane == m, jnp.broadcast_to(total, (STRIP, LANES)), moment_row)
    moment_own[...] = moment_row

    for step in range(CELLS // CHUNK):
        banks = bank_of[...]
        halves = [
            jnp.where(banks == jnp.asarray(step * 2 + half, bf16), lane_hot[...], jnp.zeros((), bf16))
            for half in range(CHUNK // LANES)
        ]
        both = jnp.dot(updates[...], jnp.concatenate(halves, axis=1), preferred_element_type=f32)
        grid[:, step * CHUNK:(step + 1) * CHUNK] = both[:ROWS] + both[ROWS:]

    for b in range(BLOCKS):
        one = (screen_ref[0, b], screen_ref[1, b])
        two = cmul(one, one)
        for q in range(HALF_PLANES):
            screens[q, 0, b] = one[0]
            screens[q, 1, b] = one[1]
            if q < HALF_PLANES - 1:
                one = cmul(one, two)

    def piece(k, e, part, q, vb):
        first = ((k * WIDE + e) * 2 + part) * STRIP
        at = pl.ds(pl.multiple_of(q * 512 + vb * LANES, LANES), LANES)
        return grid[first:first + STRIP, at]

    def one_term(k):
        for q in range(HALF_PLANES):
            residues = []
            for vb in range(4):
                halves = []
                for part in range(2):
                    spill = piece(k, TILE, part, q, (vb - 1) % 4)
                    if vb == 0:
                        spill = pltpu.roll(spill, 1, 1)
                    column = [piece(k, 0, part, q, vb) + spill]
                    column += [piece(k, e, part, q, vb) for e in range(1, TILE)]
                    halves.append(jnp.concatenate(column, axis=0))
                residues.append(jnp.concatenate(halves, axis=1))
            whole = jnp.concatenate(residues, axis=0)
            high = whole.astype(bf16)
            low = (whole - high.astype(f32)).astype(bf16)
            lines[q] = (
                jnp.dot(high, line_ref[0:256], preferred_element_type=f32)
                + jnp.dot(low, line_ref[0:256], preferred_element_type=f32)
                + jnp.dot(high, line_ref[256:512], preferred_element_type=f32)
            )
        for q in range(HALF_PLANES):
            quarters = [[], [], [], []]
            for e in range(TILE):
                x = []
                for vb in range(4):
                    first = (vb * TILE + e) * STRIP
                    value = (lines[q, first:first + STRIP, 0:LANES], lines[q, first:first + STRIP, LANES:2 * LANES])
                    if vb > 0:
                        value = cmul(value, (twist_ref[vb:vb + 1], twist_ref[36 + vb:37 + vb]))
                    x.append(value)
                for mr, value in enumerate(four_point(x)):
                    if e > 0:
                        t = 4 + e * 4 + mr
                        value = cmul(value, (twist_ref[t:t + 1], twist_ref[36 + t:37 + t]))
                    quarters[mr].append(value)
            for mr in range(4):
                for mh, value in enumerate(eight_point(quarters[mr])):
                    b = 4 * mh + mr
                    add = value[0] * screens[q, 0, b] - value[1] * screens[q, 1, b]
                    if q < HALF_PLANES - 1:
                        image[b] = image[b] + add if q > 0 else add
                    else:
                        own[k, pl.ds(b, STRIP, stride=BLOCKS), :] = image[b] + add

    low_z = lax.axis_index("chan_0")
    core = lax.axis_index("chan_1")
    flat = lax.axis_index("bl_0") * 4 + lax.axis_index("bl_1")
    deep = low_z * 4 + lax.axis_index("bl_2")

    def together(source, target, send, recv):
        return pltpu.make_async_remote_copy(
            src_ref=source, dst_ref=target, send_sem=send, recv_sem=recv,
            device_id={"chan_1": 1 - core}, device_id_type=MESH_ID,
        )

    def pair_copies(k):
        return [
            pltpu.make_async_remote_copy(
                src_ref=own.at[k, pl.ds(pl.multiple_of(z * 128 + (1 - core) * 64, 64), 64)],
                dst_ref=pair_in.at[k, pl.ds(z * 64, 64)],
                send_sem=pair_send.at[k], recv_sem=pair_recv.at[k],
                device_id={"chan_1": 1 - core}, device_id_type=MESH_ID,
            )
            for z in range(2)
        ]

    def moment_copy():
        return pltpu.make_async_remote_copy(
            src_ref=moment_own, dst_ref=moment_in, send_sem=moment_sem.at[0], recv_sem=moment_sem.at[1],
            device_id={"chan_1": 1 - core}, device_id_type=MESH_ID,
        )

    def plane_copies(k):
        copies = []
        for j in range(1, 16):
            there = (flat + j) % 16
            copies.append(
                pltpu.make_async_remote_copy(
                    src_ref=pair_sum.at[k, there] if k < TAYLOR else moment_pair,
                    dst_ref=plane_in.at[k, j], send_sem=plane_send.at[k], recv_sem=plane_recv.at[k],
                    device_id={"bl_0": there // 4, "bl_1": there % 4}, device_id_type=MESH_ID,
                )
            )
        return copies

    def join_pair(k):
        together(own.at[k, 0:128], pair_in.at[k], pair_send.at[k], pair_recv.at[k]).wait()
        sums = [
            own[k, pl.ds(pl.multiple_of(z * 128 + core * 64, 64), 64)] + pair_in[k, z * 64:z * 64 + 64] for z in range(2)
        ]
        for xy in range(16):
            pair_sum[k, xy] = jnp.concatenate([sums[z][xy * 4:xy * 4 + 4] for z in range(2)], axis=0)
        for copy in plane_copies(k):
            copy.start()

    for k in range(TAYLOR):
        one_term(k)
        if k == 0:
            pl.semaphore_wait(barrier, 23)
            moment_copy().start()
        for copy in pair_copies(k):
            copy.start()
        if k == 0:
            moment_copy().wait()
            moment_pair[...] = moment_own[...] + moment_in[...]
            for copy in plane_copies(TAYLOR):
                copy.start()
        else:
            join_pair(k - 1)
    join_pair(TAYLOR - 1)

    for k in (TAYLOR, 0, 1, 2):
        total = pair_sum[k, flat] if k < TAYLOR else moment_pair[...]
        together(pair_sum.at[0, 0:15], plane_in.at[k, 1:16], plane_send.at[k], plane_recv.at[k]).wait()
        for j in range(1, 16):
            total = total + plane_in[k, j]
        for r in range(8):
            plane_sum[r, k:k + 1] = total[r:r + 1]

    for j in range(1, 8):
        there = (deep + j) % 8
        pltpu.make_async_remote_copy(
            src_ref=plane_sum.at[there], dst_ref=line_in.at[j], send_sem=line_send, recv_sem=line_recv,
            device_id={"bl_2": there % 4, "chan_0": there // 4}, device_id_type=MESH_ID,
        ).start()
    total = plane_sum[deep]
    together(plane_sum.at[0:7], line_in.at[1:8], line_send, line_recv).wait()
    for j in range(1, 8):
        total = total + line_in[j]
    moments = [total[TAYLOR:TAYLOR + 1, m:m + 1] for m in range(MOMENTS)]
    images = [total[k:k + 1] for k in range(TAYLOR)]
    rows, determinant = solve_taylor(moments, images)
    for k in range(TAYLOR):
        out_ref[0, k:k + 1] = rows[k]
        out_ref[1, k:k + 1] = jnp.broadcast_to(determinant, (1, LANES))


def device_image(counts, offsets, vis, weight, kernel, tile, plane, chan):
    vmem = pl.BlockSpec(memory_space=pltpu.VMEM)
    dma = pltpu.SemaphoreType.DMA
    return pl.pallas_call(
        image_kernel,
        out_shape=jax.ShapeDtypeStruct((2, TAYLOR, LANES), f32),
        in_specs=[vmem] * 12,
        out_specs=vmem,
        scratch_shapes=[
            pltpu.VMEM((272, SLOTS), f32),
            pltpu.VMEM((2 * ROWS, SLOTS), bf16),
            pltpu.VMEM((SLOTS, LANES), bf16),
            pltpu.VMEM((SLOTS, LANES), bf16),
            pltpu.VMEM((ROWS, CELLS), f32),
            pltpu.VMEM((HALF_PLANES, 256, 256), f32),
            pltpu.VMEM((HALF_PLANES, 2, BLOCKS, STRIP, LANES), f32),
            pltpu.VMEM((BLOCKS, STRIP, LANES), f32),
            pltpu.VMEM((TAYLOR, 256, LANES), f32),
            pltpu.VMEM((TAYLOR, 128, LANES), f32),
            pltpu.VMEM((TAYLOR, 16, 8, LANES), f32),
            pltpu.VMEM((TAYLOR + 1, 16, 8, LANES), f32),
            pltpu.VMEM((8, 4, LANES), f32),
            pltpu.VMEM((8, 4, LANES), f32),
            pltpu.VMEM((8, LANES), f32),
            pltpu.VMEM((8, LANES), f32),
            pltpu.VMEM((8, LANES), f32),
            dma((3,)), dma((3,)), dma((2,)), dma((4,)), dma((4,)), dma, dma,
        ],
        compiler_params=pltpu.CompilerParams(
            vmem_limit_bytes=40 * 1024 * 1024, collective_id=0, has_side_effects=True
        ),
        name="strip_image",
    )(
        counts, offsets, vis, weight, kernel, tile, plane, chan,
        jnp.asarray(tap_table()), jnp.asarray(line_table()), jnp.asarray(twist_table()), jnp.asarray(screen_table()),
    )


def solve_taylor(moments, images):
    entry_00, entry_01, entry_02 = (moments[0], moments[1], moments[2])
    entry_11, entry_12, entry_22 = (moments[2], moments[3], moments[4])
    minor_00 = entry_11 * entry_22 - entry_12 * entry_12
    minor_01 = entry_02 * entry_12 - entry_01 * entry_22
    minor_02 = entry_01 * entry_12 - entry_02 * entry_11
    minor_11 = entry_00 * entry_22 - entry_02 * entry_02
    minor_12 = entry_01 * entry_02 - entry_00 * entry_12
    minor_22 = entry_00 * entry_11 - entry_01 * entry_01
    determinant = entry_00 * minor_00 + entry_01 * minor_01 + entry_02 * minor_02
    first = minor_00 * images[0] + minor_01 * images[1] + minor_02 * images[2]
    second = minor_01 * images[0] + minor_11 * images[1] + minor_12 * images[2]
    third = minor_02 * images[0] + minor_12 * images[1] + minor_22 * images[2]
    return (first, second, third), determinant


MESH_ID = pl.DeviceIdType.MESH


def body(vis_value, vis_weight, kernel, tile_index, plane_index, chan_index, chan_offset, counts):
    scaled = device_image(
        counts, chan_offset, vis_value[0, 0], vis_weight[0], kernel[0, 0],
        tile_index[0], plane_index[0], chan_index[0],
    )
    return scaled[0] / scaled[1]


def solution(mesh):
    split = Mesh(mesh.devices.reshape(2, 2, 4, 4, 4), ("chan_0", "chan_1", "bl_0", "bl_1", "bl_2"))
    return jax.shard_map(
        body,
        mesh=split,
        in_specs=(
            P(CHAN, BL, None, None),
            P(CHAN, BL, None),
            P(CHAN, BL, None, None),
            P(CHAN, BL, None),
            P(CHAN, BL, None),
            P(CHAN, BL, None),
            P(CHAN, None),
            P(CHAN, BL),
        ),
        out_specs=P(None, CHAN_BL),
        check_vma=False,
    )
```

```python
import functools
import math

import jax
import jax.numpy as jnp
import numpy as np
from jax import lax
from jax.experimental import pallas as pl
from jax.experimental.pallas import tpu as pltpu
from jax.sharding import Mesh
from jax.sharding import PartitionSpec as P

NPIX = 4096
TILE = 8
TAYLOR = 3
MOMENTS = 5
STRIP = 8
SLOTS = 2048
HALF_PLANES = 4
WIDE = TILE + 1
ROWS = TAYLOR * WIDE * 2 * STRIP
CELLS = HALF_PLANES * NPIX // TILE
BLOCKS = 32
LANES = 128
CHUNK = 256
CHAN_BL = ("chan_0", "chan_1", "bl_0", "bl_1", "bl_2")
CHAN = ("chan_0", "chan_1")
BL = ("bl_0", "bl_1", "bl_2")
f32 = jnp.float32
bf16 = jnp.bfloat16


def split_pair(table):
    high = table.astype(np.float32).astype(bf16)
    low = (table - high.astype(np.float64)).astype(np.float32).astype(bf16)
    return high, low


def tap_table():
    a = np.arange(TILE)[None, :]
    l = np.arange(STRIP)[:, None] - STRIP // 2
    angle = 2.0 * math.pi * ((a - NPIX // 2) * l % NPIX) / NPIX
    table = np.zeros((2, TILE, STRIP, TILE, TILE))
    for e in range(TILE):
        table[0, e, :, :, e] = np.cos(angle)
        table[1, e, :, :, e] = np.sin(angle)
    high, low = split_pair(table.reshape(2 * TILE * STRIP, TILE * TILE))
    ones = np.zeros((16, TILE * TILE), np.float32)
    ones[0] = 1.0
    return np.concatenate([high, low, ones.astype(bf16)], axis=0)


def line_table():
    n = np.arange(LANES)
    angle = 2.0 * math.pi * (n[:, None] * n[None, :] % LANES) / LANES
    sign = 1.0 - 2.0 * (n % 2)
    c, s = np.cos(angle) * sign, np.sin(angle) * sign
    return np.concatenate(split_pair(np.block([[c, s], [-s, c]])), axis=0)


def twist_table():
    mq = np.arange(LANES)
    rows = [2.0 * math.pi * 8 * vb * mq / NPIX for vb in range(4)]
    for e in range(TILE):
        for mr in range(4):
            rows.append(2.0 * math.pi * e * (mq + LANES * mr) / NPIX + math.pi * e)
    angle = np.stack(rows)
    return np.concatenate([np.cos(angle), np.sin(angle)], axis=0).astype(np.float32)


def screen_table():
    cell = 0.5 / NPIX
    l = np.arange(STRIP)[None, :, None] - STRIP // 2
    m = (np.arange(BLOCKS)[:, None, None] - BLOCKS // 2) * LANES + np.arange(LANES)[None, None, :]
    radius = (l * cell) ** 2 + (m * cell) ** 2
    s = -radius / (1.0 + np.sqrt(1.0 - radius))
    angle = 2.0 * math.pi * 20.0 * s
    return np.stack([np.cos(angle), np.sin(angle)]).astype(np.float32)


def unit_circle(index):
    quarter = ((index + 64) >> 7) & 3
    x = (((index + 64) & 127) - 64).astype(f32) * (2.0 * math.pi / 512.0)
    x2 = x * x
    s = x * (1.0 + x2 * (-1.0 / 6 + x2 * (1.0 / 120 + x2 * (-1.0 / 5040 + x2 * (1.0 / 362880)))))
    c = 1.0 + x2 * (-0.5 + x2 * (1.0 / 24 + x2 * (-1.0 / 720 + x2 * (1.0 / 40320))))
    odd = (quarter & 1) == 1
    cos = jnp.where(odd, s, c)
    sin = jnp.where(odd, c, s)
    cos = jnp.where((quarter == 1) | (quarter == 2), -cos, cos)
    sin = jnp.where(quarter >= 2, -sin, sin)
    return cos, sin


def cmul(a, b):
    return a[0] * b[0] - a[1] * b[1], a[0] * b[1] + a[1] * b[0]


def cadd(a, b):
    return a[0] + b[0], a[1] + b[1]


def csub(a, b):
    return a[0] - b[0], a[1] - b[1]


def turn(a):
    return -a[1], a[0]


def four_point(x):
    a, b = cadd(x[0], x[2]), csub(x[0], x[2])
    c, d = cadd(x[1], x[3]), turn(csub(x[1], x[3]))
    return [cadd(a, c), cadd(b, d), csub(a, c), csub(b, d)]


def eight_point(x):
    even, odd = four_point(x[0::2]), four_point(x[1::2])
    r = math.sqrt(0.5)
    odd = [
        odd[0],
        ((odd[1][0] - odd[1][1]) * r, (odd[1][0] + odd[1][1]) * r),
        turn(odd[2]),
        ((-odd[3][0] - odd[3][1]) * r, (odd[3][0] - odd[3][1]) * r),
    ]
    return [cadd(e, o) for e, o in zip(even, odd)] + [csub(e, o) for e, o in zip(even, odd)]


def image_kernel(*refs):
    (
        count_ref, offset_ref, vis_ref, weight_ref, kernel_ref, tile_ref, plane_ref, chan_ref,
        tap_ref, line_ref, twist_ref, screen_ref,
    ) = refs[13:25]
    fetches = [pltpu.make_async_copy(refs[i], refs[13 + i], refs[-1].at[i]) for i in range(12)]
    for i in FETCH_ORDER:
        fetches[i].start()
    out_ref = refs[12]
    image_body(
        fetches, count_ref, offset_ref, vis_ref, weight_ref, kernel_ref, tile_ref, plane_ref, chan_ref,
        tap_ref, line_ref, twist_ref, screen_ref, out_ref, *refs[25:-1]
    )


FETCH_ORDER = (8, 4, 0, 1, 2, 3, 5, 6, 7, 9, 10, 11)


def image_body(
    fetches, count_ref, offset_ref, vis_ref, weight_ref, kernel_ref, tile_ref, plane_ref, chan_ref,
    tap_ref, line_ref, twist_ref, screen_ref, out_ref, taps, updates, bank_of, lane_hot, grid, lines, screens, image,
    own, pair_in, pair_sum, plane_in, plane_sum, line_in, moment_own, moment_in, moment_pair,
    pair_send, pair_recv, moment_sem, plane_send, plane_recv, line_send, line_recv,
):
    barrier = pltpu.get_barrier_semaphore()
    signal = functools.partial(pl.semaphore_signal, barrier, inc=1, device_id_type=MESH_ID)
    signal(device_id={"chan_1": 1 - lax.axis_index("chan_1")})
    flat = lax.axis_index("bl_0") * 4 + lax.axis_index("bl_1")
    for j in range(1, 16):
        there = (flat + j) % 16
        signal(device_id={"bl_0": there // 4, "bl_1": there % 4})
    deep = lax.axis_index("chan_0") * 4 + lax.axis_index("bl_2")
    for j in range(1, 8):
        there = (deep + j) % 8
        signal(device_id={"bl_2": there % 4, "chan_0": there // 4})

    for i in (8, 4):
        fetches[i].wait()
    taps[...] = jnp.dot(tap_ref[...], kernel_ref[...], preferred_element_type=f32)
    for i in (0, 1, 2, 3, 5, 6, 7):
        fetches[i].wait()
    count = jnp.broadcast_to(count_ref[0:1, 0:1], (1, CHUNK))
    offsets = [jnp.broadcast_to(offset_ref[0:1, c:c + 1], (1, CHUNK)) for c in range(16)]

    def one_chunk(step, sums):
        at = pl.ds(pl.multiple_of(step * CHUNK, CHUNK), CHUNK)
        slot = step * CHUNK + lax.broadcasted_iota(jnp.int32, (1, CHUNK), 1)
        weight = jnp.where(slot < count, weight_ref[:, at].astype(f32), 0.0)
        chan = chan_ref[:, at]
        coord = jnp.zeros((1, CHUNK), f32)
        for c in range(16):
            coord = jnp.where(chan == c, offsets[c], coord)
        tile = tile_ref[:, at]
        plane = plane_ref[:, at]
        direct = plane >= HALF_PLANES
        tile_v = tile & 511
        tile_v = jnp.where(direct, tile_v, 511 - tile_v)
        half = jnp.where(direct, plane - HALF_PLANES, HALF_PLANES - 1 - plane)
        across = lambda row: jnp.transpose(jnp.broadcast_to(row.astype(f32), (LANES, CHUNK)))
        bank_of[at, :] = across(half * 4 + (tile_v & 3)).astype(bf16)
        lane = lax.broadcasted_iota(jnp.int32, (CHUNK, LANES), 1).astype(f32)
        lane_hot[at, :] = jnp.where(across(tile_v >> 2) == lane, 1.0, 0.0).astype(bf16)
        weighted = weight * taps[256:257, at]
        new_sums = []
        power = weighted
        for m in range(MOMENTS):
            new_sums.append(sums[m] + power)
            power = power * coord
        vis = vis_ref[:, at].astype(f32)
        base = (weight * vis[0:1], weight * vis[1:2])
        row = lax.broadcasted_iota(jnp.int32, (STRIP, CHUNK), 0) - STRIP // 2
        phase = unit_circle(((tile >> 9) * row) & 511)
        turned = cmul(phase, base)
        mirror = jnp.where(direct, 1.0, -1.0)
        flipped = (turned[0] * mirror, turned[1] * mirror)
        direct_rows = jnp.broadcast_to(direct, (STRIP, CHUNK))
        coord_rows = jnp.broadcast_to(coord, (STRIP, CHUNK))
        parts = []
        for e in range(TILE):
            r = slice(e * STRIP, (e + 1) * STRIP)
            i = slice(64 + e * STRIP, 64 + (e + 1) * STRIP)
            tap_r = taps[r, at] + taps[128 + r.start:128 + r.stop, at]
            tap_i = taps[i, at] + taps[128 + i.start:128 + i.stop, at]
            parts.append(
                (turned[0] * tap_r - turned[1] * tap_i, flipped[0] * tap_i + flipped[1] * tap_r)
            )
        zero = jnp.zeros((STRIP, CHUNK), f32)
        for e in range(WIDE):
            there = parts[e] if e < TILE else (zero, zero)
            back = parts[TILE - e] if e > 0 else (zero, zero)
            both = jnp.concatenate(
                [jnp.where(direct_rows, there[0], back[0]), jnp.where(direct_rows, there[1], back[1])], axis=0
            )
            for k in range(TAYLOR):
                if k > 0:
                    both = both * jnp.concatenate([coord_rows, coord_rows], axis=0)
                high = both.astype(bf16)
                low = (both - high.astype(f32)).astype(bf16)
                first = (k * WIDE + e) * 16
                updates[first:first + 16, at] = high
                updates[ROWS + first:ROWS + first + 16, at] = low
        return tuple(new_sums)

    sums = lax.fori_loop(
        0, SLOTS // CHUNK, one_chunk, tuple(jnp.zeros((1, CHUNK), f32) for _ in range(MOMENTS))
    )
    lane = lax.broadcasted_iota(jnp.int32, (STRIP, LANES), 1)
    moment_row = jnp.zeros((STRIP, LANES), f32)
    for m in range(MOMENTS):
        total = jnp.sum(sums[m], axis=1, keepdims=True)
        moment_row = jnp.where(lane == m, jnp.broadcast_to(total, (STRIP, LANES)), moment_row)
    moment_own[...] = moment_row

    for i in (9, 10, 11):
        fetches[i].wait()
    for step in range(CELLS // CHUNK):
        banks = bank_of[...]
        halves = [
            jnp.where(banks == jnp.asarray(step * 2 + half, bf16), lane_hot[...], jnp.zeros((), bf16))
            for half in range(CHUNK // LANES)
        ]
        both = jnp.dot(updates[...], jnp.concatenate(halves, axis=1), preferred_element_type=f32)
        grid[:, step * CHUNK:(step + 1) * CHUNK] = both[:ROWS] + both[ROWS:]

    for b in range(BLOCKS):
        one = (screen_ref[0, b], screen_ref[1, b])
        two = cmul(one, one)
        for q in range(HALF_PLANES):
            screens[q, 0, b] = one[0]
            screens[q, 1, b] = one[1]
            if q < HALF_PLANES - 1:
                one = cmul(one, two)

    def piece(k, e, part, q, vb):
        first = ((k * WIDE + e) * 2 + part) * STRIP
        at = pl.ds(pl.multiple_of(q * 512 + vb * LANES, LANES), LANES)
        return grid[first:first + STRIP, at]

    def one_term(k):
        for q in range(HALF_PLANES):
            residues = []
            for vb in range(4):
                halves = []
                for part in range(2):
                    spill = piece(k, TILE, part, q, (vb - 1) % 4)
                    if vb == 0:
                        spill = pltpu.roll(spill, 1, 1)
                    column = [piece(k, 0, part, q, vb) + spill]
                    column += [piece(k, e, part, q, vb) for e in range(1, TILE)]
                    halves.append(jnp.concatenate(column, axis=0))
                residues.append(jnp.concatenate(halves, axis=1))
            whole = jnp.concatenate(residues, axis=0)
            high = whole.astype(bf16)
            low = (whole - high.astype(f32)).astype(bf16)
            lines[q] = (
                jnp.dot(high, line_ref[0:256], preferred_element_type=f32)
                + jnp.dot(low, line_ref[0:256], preferred_element_type=f32)
                + jnp.dot(high, line_ref[256:512], preferred_element_type=f32)
            )
        for q in range(HALF_PLANES):
            quarters = [[], [], [], []]
            for e in range(TILE):
                x = []
                for vb in range(4):
                    first = (vb * TILE + e) * STRIP
                    value = (lines[q, first:first + STRIP, 0:LANES], lines[q, first:first + STRIP, LANES:2 * LANES])
                    if vb > 0:
                        value = cmul(value, (twist_ref[vb:vb + 1], twist_ref[36 + vb:37 + vb]))
                    x.append(value)
                for mr, value in enumerate(four_point(x)):
                    if e > 0:
                        t = 4 + e * 4 + mr
                        value = cmul(value, (twist_ref[t:t + 1], twist_ref[36 + t:37 + t]))
                    quarters[mr].append(value)
            for mr in range(4):
                for mh, value in enumerate(eight_point(quarters[mr])):
                    b = 4 * mh + mr
                    add = value[0] * screens[q, 0, b] - value[1] * screens[q, 1, b]
                    if q < HALF_PLANES - 1:
                        image[b] = image[b] + add if q > 0 else add
                    else:
                        own[k, pl.ds(b, STRIP, stride=BLOCKS), :] = image[b] + add

    low_z = lax.axis_index("chan_0")
    core = lax.axis_index("chan_1")
    flat = lax.axis_index("bl_0") * 4 + lax.axis_index("bl_1")
    deep = low_z * 4 + lax.axis_index("bl_2")

    def together(source, target, send, recv):
        return pltpu.make_async_remote_copy(
            src_ref=source, dst_ref=target, send_sem=send, recv_sem=recv,
            device_id={"chan_1": 1 - core}, device_id_type=MESH_ID,
        )

    def pair_copies(k):
        return [
            pltpu.make_async_remote_copy(
                src_ref=own.at[k, pl.ds(pl.multiple_of(z * 128 + (1 - core) * 64, 64), 64)],
                dst_ref=pair_in.at[k, pl.ds(z * 64, 64)],
                send_sem=pair_send.at[k], recv_sem=pair_recv.at[k],
                device_id={"chan_1": 1 - core}, device_id_type=MESH_ID,
            )
            for z in range(2)
        ]

    def moment_copy():
        return pltpu.make_async_remote_copy(
            src_ref=moment_own, dst_ref=moment_in, send_sem=moment_sem.at[0], recv_sem=moment_sem.at[1],
            device_id={"chan_1": 1 - core}, device_id_type=MESH_ID,
        )

    def plane_copies(k):
        copies = []
        for j in range(1, 16):
            there = (flat + j) % 16
            copies.append(
                pltpu.make_async_remote_copy(
                    src_ref=pair_sum.at[k, there] if k < TAYLOR else moment_pair,
                    dst_ref=plane_in.at[k, j], send_sem=plane_send.at[k], recv_sem=plane_recv.at[k],
                    device_id={"bl_0": there // 4, "bl_1": there % 4}, device_id_type=MESH_ID,
                )
            )
        return copies

    def join_pair(k):
        together(own.at[k, 0:128], pair_in.at[k], pair_send.at[k], pair_recv.at[k]).wait()
        sums = [
            own[k, pl.ds(pl.multiple_of(z * 128 + core * 64, 64), 64)] + pair_in[k, z * 64:z * 64 + 64] for z in range(2)
        ]
        for xy in range(16):
            pair_sum[k, xy] = jnp.concatenate([sums[z][xy * 4:xy * 4 + 4] for z in range(2)], axis=0)
        for copy in plane_copies(k):
            copy.start()

    for k in range(TAYLOR):
        one_term(k)
        if k == 0:
            pl.semaphore_wait(barrier, 23)
            moment_copy().start()
        for copy in pair_copies(k):
            copy.start()
        if k == 0:
            moment_copy().wait()
            moment_pair[...] = moment_own[...] + moment_in[...]
            for copy in plane_copies(TAYLOR):
                copy.start()
        else:
            join_pair(k - 1)
    join_pair(TAYLOR - 1)

    for k in (TAYLOR, 0, 1, 2):
        total = pair_sum[k, flat] if k < TAYLOR else moment_pair[...]
        together(pair_sum.at[0, 0:15], plane_in.at[k, 1:16], plane_send.at[k], plane_recv.at[k]).wait()
        for j in range(1, 16):
            total = total + plane_in[k, j]
        for r in range(8):
            plane_sum[r, k:k + 1] = total[r:r + 1]

    for j in range(1, 8):
        there = (deep + j) % 8
        pltpu.make_async_remote_copy(
            src_ref=plane_sum.at[there], dst_ref=line_in.at[j], send_sem=line_send, recv_sem=line_recv,
            device_id={"bl_2": there % 4, "chan_0": there // 4}, device_id_type=MESH_ID,
        ).start()
    total = plane_sum[deep]
    together(plane_sum.at[0:7], line_in.at[1:8], line_send, line_recv).wait()
    for j in range(1, 8):
        total = total + line_in[j]
    moments = [total[TAYLOR:TAYLOR + 1, m:m + 1] for m in range(MOMENTS)]
    images = [total[k:k + 1] for k in range(TAYLOR)]
    rows, determinant = solve_taylor(moments, images)
    for k in range(TAYLOR):
        out_ref[0, k:k + 1] = rows[k]
        out_ref[1, k:k + 1] = jnp.broadcast_to(determinant, (1, LANES))


def device_image(counts, offsets, vis, weight, kernel, tile, plane, chan):
    vmem = pl.BlockSpec(memory_space=pltpu.VMEM)
    dma = pltpu.SemaphoreType.DMA
    operands = (
        counts, offsets, vis, weight, kernel, tile, plane, chan,
        jnp.asarray(tap_table()), jnp.asarray(line_table()), jnp.asarray(twist_table()), jnp.asarray(screen_table()),
    )
    return pl.pallas_call(
        image_kernel,
        out_shape=jax.ShapeDtypeStruct((2, TAYLOR, LANES), f32),
        in_specs=[pl.BlockSpec(memory_space=pltpu.HBM)] * 12,
        out_specs=vmem,
        scratch_shapes=[pltpu.VMEM(a.shape, a.dtype) for a in operands] + [
            pltpu.VMEM((272, SLOTS), f32),
            pltpu.VMEM((2 * ROWS, SLOTS), bf16),
            pltpu.VMEM((SLOTS, LANES), bf16),
            pltpu.VMEM((SLOTS, LANES), bf16),
            pltpu.VMEM((ROWS, CELLS), f32),
            pltpu.VMEM((HALF_PLANES, 256, 256), f32),
            pltpu.VMEM((HALF_PLANES, 2, BLOCKS, STRIP, LANES), f32),
            pltpu.VMEM((BLOCKS, STRIP, LANES), f32),
            pltpu.VMEM((TAYLOR, 256, LANES), f32),
            pltpu.VMEM((TAYLOR, 128, LANES), f32),
            pltpu.VMEM((TAYLOR, 16, 8, LANES), f32),
            pltpu.VMEM((TAYLOR + 1, 16, 8, LANES), f32),
            pltpu.VMEM((8, 4, LANES), f32),
            pltpu.VMEM((8, 4, LANES), f32),
            pltpu.VMEM((8, LANES), f32),
            pltpu.VMEM((8, LANES), f32),
            pltpu.VMEM((8, LANES), f32),
            dma((3,)), dma((3,)), dma((2,)), dma((4,)), dma((4,)), dma, dma, dma((12,)),
        ],
        compiler_params=pltpu.CompilerParams(
            vmem_limit_bytes=56 * 1024 * 1024, collective_id=0, has_side_effects=True
        ),
        name="strip_image",
    )(*operands)


def solve_taylor(moments, images):
    entry_00, entry_01, entry_02 = (moments[0], moments[1], moments[2])
    entry_11, entry_12, entry_22 = (moments[2], moments[3], moments[4])
    minor_00 = entry_11 * entry_22 - entry_12 * entry_12
    minor_01 = entry_02 * entry_12 - entry_01 * entry_22
    minor_02 = entry_01 * entry_12 - entry_02 * entry_11
    minor_11 = entry_00 * entry_22 - entry_02 * entry_02
    minor_12 = entry_01 * entry_02 - entry_00 * entry_12
    minor_22 = entry_00 * entry_11 - entry_01 * entry_01
    determinant = entry_00 * minor_00 + entry_01 * minor_01 + entry_02 * minor_02
    first = minor_00 * images[0] + minor_01 * images[1] + minor_02 * images[2]
    second = minor_01 * images[0] + minor_11 * images[1] + minor_12 * images[2]
    third = minor_02 * images[0] + minor_12 * images[1] + minor_22 * images[2]
    return (first, second, third), determinant


MESH_ID = pl.DeviceIdType.MESH


def body(vis_value, vis_weight, kernel, tile_index, plane_index, chan_index, chan_offset, counts):
    scaled = device_image(
        counts, chan_offset, vis_value[0, 0], vis_weight[0], kernel[0, 0],
        tile_index[0], plane_index[0], chan_index[0],
    )
    return scaled[0] / scaled[1]


def solution(mesh):
    split = Mesh(mesh.devices.reshape(2, 2, 4, 4, 4), ("chan_0", "chan_1", "bl_0", "bl_1", "bl_2"))
    return jax.shard_map(
        body,
        mesh=split,
        in_specs=(
            P(CHAN, BL, None, None),
            P(CHAN, BL, None),
            P(CHAN, BL, None, None),
            P(CHAN, BL, None),
            P(CHAN, BL, None),
            P(CHAN, BL, None),
            P(CHAN, None),
            P(CHAN, BL),
        ),
        out_specs=P(None, CHAN_BL),
        check_vma=False,
    )
```

```python
import functools
import math

import jax
import jax.numpy as jnp
import numpy as np
from jax import lax
from jax.experimental import pallas as pl
from jax.experimental.pallas import tpu as pltpu
from jax.sharding import Mesh
from jax.sharding import PartitionSpec as P

NPIX = 4096
TILE = 8
TAYLOR = 3
MOMENTS = 5
STRIP = 8
SLOTS = 2048
HALF_PLANES = 4
WIDE = TILE + 1
ROWS = TAYLOR * WIDE * 2 * STRIP
SPAN = WIDE * 2 * STRIP
CELLS = HALF_PLANES * NPIX // TILE
BLOCKS = 32
LANES = 128
CHUNK = 256
CHAN_BL = ("chan_0", "chan_1", "bl_0", "bl_1", "bl_2")
CHAN = ("chan_0", "chan_1")
BL = ("bl_0", "bl_1", "bl_2")
f32 = jnp.float32
bf16 = jnp.bfloat16


def split_pair(table):
    high = table.astype(np.float32).astype(bf16)
    low = (table - high.astype(np.float64)).astype(np.float32).astype(bf16)
    return high, low


def tap_table():
    a = np.arange(TILE)[None, :]
    l = np.arange(STRIP)[:, None] - STRIP // 2
    angle = 2.0 * math.pi * ((a - NPIX // 2) * l % NPIX) / NPIX
    table = np.zeros((2, TILE, STRIP, TILE, TILE))
    for e in range(TILE):
        table[0, e, :, :, e] = np.cos(angle)
        table[1, e, :, :, e] = np.sin(angle)
    high, low = split_pair(table.reshape(2 * TILE * STRIP, TILE * TILE))
    ones = np.zeros((16, TILE * TILE), np.float32)
    ones[0] = 1.0
    return np.concatenate([high, low, ones.astype(bf16)], axis=0)


def line_table():
    n = np.arange(LANES)
    angle = 2.0 * math.pi * (n[:, None] * n[None, :] % LANES) / LANES
    sign = 1.0 - 2.0 * (n % 2)
    c, s = np.cos(angle) * sign, np.sin(angle) * sign
    return np.concatenate(split_pair(np.block([[c, s], [-s, c]])), axis=0)


def twist_table():
    mq = np.arange(LANES)
    rows = [2.0 * math.pi * 8 * vb * mq / NPIX for vb in range(4)]
    for e in range(TILE):
        for mr in range(4):
            rows.append(2.0 * math.pi * e * (mq + LANES * mr) / NPIX + math.pi * e)
    angle = np.stack(rows)
    return np.concatenate([np.cos(angle), np.sin(angle)], axis=0).astype(np.float32)


def screen_table():
    cell = 0.5 / NPIX
    l = np.arange(STRIP)[None, :, None] - STRIP // 2
    m = (np.arange(BLOCKS)[:, None, None] - BLOCKS // 2) * LANES + np.arange(LANES)[None, None, :]
    radius = (l * cell) ** 2 + (m * cell) ** 2
    s = -radius / (1.0 + np.sqrt(1.0 - radius))
    angle = 2.0 * math.pi * 20.0 * s
    return np.stack([np.cos(angle), np.sin(angle)]).astype(np.float32)


def unit_circle(index):
    quarter = ((index + 64) >> 7) & 3
    x = (((index + 64) & 127) - 64).astype(f32) * (2.0 * math.pi / 512.0)
    x2 = x * x
    s = x * (1.0 + x2 * (-1.0 / 6 + x2 * (1.0 / 120 + x2 * (-1.0 / 5040 + x2 * (1.0 / 362880)))))
    c = 1.0 + x2 * (-0.5 + x2 * (1.0 / 24 + x2 * (-1.0 / 720 + x2 * (1.0 / 40320))))
    odd = (quarter & 1) == 1
    cos = jnp.where(odd, s, c)
    sin = jnp.where(odd, c, s)
    cos = jnp.where((quarter == 1) | (quarter == 2), -cos, cos)
    sin = jnp.where(quarter >= 2, -sin, sin)
    return cos, sin


def cmul(a, b):
    return a[0] * b[0] - a[1] * b[1], a[0] * b[1] + a[1] * b[0]


def cadd(a, b):
    return a[0] + b[0], a[1] + b[1]


def csub(a, b):
    return a[0] - b[0], a[1] - b[1]


def turn(a):
    return -a[1], a[0]


def four_point(x):
    a, b = cadd(x[0], x[2]), csub(x[0], x[2])
    c, d = cadd(x[1], x[3]), turn(csub(x[1], x[3]))
    return [cadd(a, c), cadd(b, d), csub(a, c), csub(b, d)]


def eight_point(x):
    even, odd = four_point(x[0::2]), four_point(x[1::2])
    r = math.sqrt(0.5)
    odd = [
        odd[0],
        ((odd[1][0] - odd[1][1]) * r, (odd[1][0] + odd[1][1]) * r),
        turn(odd[2]),
        ((-odd[3][0] - odd[3][1]) * r, (odd[3][0] - odd[3][1]) * r),
    ]
    return [cadd(e, o) for e, o in zip(even, odd)] + [csub(e, o) for e, o in zip(even, odd)]


def image_kernel(*refs):
    (
        count_ref, offset_ref, vis_ref, weight_ref, kernel_ref, tile_ref, plane_ref, chan_ref,
        tap_ref, line_ref, twist_ref, screen_ref,
    ) = refs[13:25]
    fetches = [pltpu.make_async_copy(refs[i], refs[13 + i], refs[-1].at[i]) for i in range(12)]
    for i in FETCH_ORDER:
        fetches[i].start()
    out_ref = refs[12]
    image_body(
        fetches, count_ref, offset_ref, vis_ref, weight_ref, kernel_ref, tile_ref, plane_ref, chan_ref,
        tap_ref, line_ref, twist_ref, screen_ref, out_ref, *refs[25:-1]
    )


SEND_ORDER = (10, 26, 8, 24, 2, 18, 9, 25, 11, 27, 6, 22, 14, 30, 5, 21, 7, 23, 13, 29, 15, 31, 4, 20, 12, 28, 1, 17, 3, 19, 16)


def plane_peer(me, j):
    there = (me + j) % 32
    return there, {"chan_1": there // 16, "bl_0": there // 4 % 4, "bl_1": there % 4}


FETCH_ORDER = (8, 4, 0, 1, 2, 3, 5, 6, 7, 9, 10, 11)


def image_body(
    fetches, count_ref, offset_ref, vis_ref, weight_ref, kernel_ref, tile_ref, plane_ref, chan_ref,
    tap_ref, line_ref, twist_ref, screen_ref, out_ref, taps, updates, bank_of, lane_hot, grid, lines, screens, image,
    own, plane_in, plane_sum, line_in, moment_own, plane_send, plane_recv, line_send, line_recv,
):
    barrier = pltpu.get_barrier_semaphore()
    signal = functools.partial(pl.semaphore_signal, barrier, inc=1, device_id_type=MESH_ID)
    me = lax.axis_index("chan_1") * 16 + lax.axis_index("bl_0") * 4 + lax.axis_index("bl_1")
    for j in range(1, 32):
        signal(device_id=plane_peer(me, j)[1])
    deep = lax.axis_index("chan_0") * 4 + lax.axis_index("bl_2")
    for j in range(1, 8):
        there = (deep + j) % 8
        signal(device_id={"bl_2": there % 4, "chan_0": there // 4})

    for i in (8, 4):
        fetches[i].wait()
    taps[...] = jnp.dot(tap_ref[...], kernel_ref[...], preferred_element_type=f32)
    for i in (0, 1, 2, 3, 5, 6, 7):
        fetches[i].wait()
    count = jnp.broadcast_to(count_ref[0:1, 0:1], (1, CHUNK))
    offsets = [jnp.broadcast_to(offset_ref[0:1, c:c + 1], (1, CHUNK)) for c in range(16)]

    def one_chunk(step, sums):
        at = pl.ds(pl.multiple_of(step * CHUNK, CHUNK), CHUNK)
        slot = step * CHUNK + lax.broadcasted_iota(jnp.int32, (1, CHUNK), 1)
        weight = jnp.where(slot < count, weight_ref[:, at].astype(f32), 0.0)
        chan = chan_ref[:, at]
        coord = jnp.zeros((1, CHUNK), f32)
        for c in range(16):
            coord = jnp.where(chan == c, offsets[c], coord)
        tile = tile_ref[:, at]
        plane = plane_ref[:, at]
        direct = plane >= HALF_PLANES
        tile_v = tile & 511
        tile_v = jnp.where(direct, tile_v, 511 - tile_v)
        half = jnp.where(direct, plane - HALF_PLANES, HALF_PLANES - 1 - plane)
        across = lambda row: jnp.transpose(jnp.broadcast_to(row.astype(f32), (LANES, CHUNK)))
        bank_of[at, :] = across(half * 4 + (tile_v & 3)).astype(bf16)
        lane = lax.broadcasted_iota(jnp.int32, (CHUNK, LANES), 1).astype(f32)
        lane_hot[at, :] = jnp.where(across(tile_v >> 2) == lane, 1.0, 0.0).astype(bf16)
        weighted = weight * taps[256:257, at]
        new_sums = []
        power = weighted
        for m in range(MOMENTS):
            new_sums.append(sums[m] + power)
            power = power * coord
        vis = vis_ref[:, at].astype(f32)
        base = (weight * vis[0:1], weight * vis[1:2])
        row = lax.broadcasted_iota(jnp.int32, (STRIP, CHUNK), 0) - STRIP // 2
        phase = unit_circle(((tile >> 9) * row) & 511)
        turned = cmul(phase, base)
        mirror = jnp.where(direct, 1.0, -1.0)
        flipped = (turned[0] * mirror, turned[1] * mirror)
        direct_rows = jnp.broadcast_to(direct, (STRIP, CHUNK))
        coord_rows = jnp.broadcast_to(coord, (STRIP, CHUNK))
        parts = []
        for e in range(TILE):
            r = slice(e * STRIP, (e + 1) * STRIP)
            i = slice(64 + e * STRIP, 64 + (e + 1) * STRIP)
            tap_r = taps[r, at] + taps[128 + r.start:128 + r.stop, at]
            tap_i = taps[i, at] + taps[128 + i.start:128 + i.stop, at]
            parts.append(
                (turned[0] * tap_r - turned[1] * tap_i, flipped[0] * tap_i + flipped[1] * tap_r)
            )
        zero = jnp.zeros((STRIP, CHUNK), f32)
        for e in range(WIDE):
            there = parts[e] if e < TILE else (zero, zero)
            back = parts[TILE - e] if e > 0 else (zero, zero)
            both = jnp.concatenate(
                [jnp.where(direct_rows, there[0], back[0]), jnp.where(direct_rows, there[1], back[1])], axis=0
            )
            for k in range(TAYLOR):
                if k > 0:
                    both = both * jnp.concatenate([coord_rows, coord_rows], axis=0)
                high = both.astype(bf16)
                low = (both - high.astype(f32)).astype(bf16)
                first = 2 * k * SPAN + e * 16
                updates[first:first + 16, at] = high
                updates[first + SPAN:first + SPAN + 16, at] = low
        return tuple(new_sums)

    sums = lax.fori_loop(
        0, SLOTS // CHUNK, one_chunk, tuple(jnp.zeros((1, CHUNK), f32) for _ in range(MOMENTS))
    )
    lane = lax.broadcasted_iota(jnp.int32, (STRIP, LANES), 1)
    moment_row = jnp.zeros((STRIP, LANES), f32)
    for m in range(MOMENTS):
        total = jnp.sum(sums[m], axis=1, keepdims=True)
        moment_row = jnp.where(lane == m, jnp.broadcast_to(total, (STRIP, LANES)), moment_row)
    moment_own[...] = moment_row

    def spread(k):
        for step in range(CELLS // CHUNK):
            banks = bank_of[...]
            halves = [
                jnp.where(banks == jnp.asarray(step * 2 + half, bf16), lane_hot[...], jnp.zeros((), bf16))
                for half in range(CHUNK // LANES)
            ]
            both = jnp.dot(
                updates[2 * SPAN * k:2 * SPAN * (k + 1)], jnp.concatenate(halves, axis=1), preferred_element_type=f32
            )
            grid[SPAN * k:SPAN * (k + 1), step * CHUNK:(step + 1) * CHUNK] = both[:SPAN] + both[SPAN:]

    for i in (9, 10, 11):
        fetches[i].wait()
    for b in range(BLOCKS):
        one = (screen_ref[0, b], screen_ref[1, b])
        two = cmul(one, one)
        for q in range(HALF_PLANES):
            screens[q, 0, b] = one[0]
            screens[q, 1, b] = one[1]
            if q < HALF_PLANES - 1:
                one = cmul(one, two)

    def piece(k, e, part, q, vb):
        first = ((k * WIDE + e) * 2 + part) * STRIP
        at = pl.ds(pl.multiple_of(q * 512 + vb * LANES, LANES), LANES)
        return grid[first:first + STRIP, at]

    def one_term(k):
        for q in range(HALF_PLANES):
            residues = []
            for vb in range(4):
                halves = []
                for part in range(2):
                    spill = piece(k, TILE, part, q, (vb - 1) % 4)
                    if vb == 0:
                        spill = pltpu.roll(spill, 1, 1)
                    column = [piece(k, 0, part, q, vb) + spill]
                    column += [piece(k, e, part, q, vb) for e in range(1, TILE)]
                    halves.append(jnp.concatenate(column, axis=0))
                residues.append(jnp.concatenate(halves, axis=1))
            whole = jnp.concatenate(residues, axis=0)
            high = whole.astype(bf16)
            low = (whole - high.astype(f32)).astype(bf16)
            lines[q] = (
                jnp.dot(high, line_ref[0:256], preferred_element_type=f32)
                + jnp.dot(low, line_ref[0:256], preferred_element_type=f32)
                + jnp.dot(high, line_ref[256:512], preferred_element_type=f32)
            )
        for q in range(HALF_PLANES):
            quarters = [[], [], [], []]
            for e in range(TILE):
                x = []
                for vb in range(4):
                    first = (vb * TILE + e) * STRIP
                    value = (lines[q, first:first + STRIP, 0:LANES], lines[q, first:first + STRIP, LANES:2 * LANES])
                    if vb > 0:
                        value = cmul(value, (twist_ref[vb:vb + 1], twist_ref[36 + vb:37 + vb]))
                    x.append(value)
                for mr, value in enumerate(four_point(x)):
                    if e > 0:
                        t = 4 + e * 4 + mr
                        value = cmul(value, (twist_ref[t:t + 1], twist_ref[36 + t:37 + t]))
                    quarters[mr].append(value)
            for mr in range(4):
                for mh, value in enumerate(eight_point(quarters[mr])):
                    b = 4 * mh + mr
                    add = value[0] * screens[q, 0, b] - value[1] * screens[q, 1, b]
                    if q < HALF_PLANES - 1:
                        image[b] = image[b] + add if q > 0 else add
                    else:
                        total = image[b] + add
                        first = b // 4 * 8 + b % 4
                        own[k, pl.ds(first, 4, stride=64), :] = total[0:4]
                        own[k, pl.ds(first + 4, 4, stride=64), :] = total[4:8]

    low_z = lax.axis_index("chan_0")
    core = lax.axis_index("chan_1")
    me = core * 16 + lax.axis_index("bl_0") * 4 + lax.axis_index("bl_1")
    deep = low_z * 4 + lax.axis_index("bl_2")

    def together(source, target, send, recv):
        return pltpu.make_async_remote_copy(
            src_ref=source, dst_ref=target, send_sem=send, recv_sem=recv,
            device_id={"chan_1": 1 - core}, device_id_type=MESH_ID,
        )

    def send_plane(k):
        for j in SEND_ORDER:
            there, where = plane_peer(me, j)
            pltpu.make_async_remote_copy(
                src_ref=own.at[k, pl.ds(pl.multiple_of(there * 8, 8), 8)] if k < TAYLOR else moment_own,
                dst_ref=plane_in.at[k, j], send_sem=plane_send.at[k], recv_sem=plane_recv.at[k],
                device_id=where, device_id_type=MESH_ID,
            ).start()

    pl.semaphore_wait(barrier, 38)
    send_plane(TAYLOR)
    for k in range(TAYLOR):
        spread(k)
        one_term(k)
        send_plane(k)

    for k in (TAYLOR, 0, 1, 2):
        total = own[k, pl.ds(pl.multiple_of(me * 8, 8), 8)] if k < TAYLOR else moment_own[...]
        together(plane_in.at[3, 1:32], plane_in.at[k, 1:32], plane_send.at[k], plane_recv.at[k]).wait()
        for j in range(1, 32):
            total = total + plane_in[k, j]
        for r in range(8):
            plane_sum[r, k:k + 1] = total[r:r + 1]

    for j in range(1, 8):
        there = (deep + j) % 8
        pltpu.make_async_remote_copy(
            src_ref=plane_sum.at[there], dst_ref=line_in.at[j], send_sem=line_send, recv_sem=line_recv,
            device_id={"bl_2": there % 4, "chan_0": there // 4}, device_id_type=MESH_ID,
        ).start()
    total = plane_sum[deep]
    together(plane_sum.at[0:7], line_in.at[1:8], line_send, line_recv).wait()
    for j in range(1, 8):
        total = total + line_in[j]
    moments = [total[TAYLOR:TAYLOR + 1, m:m + 1] for m in range(MOMENTS)]
    images = [total[k:k + 1] for k in range(TAYLOR)]
    rows, determinant = solve_taylor(moments, images)
    for k in range(TAYLOR):
        out_ref[0, k:k + 1] = rows[k]
        out_ref[1, k:k + 1] = jnp.broadcast_to(determinant, (1, LANES))


def device_image(counts, offsets, vis, weight, kernel, tile, plane, chan):
    vmem = pl.BlockSpec(memory_space=pltpu.VMEM)
    dma = pltpu.SemaphoreType.DMA
    operands = (
        counts, offsets, vis, weight, kernel, tile, plane, chan,
        jnp.asarray(tap_table()), jnp.asarray(line_table()), jnp.asarray(twist_table()), jnp.asarray(screen_table()),
    )
    return pl.pallas_call(
        image_kernel,
        out_shape=jax.ShapeDtypeStruct((2, TAYLOR, LANES), f32),
        in_specs=[pl.BlockSpec(memory_space=pltpu.HBM)] * 12,
        out_specs=vmem,
        scratch_shapes=[pltpu.VMEM(a.shape, a.dtype) for a in operands] + [
            pltpu.VMEM((272, SLOTS), f32),
            pltpu.VMEM((2 * ROWS, SLOTS), bf16),
            pltpu.VMEM((SLOTS, LANES), bf16),
            pltpu.VMEM((SLOTS, LANES), bf16),
            pltpu.VMEM((ROWS, CELLS), f32),
            pltpu.VMEM((HALF_PLANES, 256, 256), f32),
            pltpu.VMEM((HALF_PLANES, 2, BLOCKS, STRIP, LANES), f32),
            pltpu.VMEM((BLOCKS, STRIP, LANES), f32),
            pltpu.VMEM((TAYLOR, 256, LANES), f32),
            pltpu.VMEM((TAYLOR + 1, 32, 8, LANES), f32),
            pltpu.VMEM((8, 4, LANES), f32),
            pltpu.VMEM((8, 4, LANES), f32),
            pltpu.VMEM((8, LANES), f32),
            dma((4,)), dma((4,)), dma, dma, dma((12,)),
        ],
        compiler_params=pltpu.CompilerParams(
            vmem_limit_bytes=56 * 1024 * 1024, collective_id=0, has_side_effects=True
        ),
        name="strip_image",
    )(*operands)


def solve_taylor(moments, images):
    entry_00, entry_01, entry_02 = (moments[0], moments[1], moments[2])
    entry_11, entry_12, entry_22 = (moments[2], moments[3], moments[4])
    minor_00 = entry_11 * entry_22 - entry_12 * entry_12
    minor_01 = entry_02 * entry_12 - entry_01 * entry_22
    minor_02 = entry_01 * entry_12 - entry_02 * entry_11
    minor_11 = entry_00 * entry_22 - entry_02 * entry_02
    minor_12 = entry_01 * entry_02 - entry_00 * entry_12
    minor_22 = entry_00 * entry_11 - entry_01 * entry_01
    determinant = entry_00 * minor_00 + entry_01 * minor_01 + entry_02 * minor_02
    first = minor_00 * images[0] + minor_01 * images[1] + minor_02 * images[2]
    second = minor_01 * images[0] + minor_11 * images[1] + minor_12 * images[2]
    third = minor_02 * images[0] + minor_12 * images[1] + minor_22 * images[2]
    return (first, second, third), determinant


MESH_ID = pl.DeviceIdType.MESH


def body(vis_value, vis_weight, kernel, tile_index, plane_index, chan_index, chan_offset, counts):
    scaled = device_image(
        counts, chan_offset, vis_value[0, 0], vis_weight[0], kernel[0, 0],
        tile_index[0], plane_index[0], chan_index[0],
    )
    return scaled[0] / scaled[1]


def solution(mesh):
    split = Mesh(mesh.devices.reshape(2, 2, 4, 4, 4), ("chan_0", "chan_1", "bl_0", "bl_1", "bl_2"))
    return jax.shard_map(
        body,
        mesh=split,
        in_specs=(
            P(CHAN, BL, None, None),
            P(CHAN, BL, None),
            P(CHAN, BL, None, None),
            P(CHAN, BL, None),
            P(CHAN, BL, None),
            P(CHAN, BL, None),
            P(CHAN, None),
            P(CHAN, BL),
        ),
        out_specs=P(None, CHAN_BL),
        check_vma=False,
    )
```

```python
import functools
import math

import jax
import jax.numpy as jnp
import numpy as np
from jax import lax
from jax.experimental import pallas as pl
from jax.experimental.pallas import tpu as pltpu
from jax.sharding import Mesh
from jax.sharding import PartitionSpec as P

NPIX = 4096
TILE = 8
TAYLOR = 3
MOMENTS = 5
STRIP = 8
SLOTS = 2048
HALF_PLANES = 4
WIDE = TILE + 1
ROWS = TAYLOR * WIDE * 2 * STRIP
SPAN = WIDE * 2 * STRIP
CELLS = HALF_PLANES * NPIX // TILE
BLOCKS = 32
LANES = 128
CHUNK = 256
CHAN_BL = ("chan_0", "chan_1", "bl_0", "bl_1", "bl_2")
CHAN = ("chan_0", "chan_1")
BL = ("bl_0", "bl_1", "bl_2")
f32 = jnp.float32
bf16 = jnp.bfloat16


def split_pair(table):
    high = table.astype(np.float32).astype(bf16)
    low = (table - high.astype(np.float64)).astype(np.float32).astype(bf16)
    return high, low


def tap_table():
    a = np.arange(TILE)[None, :]
    l = np.arange(STRIP)[:, None] - STRIP // 2
    angle = 2.0 * math.pi * ((a - NPIX // 2) * l % NPIX) / NPIX
    table = np.zeros((2, TILE, STRIP, TILE, TILE))
    for e in range(TILE):
        table[0, e, :, :, e] = np.cos(angle)
        table[1, e, :, :, e] = np.sin(angle)
    high, low = split_pair(table.reshape(2 * TILE * STRIP, TILE * TILE))
    ones = np.zeros((16, 2 * TILE * TILE), np.float32)
    ones[0, :TILE * TILE] = 1.0
    return np.concatenate([np.concatenate([high, low], axis=1), ones.astype(bf16)], axis=0)


def line_table():
    n = np.arange(LANES)
    angle = 2.0 * math.pi * (n[:, None] * n[None, :] % LANES) / LANES
    sign = 1.0 - 2.0 * (n % 2)
    c, s = np.cos(angle) * sign, np.sin(angle) * sign
    return np.concatenate(split_pair(np.block([[c, s], [-s, c]])), axis=0)


def twist_table():
    mq = np.arange(LANES)
    rows = [2.0 * math.pi * 8 * vb * mq / NPIX for vb in range(4)]
    for e in range(TILE):
        for mr in range(4):
            rows.append(2.0 * math.pi * e * (mq + LANES * mr) / NPIX + math.pi * e)
    angle = np.stack(rows)
    return np.concatenate([np.cos(angle), np.sin(angle)], axis=0).astype(np.float32)


def screen_table():
    cell = 0.5 / NPIX
    l = np.arange(STRIP)[None, :, None] - STRIP // 2
    m = (np.arange(BLOCKS)[:, None, None] - BLOCKS // 2) * LANES + np.arange(LANES)[None, None, :]
    radius = (l * cell) ** 2 + (m * cell) ** 2
    s = -radius / (1.0 + np.sqrt(1.0 - radius))
    angle = 2.0 * math.pi * 20.0 * s
    return np.stack([np.cos(angle), np.sin(angle)]).astype(np.float32)


def unit_circle(index):
    quarter = ((index + 64) >> 7) & 3
    x = (((index + 64) & 127) - 64).astype(f32) * (2.0 * math.pi / 512.0)
    x2 = x * x
    s = x * (1.0 + x2 * (-1.0 / 6 + x2 * (1.0 / 120 + x2 * (-1.0 / 5040 + x2 * (1.0 / 362880)))))
    c = 1.0 + x2 * (-0.5 + x2 * (1.0 / 24 + x2 * (-1.0 / 720 + x2 * (1.0 / 40320))))
    odd = (quarter & 1) == 1
    cos = jnp.where(odd, s, c)
    sin = jnp.where(odd, c, s)
    cos = jnp.where((quarter == 1) | (quarter == 2), -cos, cos)
    sin = jnp.where(quarter >= 2, -sin, sin)
    return cos, sin


def cmul(a, b):
    return a[0] * b[0] - a[1] * b[1], a[0] * b[1] + a[1] * b[0]


def cadd(a, b):
    return a[0] + b[0], a[1] + b[1]


def csub(a, b):
    return a[0] - b[0], a[1] - b[1]


def turn(a):
    return -a[1], a[0]


def four_point(x):
    a, b = cadd(x[0], x[2]), csub(x[0], x[2])
    c, d = cadd(x[1], x[3]), turn(csub(x[1], x[3]))
    return [cadd(a, c), cadd(b, d), csub(a, c), csub(b, d)]


def eight_point(x):
    even, odd = four_point(x[0::2]), four_point(x[1::2])
    r = math.sqrt(0.5)
    odd = [
        odd[0],
        ((odd[1][0] - odd[1][1]) * r, (odd[1][0] + odd[1][1]) * r),
        turn(odd[2]),
        ((-odd[3][0] - odd[3][1]) * r, (odd[3][0] - odd[3][1]) * r),
    ]
    return [cadd(e, o) for e, o in zip(even, odd)] + [csub(e, o) for e, o in zip(even, odd)]


def image_kernel(*refs):
    offset_ref = refs[0]
    (
        count_ref, vis_ref, weight_ref, kernel_ref, tile_ref, plane_ref, chan_ref,
        tap_ref, line_ref, twist_ref, screen_ref,
    ) = refs[13:24]
    fetches = [pltpu.make_async_copy(refs[1 + i], refs[13 + i], refs[-1].at[i]) for i in range(11)]
    for i in FETCH_ORDER:
        fetches[i].start()
    out_ref = refs[12]
    image_body(
        fetches, count_ref, offset_ref, vis_ref, weight_ref, kernel_ref, tile_ref, plane_ref, chan_ref,
        tap_ref, line_ref, twist_ref, screen_ref, out_ref, *refs[24:-1]
    )


START_X = (0.0, 0.8, 1.7, 1.8)
START_Z = (0, 1, 2, 3, 7, 4, 5, 6)
PLANE_ORDER = sorted(range(32), key=lambda t: START_X[t // 4 % 4] + START_X[t % 4] + 1.2 * (t // 16))
LINE_ORDER = tuple(z % 2 * 4 + z // 2 for z in START_Z)


def plane_peer(me, j):
    there = (me + j) % 32
    return there, {"chan_1": there // 16, "bl_0": there // 4 % 4, "bl_1": there % 4}


FETCH_ORDER = (7, 3, 0, 1, 2, 4, 5, 6, 8, 9, 10)


def image_body(
    fetches, count_ref, offset_ref, vis_ref, weight_ref, kernel_ref, tile_ref, plane_ref, chan_ref,
    tap_ref, line_ref, twist_ref, screen_ref, out_ref, taps, updates, bank_of, lane_hot, grid, lines, screens, image,
    own, plane_in, plane_sum, line_in, moment_own, plane_send, plane_recv, line_send, line_recv,
):
    barrier = pltpu.get_barrier_semaphore()
    signal = functools.partial(pl.semaphore_signal, barrier, inc=1, device_id_type=MESH_ID)
    me = lax.axis_index("chan_1") * 16 + lax.axis_index("bl_0") * 4 + lax.axis_index("bl_1")
    for j in range(1, 32):
        signal(device_id=plane_peer(me, j)[1])
    deep = lax.axis_index("chan_0") * 4 + lax.axis_index("bl_2")
    for j in range(1, 8):
        there = (deep + j) % 8
        signal(device_id={"bl_2": there % 4, "chan_0": there // 4})

    for i in (7, 3):
        fetches[i].wait()
    taps[...] = jnp.dot(
        tap_ref[...], jnp.concatenate([kernel_ref[...], kernel_ref[...]], axis=0), preferred_element_type=f32
    )
    for i in (0, 1, 2, 4, 5, 6):
        fetches[i].wait()
    count = jnp.broadcast_to(count_ref[0:1, 0:1], (1, CHUNK))
    offsets = [jnp.broadcast_to(offset_ref[0:1, c:c + 1], (1, CHUNK)) for c in range(16)]

    def one_chunk(step, sums):
        at = pl.ds(pl.multiple_of(step * CHUNK, CHUNK), CHUNK)
        slot = step * CHUNK + lax.broadcasted_iota(jnp.int32, (1, CHUNK), 1)
        weight = jnp.where(slot < count, weight_ref[:, at].astype(f32), 0.0)
        chan = chan_ref[:, at]
        coord = jnp.zeros((1, CHUNK), f32)
        for c in range(16):
            coord = jnp.where(chan == c, offsets[c], coord)
        tile = tile_ref[:, at]
        plane = plane_ref[:, at]
        direct = plane >= HALF_PLANES
        tile_v = tile & 511
        tile_v = jnp.where(direct, tile_v, 511 - tile_v)
        half = jnp.where(direct, plane - HALF_PLANES, HALF_PLANES - 1 - plane)
        across = lambda row: jnp.transpose(jnp.broadcast_to(row.astype(f32), (LANES, CHUNK)))
        bank_of[at, :] = across(half * 4 + (tile_v & 3)).astype(bf16)
        lane = lax.broadcasted_iota(jnp.int32, (CHUNK, LANES), 1).astype(f32)
        lane_hot[at, :] = jnp.where(across(tile_v >> 2) == lane, 1.0, 0.0).astype(bf16)
        weighted = weight * taps[128:129, at]
        new_sums = []
        power = weighted
        for m in range(MOMENTS):
            new_sums.append(sums[m] + power)
            power = power * coord
        vis = vis_ref[:, at].astype(f32)
        base = (weight * vis[0:1], weight * vis[1:2])
        row = lax.broadcasted_iota(jnp.int32, (STRIP, CHUNK), 0) - STRIP // 2
        phase = unit_circle(((tile >> 9) * row) & 511)
        turned = cmul(phase, base)
        mirror = jnp.where(direct, 1.0, -1.0)
        flipped = (turned[0] * mirror, turned[1] * mirror)
        direct_rows = jnp.broadcast_to(direct, (STRIP, CHUNK))
        coord_rows = jnp.broadcast_to(coord, (STRIP, CHUNK))
        parts = []
        for e in range(TILE):
            r = slice(e * STRIP, (e + 1) * STRIP)
            i = slice(64 + e * STRIP, 64 + (e + 1) * STRIP)
            tap_r, tap_i = taps[r, at], taps[i, at]
            parts.append(
                (turned[0] * tap_r - turned[1] * tap_i, flipped[0] * tap_i + flipped[1] * tap_r)
            )
        zero = jnp.zeros((STRIP, CHUNK), f32)
        for e in range(WIDE):
            there = parts[e] if e < TILE else (zero, zero)
            back = parts[TILE - e] if e > 0 else (zero, zero)
            both = jnp.concatenate(
                [jnp.where(direct_rows, there[0], back[0]), jnp.where(direct_rows, there[1], back[1])], axis=0
            )
            for k in range(TAYLOR):
                if k > 0:
                    both = both * jnp.concatenate([coord_rows, coord_rows], axis=0)
                high = both.astype(bf16)
                low = (both - high.astype(f32)).astype(bf16)
                first = 2 * k * SPAN + e * 16
                updates[first:first + 16, at] = high
                updates[first + SPAN:first + SPAN + 16, at] = low
        return tuple(new_sums)

    sums = lax.fori_loop(
        0, SLOTS // CHUNK, one_chunk, tuple(jnp.zeros((1, CHUNK), f32) for _ in range(MOMENTS))
    )
    lane = lax.broadcasted_iota(jnp.int32, (STRIP, LANES), 1)
    moment_row = jnp.zeros((STRIP, LANES), f32)
    for m in range(MOMENTS):
        total = jnp.sum(sums[m], axis=1, keepdims=True)
        moment_row = jnp.where(lane == m, jnp.broadcast_to(total, (STRIP, LANES)), moment_row)
    moment_own[...] = moment_row

    def spread(k):
        for step in range(CELLS // CHUNK):
            banks = bank_of[...]
            halves = [
                jnp.where(banks == jnp.asarray(step * 2 + half, bf16), lane_hot[...], jnp.zeros((), bf16))
                for half in range(CHUNK // LANES)
            ]
            both = jnp.dot(
                updates[2 * SPAN * k:2 * SPAN * (k + 1)], jnp.concatenate(halves, axis=1), preferred_element_type=f32
            )
            grid[SPAN * k:SPAN * (k + 1), step * CHUNK:(step + 1) * CHUNK] = both[:SPAN] + both[SPAN:]

    for i in (8, 9, 10):
        fetches[i].wait()
    for b in range(BLOCKS):
        one = (screen_ref[0, b], screen_ref[1, b])
        two = cmul(one, one)
        for q in range(HALF_PLANES):
            screens[q, 0, b] = one[0]
            screens[q, 1, b] = one[1]
            if q < HALF_PLANES - 1:
                one = cmul(one, two)

    def piece(k, e, part, q, vb):
        first = ((k * WIDE + e) * 2 + part) * STRIP
        at = pl.ds(pl.multiple_of(q * 512 + vb * LANES, LANES), LANES)
        return grid[first:first + STRIP, at]

    def one_term(k):
        for q in range(HALF_PLANES):
            residues = []
            for vb in range(4):
                halves = []
                for part in range(2):
                    spill = piece(k, TILE, part, q, (vb - 1) % 4)
                    if vb == 0:
                        spill = pltpu.roll(spill, 1, 1)
                    column = [piece(k, 0, part, q, vb) + spill]
                    column += [piece(k, e, part, q, vb) for e in range(1, TILE)]
                    halves.append(jnp.concatenate(column, axis=0))
                residues.append(jnp.concatenate(halves, axis=1))
            whole = jnp.concatenate(residues, axis=0)
            high = whole.astype(bf16)
            low = (whole - high.astype(f32)).astype(bf16)
            lines[q] = (
                jnp.dot(high, line_ref[0:256], preferred_element_type=f32)
                + jnp.dot(low, line_ref[0:256], preferred_element_type=f32)
                + jnp.dot(high, line_ref[256:512], preferred_element_type=f32)
            )
        for q in range(HALF_PLANES):
            quarters = [[], [], [], []]
            for e in range(TILE):
                x = []
                for vb in range(4):
                    first = (vb * TILE + e) * STRIP
                    value = (lines[q, first:first + STRIP, 0:LANES], lines[q, first:first + STRIP, LANES:2 * LANES])
                    if vb > 0:
                        value = cmul(value, (twist_ref[vb:vb + 1], twist_ref[36 + vb:37 + vb]))
                    x.append(value)
                for mr, value in enumerate(four_point(x)):
                    if e > 0:
                        t = 4 + e * 4 + mr
                        value = cmul(value, (twist_ref[t:t + 1], twist_ref[36 + t:37 + t]))
                    quarters[mr].append(value)
            for mr in range(4):
                for mh, value in enumerate(eight_point(quarters[mr])):
                    b = 4 * mh + mr
                    add = value[0] * screens[q, 0, b] - value[1] * screens[q, 1, b]
                    if q < HALF_PLANES - 1:
                        image[b] = image[b] + add if q > 0 else add
                    else:
                        total = image[b] + add
                        first = b // 4 * 8 + b % 4
                        own[k, pl.ds(first, 4, stride=64), :] = total[0:4]
                        own[k, pl.ds(first + 4, 4, stride=64), :] = total[4:8]

    low_z = lax.axis_index("chan_0")
    core = lax.axis_index("chan_1")
    me = core * 16 + lax.axis_index("bl_0") * 4 + lax.axis_index("bl_1")
    deep = low_z * 4 + lax.axis_index("bl_2")

    def together(source, target, send, recv):
        return pltpu.make_async_remote_copy(
            src_ref=source, dst_ref=target, send_sem=send, recv_sem=recv,
            device_id={"chan_1": 1 - core}, device_id_type=MESH_ID,
        )

    def send_plane(k):
        for there in PLANE_ORDER:
            copy = pltpu.make_async_remote_copy(
                src_ref=own.at[k, there * 8:there * 8 + 8] if k < TAYLOR else moment_own,
                dst_ref=plane_in.at[k, (me - there) % 32], send_sem=plane_send.at[k], recv_sem=plane_recv.at[k],
                device_id={"chan_1": there // 16, "bl_0": there // 4 % 4, "bl_1": there % 4}, device_id_type=MESH_ID,
            )
            pl.when(me != there)(copy.start)

    for k in range(TAYLOR):
        spread(k)
        one_term(k)
        if k == 0:
            pl.semaphore_wait(barrier, 38)
            send_plane(TAYLOR)
        send_plane(k)

    for k in (TAYLOR, 0, 1, 2):
        total = own[k, pl.ds(pl.multiple_of(me * 8, 8), 8)] if k < TAYLOR else moment_own[...]
        together(plane_in.at[3, 1:32], plane_in.at[k, 1:32], plane_send.at[k], plane_recv.at[k]).wait()
        for j in range(1, 32):
            total = total + plane_in[k, j]
        for r in range(8):
            plane_sum[r, k:k + 1] = total[r:r + 1]

    for there in LINE_ORDER:
        copy = pltpu.make_async_remote_copy(
            src_ref=plane_sum.at[there], dst_ref=line_in.at[(deep - there) % 8], send_sem=line_send, recv_sem=line_recv,
            device_id={"bl_2": there % 4, "chan_0": there // 4}, device_id_type=MESH_ID,
        )
        pl.when(deep != there)(copy.start)
    total = plane_sum[deep]
    together(plane_sum.at[0:7], line_in.at[1:8], line_send, line_recv).wait()
    for j in range(1, 8):
        total = total + line_in[j]
    moments = [total[TAYLOR:TAYLOR + 1, m:m + 1] for m in range(MOMENTS)]
    images = [total[k:k + 1] for k in range(TAYLOR)]
    rows, determinant = solve_taylor(moments, images)
    for k in range(TAYLOR):
        out_ref[0, k:k + 1] = rows[k]
        out_ref[1, k:k + 1] = jnp.broadcast_to(determinant, (1, LANES))


def device_image(counts, offsets, vis, weight, kernel, tile, plane, chan):
    vmem = pl.BlockSpec(memory_space=pltpu.VMEM)
    dma = pltpu.SemaphoreType.DMA
    operands = (
        counts, vis, weight, kernel, tile, plane, chan,
        jnp.asarray(tap_table()), jnp.asarray(line_table()), jnp.asarray(twist_table()), jnp.asarray(screen_table()),
    )
    return pl.pallas_call(
        image_kernel,
        out_shape=jax.ShapeDtypeStruct((2, TAYLOR, LANES), f32),
        in_specs=[vmem] + [pl.BlockSpec(memory_space=pltpu.HBM)] * 11,
        out_specs=vmem,
        scratch_shapes=[pltpu.VMEM(a.shape, a.dtype) for a in operands] + [
            pltpu.VMEM((144, SLOTS), f32),
            pltpu.VMEM((2 * ROWS, SLOTS), bf16),
            pltpu.VMEM((SLOTS, LANES), bf16),
            pltpu.VMEM((SLOTS, LANES), bf16),
            pltpu.VMEM((ROWS, CELLS), f32),
            pltpu.VMEM((HALF_PLANES, 256, 256), f32),
            pltpu.VMEM((HALF_PLANES, 2, BLOCKS, STRIP, LANES), f32),
            pltpu.VMEM((BLOCKS, STRIP, LANES), f32),
            pltpu.VMEM((TAYLOR, 256, LANES), f32),
            pltpu.VMEM((TAYLOR + 1, 32, 8, LANES), f32),
            pltpu.VMEM((8, 4, LANES), f32),
            pltpu.VMEM((8, 4, LANES), f32),
            pltpu.VMEM((8, LANES), f32),
            dma((4,)), dma((4,)), dma, dma, dma((11,)),
        ],
        compiler_params=pltpu.CompilerParams(
            vmem_limit_bytes=55220 * 1024, collective_id=0, has_side_effects=True
        ),
        name="strip_image",
    )(offsets, *operands)


def solve_taylor(moments, images):
    entry_00, entry_01, entry_02 = (moments[0], moments[1], moments[2])
    entry_11, entry_12, entry_22 = (moments[2], moments[3], moments[4])
    minor_00 = entry_11 * entry_22 - entry_12 * entry_12
    minor_01 = entry_02 * entry_12 - entry_01 * entry_22
    minor_02 = entry_01 * entry_12 - entry_02 * entry_11
    minor_11 = entry_00 * entry_22 - entry_02 * entry_02
    minor_12 = entry_01 * entry_02 - entry_00 * entry_12
    minor_22 = entry_00 * entry_11 - entry_01 * entry_01
    determinant = entry_00 * minor_00 + entry_01 * minor_01 + entry_02 * minor_02
    first = minor_00 * images[0] + minor_01 * images[1] + minor_02 * images[2]
    second = minor_01 * images[0] + minor_11 * images[1] + minor_12 * images[2]
    third = minor_02 * images[0] + minor_12 * images[1] + minor_22 * images[2]
    return (first, second, third), determinant


MESH_ID = pl.DeviceIdType.MESH


def body(vis_value, vis_weight, kernel, tile_index, plane_index, chan_index, chan_offset, counts):
    scaled = device_image(
        counts, chan_offset, vis_value[0, 0], vis_weight[0], kernel[0, 0],
        tile_index[0], plane_index[0], chan_index[0],
    )
    return scaled[0] / scaled[1]


def solution(mesh):
    split = Mesh(mesh.devices.reshape(2, 2, 4, 4, 4), ("chan_0", "chan_1", "bl_0", "bl_1", "bl_2"))
    return jax.shard_map(
        body,
        mesh=split,
        in_specs=(
            P(CHAN, BL, None, None),
            P(CHAN, BL, None),
            P(CHAN, BL, None, None),
            P(CHAN, BL, None),
            P(CHAN, BL, None),
            P(CHAN, BL, None),
            P(CHAN, None),
            P(CHAN, BL),
        ),
        out_specs=P(None, CHAN_BL),
        check_vma=False,
    )
```

```python
import functools
import math

import jax
import jax.numpy as jnp
import numpy as np
from jax import lax
from jax.experimental import pallas as pl
from jax.experimental.pallas import tpu as pltpu
from jax.sharding import Mesh
from jax.sharding import PartitionSpec as P

NPIX = 4096
TILE = 8
TAYLOR = 3
MOMENTS = 5
STRIP = 8
SLOTS = 2048
HALF_PLANES = 4
WIDE = TILE + 1
ROWS = TAYLOR * WIDE * 2 * STRIP
SPAN = WIDE * 2 * STRIP
CELLS = HALF_PLANES * NPIX // TILE
BLOCKS = 32
LANES = 128
CHUNK = 256
CHAN_BL = ("chan_0", "chan_1", "bl_0", "bl_1", "bl_2")
CHAN = ("chan_0", "chan_1")
BL = ("bl_0", "bl_1", "bl_2")
f32 = jnp.float32
bf16 = jnp.bfloat16


def split_pair(table):
    high = table.astype(np.float32).astype(bf16)
    low = (table - high.astype(np.float64)).astype(np.float32).astype(bf16)
    return high, low


def tap_table():
    a = np.arange(TILE)[None, :]
    l = np.arange(STRIP)[:, None] - STRIP // 2
    angle = 2.0 * math.pi * ((a - NPIX // 2) * l % NPIX) / NPIX
    table = np.zeros((2, TILE, STRIP, TILE, TILE))
    for e in range(TILE):
        table[0, e, :, :, e] = np.cos(angle)
        table[1, e, :, :, e] = np.sin(angle)
    high, low = split_pair(table.reshape(2 * TILE * STRIP, TILE * TILE))
    ones = np.zeros((16, 2 * TILE * TILE), np.float32)
    ones[0, :TILE * TILE] = 1.0
    return np.concatenate([np.concatenate([high, low], axis=1), ones.astype(bf16)], axis=0)


def line_table():
    n = np.arange(LANES)
    angle = 2.0 * math.pi * (n[:, None] * n[None, :] % LANES) / LANES
    sign = 1.0 - 2.0 * (n % 2)
    c, s = np.cos(angle) * sign, np.sin(angle) * sign
    return np.concatenate(split_pair(np.block([[c, s], [-s, c]])), axis=0)


def twist_table():
    mq = np.arange(LANES)
    rows = [2.0 * math.pi * 8 * vb * mq / NPIX for vb in range(4)]
    for e in range(TILE):
        for mr in range(4):
            rows.append(2.0 * math.pi * e * (mq + LANES * mr) / NPIX + math.pi * e)
    angle = np.stack(rows)
    return np.concatenate([np.cos(angle), np.sin(angle)], axis=0).astype(np.float32)


def screen_table():
    cell = 0.5 / NPIX
    l = np.arange(STRIP)[None, :, None] - STRIP // 2
    m = (np.arange(BLOCKS)[:, None, None] - BLOCKS // 2) * LANES + np.arange(LANES)[None, None, :]
    radius = (l * cell) ** 2 + (m * cell) ** 2
    s = -radius / (1.0 + np.sqrt(1.0 - radius))
    angle = 2.0 * math.pi * 20.0 * s
    return np.stack([np.cos(angle), np.sin(angle)]).astype(np.float32)


def unit_circle(index):
    quarter = ((index + 64) >> 7) & 3
    x = (((index + 64) & 127) - 64).astype(f32) * (2.0 * math.pi / 512.0)
    x2 = x * x
    s = x * (1.0 + x2 * (-1.0 / 6 + x2 * (1.0 / 120 + x2 * (-1.0 / 5040 + x2 * (1.0 / 362880)))))
    c = 1.0 + x2 * (-0.5 + x2 * (1.0 / 24 + x2 * (-1.0 / 720 + x2 * (1.0 / 40320))))
    odd = (quarter & 1) == 1
    cos = jnp.where(odd, s, c)
    sin = jnp.where(odd, c, s)
    cos = jnp.where((quarter == 1) | (quarter == 2), -cos, cos)
    sin = jnp.where(quarter >= 2, -sin, sin)
    return cos, sin


def cmul(a, b):
    return a[0] * b[0] - a[1] * b[1], a[0] * b[1] + a[1] * b[0]


def cadd(a, b):
    return a[0] + b[0], a[1] + b[1]


def csub(a, b):
    return a[0] - b[0], a[1] - b[1]


def turn(a):
    return -a[1], a[0]


def four_point(x):
    a, b = cadd(x[0], x[2]), csub(x[0], x[2])
    c, d = cadd(x[1], x[3]), turn(csub(x[1], x[3]))
    return [cadd(a, c), cadd(b, d), csub(a, c), csub(b, d)]


def eight_point(x):
    even, odd = four_point(x[0::2]), four_point(x[1::2])
    r = math.sqrt(0.5)
    odd = [
        odd[0],
        ((odd[1][0] - odd[1][1]) * r, (odd[1][0] + odd[1][1]) * r),
        turn(odd[2]),
        ((-odd[3][0] - odd[3][1]) * r, (odd[3][0] - odd[3][1]) * r),
    ]
    return [cadd(e, o) for e, o in zip(even, odd)] + [csub(e, o) for e, o in zip(even, odd)]


def image_kernel(*refs):
    offset_ref = refs[0]
    (
        count_ref, vis_ref, weight_ref, kernel_ref, tile_ref, plane_ref, chan_ref,
        tap_ref, line_ref, twist_ref, screen_ref,
    ) = refs[13:24]
    fetches = [pltpu.make_async_copy(refs[1 + i], refs[13 + i], refs[-1].at[i]) for i in range(11)]
    for i in FETCH_ORDER:
        fetches[i].start()
    out_ref = refs[12]
    image_body(
        fetches, count_ref, offset_ref, vis_ref, weight_ref, kernel_ref, tile_ref, plane_ref, chan_ref,
        tap_ref, line_ref, twist_ref, screen_ref, out_ref, *refs[24:-1]
    )


START_X = (0.0, 0.8, 1.7, 1.8)
START_Z = (0, 1, 2, 3, 7, 4, 5, 6)
PLANE_ORDER = sorted(range(32), key=lambda t: START_X[t // 4 % 4] + START_X[t % 4] + 1.2 * (t // 16))
LINE_ORDER = tuple(z % 2 * 4 + z // 2 for z in START_Z)


def plane_peer(me, j):
    there = (me + j) % 32
    return there, {"chan_1": there // 16, "bl_0": there // 4 % 4, "bl_1": there % 4}


FETCH_ORDER = (7, 3, 0, 1, 2, 4, 5, 6, 8, 9, 10)


def image_body(
    fetches, count_ref, offset_ref, vis_ref, weight_ref, kernel_ref, tile_ref, plane_ref, chan_ref,
    tap_ref, line_ref, twist_ref, screen_ref, out_ref, updates, bank_of, lane_hot, grid, lines, screens, image,
    own, plane_in, plane_sum, line_in, moment_own, plane_send, plane_recv, line_send, line_recv,
):
    barrier = pltpu.get_barrier_semaphore()
    signal = functools.partial(pl.semaphore_signal, barrier, inc=1, device_id_type=MESH_ID)
    me = lax.axis_index("chan_1") * 16 + lax.axis_index("bl_0") * 4 + lax.axis_index("bl_1")
    for j in range(1, 32):
        signal(device_id=plane_peer(me, j)[1])
    deep = lax.axis_index("chan_0") * 4 + lax.axis_index("bl_2")
    for j in range(1, 8):
        there = (deep + j) % 8
        signal(device_id={"bl_2": there % 4, "chan_0": there // 4})

    for i in (7, 3):
        fetches[i].wait()
    for i in (0, 1, 2, 4, 5, 6):
        fetches[i].wait()
    count = jnp.broadcast_to(count_ref[0:1, 0:1], (1, CHUNK))
    offsets = [jnp.broadcast_to(offset_ref[0:1, c:c + 1], (1, CHUNK)) for c in range(16)]

    def one_chunk(step, sums):
        at = pl.ds(pl.multiple_of(step * CHUNK, CHUNK), CHUNK)
        chunk_kernel = kernel_ref[:, at]
        taps = jnp.dot(tap_ref[...], jnp.concatenate([chunk_kernel, chunk_kernel], axis=0), preferred_element_type=f32)
        slot = step * CHUNK + lax.broadcasted_iota(jnp.int32, (1, CHUNK), 1)
        weight = jnp.where(slot < count, weight_ref[:, at].astype(f32), 0.0)
        chan = chan_ref[:, at]
        coord = jnp.zeros((1, CHUNK), f32)
        for c in range(16):
            coord = jnp.where(chan == c, offsets[c], coord)
        tile = tile_ref[:, at]
        plane = plane_ref[:, at]
        direct = plane >= HALF_PLANES
        tile_v = tile & 511
        tile_v = jnp.where(direct, tile_v, 511 - tile_v)
        half = jnp.where(direct, plane - HALF_PLANES, HALF_PLANES - 1 - plane)
        across = lambda row: jnp.transpose(jnp.broadcast_to(row.astype(f32), (LANES, CHUNK)))
        bank_of[at, :] = across(half * 4 + (tile_v & 3)).astype(bf16)
        lane = lax.broadcasted_iota(jnp.int32, (CHUNK, LANES), 1).astype(f32)
        lane_hot[at, :] = jnp.where(across(tile_v >> 2) == lane, 1.0, 0.0).astype(bf16)
        weighted = weight * taps[128:129]
        new_sums = []
        power = weighted
        for m in range(MOMENTS):
            new_sums.append(sums[m] + power)
            power = power * coord
        vis = vis_ref[:, at].astype(f32)
        base = (weight * vis[0:1], weight * vis[1:2])
        row = lax.broadcasted_iota(jnp.int32, (STRIP, CHUNK), 0) - STRIP // 2
        phase = unit_circle(((tile >> 9) * row) & 511)
        turned = cmul(phase, base)
        mirror = jnp.where(direct, 1.0, -1.0)
        flipped = (turned[0] * mirror, turned[1] * mirror)
        direct_rows = jnp.broadcast_to(direct, (STRIP, CHUNK))
        coord_rows = jnp.broadcast_to(coord, (STRIP, CHUNK))
        parts = []
        for e in range(TILE):
            r = slice(e * STRIP, (e + 1) * STRIP)
            i = slice(64 + e * STRIP, 64 + (e + 1) * STRIP)
            tap_r, tap_i = taps[r], taps[i]
            parts.append(
                (turned[0] * tap_r - turned[1] * tap_i, flipped[0] * tap_i + flipped[1] * tap_r)
            )
        zero = jnp.zeros((STRIP, CHUNK), f32)
        for e in range(WIDE):
            there = parts[e] if e < TILE else (zero, zero)
            back = parts[TILE - e] if e > 0 else (zero, zero)
            both = jnp.concatenate(
                [jnp.where(direct_rows, there[0], back[0]), jnp.where(direct_rows, there[1], back[1])], axis=0
            )
            for k in range(TAYLOR):
                if k > 0:
                    both = both * jnp.concatenate([coord_rows, coord_rows], axis=0)
                high = both.astype(bf16)
                low = (both - high.astype(f32)).astype(bf16)
                first = 2 * k * SPAN + e * 16
                updates[first:first + 16, at] = high
                updates[first + SPAN:first + SPAN + 16, at] = low
        return tuple(new_sums)

    sums = lax.fori_loop(
        0, SLOTS // CHUNK, one_chunk, tuple(jnp.zeros((1, CHUNK), f32) for _ in range(MOMENTS)),
        unroll=True,
    )
    lane = lax.broadcasted_iota(jnp.int32, (STRIP, LANES), 1)
    moment_row = jnp.zeros((STRIP, LANES), f32)
    for m in range(MOMENTS):
        total = jnp.sum(sums[m], axis=1, keepdims=True)
        moment_row = jnp.where(lane == m, jnp.broadcast_to(total, (STRIP, LANES)), moment_row)
    moment_own[...] = moment_row

    def spread(k):
        for step in range(CELLS // CHUNK):
            banks = bank_of[...]
            halves = [
                jnp.where(banks == jnp.asarray(step * 2 + half, bf16), lane_hot[...], jnp.zeros((), bf16))
                for half in range(CHUNK // LANES)
            ]
            both = jnp.dot(
                updates[2 * SPAN * k:2 * SPAN * (k + 1)], jnp.concatenate(halves, axis=1), preferred_element_type=f32
            )
            grid[SPAN * k:SPAN * (k + 1), step * CHUNK:(step + 1) * CHUNK] = both[:SPAN] + both[SPAN:]

    for i in (8, 9, 10):
        fetches[i].wait()
    for b in range(BLOCKS):
        one = (screen_ref[0, b], screen_ref[1, b])
        two = cmul(one, one)
        for q in range(HALF_PLANES):
            screens[q, 0, b] = one[0]
            screens[q, 1, b] = one[1]
            if q < HALF_PLANES - 1:
                one = cmul(one, two)

    def piece(k, e, part, q, vb):
        first = ((k * WIDE + e) * 2 + part) * STRIP
        at = pl.ds(pl.multiple_of(q * 512 + vb * LANES, LANES), LANES)
        return grid[first:first + STRIP, at]

    def one_term(k):
        for q in range(HALF_PLANES):
            residues = []
            for vb in range(4):
                halves = []
                for part in range(2):
                    spill = piece(k, TILE, part, q, (vb - 1) % 4)
                    if vb == 0:
                        spill = pltpu.roll(spill, 1, 1)
                    column = [piece(k, 0, part, q, vb) + spill]
                    column += [piece(k, e, part, q, vb) for e in range(1, TILE)]
                    halves.append(jnp.concatenate(column, axis=0))
                residues.append(jnp.concatenate(halves, axis=1))
            whole = jnp.concatenate(residues, axis=0)
            high = whole.astype(bf16)
            low = (whole - high.astype(f32)).astype(bf16)
            lines[q] = (
                jnp.dot(high, line_ref[0:256], preferred_element_type=f32)
                + jnp.dot(low, line_ref[0:256], preferred_element_type=f32)
                + jnp.dot(high, line_ref[256:512], preferred_element_type=f32)
            )
        for q in range(HALF_PLANES):
            quarters = [[], [], [], []]
            for e in range(TILE):
                x = []
                for vb in range(4):
                    first = (vb * TILE + e) * STRIP
                    value = (lines[q, first:first + STRIP, 0:LANES], lines[q, first:first + STRIP, LANES:2 * LANES])
                    if vb > 0:
                        value = cmul(value, (twist_ref[vb:vb + 1], twist_ref[36 + vb:37 + vb]))
                    x.append(value)
                for mr, value in enumerate(four_point(x)):
                    if e > 0:
                        t = 4 + e * 4 + mr
                        value = cmul(value, (twist_ref[t:t + 1], twist_ref[36 + t:37 + t]))
                    quarters[mr].append(value)
            for mr in range(4):
                for mh, value in enumerate(eight_point(quarters[mr])):
                    b = 4 * mh + mr
                    add = value[0] * screens[q, 0, b] - value[1] * screens[q, 1, b]
                    if q < HALF_PLANES - 1:
                        image[b] = image[b] + add if q > 0 else add
                    else:
                        total = image[b] + add
                        first = b // 4 * 8 + b % 4
                        own[k, pl.ds(first, 4, stride=64), :] = total[0:4]
                        own[k, pl.ds(first + 4, 4, stride=64), :] = total[4:8]

    low_z = lax.axis_index("chan_0")
    core = lax.axis_index("chan_1")
    me = core * 16 + lax.axis_index("bl_0") * 4 + lax.axis_index("bl_1")
    deep = low_z * 4 + lax.axis_index("bl_2")

    def together(source, target, send, recv):
        return pltpu.make_async_remote_copy(
            src_ref=source, dst_ref=target, send_sem=send, recv_sem=recv,
            device_id={"chan_1": 1 - core}, device_id_type=MESH_ID,
        )

    def send_plane(k):
        for there in PLANE_ORDER:
            copy = pltpu.make_async_remote_copy(
                src_ref=own.at[k, there * 8:there * 8 + 8] if k < TAYLOR else moment_own,
                dst_ref=plane_in.at[k, (me - there) % 32], send_sem=plane_send.at[k], recv_sem=plane_recv.at[k],
                device_id={"chan_1": there // 16, "bl_0": there // 4 % 4, "bl_1": there % 4}, device_id_type=MESH_ID,
            )
            pl.when(me != there)(copy.start)

    for k in range(TAYLOR):
        spread(k)
        one_term(k)
        if k == 0:
            pl.semaphore_wait(barrier, 38)
            send_plane(TAYLOR)
        send_plane(k)

    for k in (TAYLOR, 0, 1, 2):
        total = own[k, pl.ds(pl.multiple_of(me * 8, 8), 8)] if k < TAYLOR else moment_own[...]
        together(plane_in.at[3, 1:32], plane_in.at[k, 1:32], plane_send.at[k], plane_recv.at[k]).wait()
        for j in range(1, 32):
            total = total + plane_in[k, j]
        for r in range(8):
            plane_sum[r, k:k + 1] = total[r:r + 1]

    for there in LINE_ORDER:
        copy = pltpu.make_async_remote_copy(
            src_ref=plane_sum.at[there], dst_ref=line_in.at[(deep - there) % 8], send_sem=line_send, recv_sem=line_recv,
            device_id={"bl_2": there % 4, "chan_0": there // 4}, device_id_type=MESH_ID,
        )
        pl.when(deep != there)(copy.start)
    total = plane_sum[deep]
    together(plane_sum.at[0:7], line_in.at[1:8], line_send, line_recv).wait()
    for j in range(1, 8):
        total = total + line_in[j]
    moments = [total[TAYLOR:TAYLOR + 1, m:m + 1] for m in range(MOMENTS)]
    images = [total[k:k + 1] for k in range(TAYLOR)]
    rows, determinant = solve_taylor(moments, images)
    for k in range(TAYLOR):
        out_ref[0, k:k + 1] = rows[k]
        out_ref[1, k:k + 1] = jnp.broadcast_to(determinant, (1, LANES))


def device_image(counts, offsets, vis, weight, kernel, tile, plane, chan):
    vmem = pl.BlockSpec(memory_space=pltpu.VMEM)
    dma = pltpu.SemaphoreType.DMA
    operands = (
        counts, vis, weight, kernel, tile, plane, chan,
        jnp.asarray(tap_table()), jnp.asarray(line_table()), jnp.asarray(twist_table()), jnp.asarray(screen_table()),
    )
    return pl.pallas_call(
        image_kernel,
        out_shape=jax.ShapeDtypeStruct((2, TAYLOR, LANES), f32),
        in_specs=[vmem] + [pl.BlockSpec(memory_space=pltpu.HBM)] * 11,
        out_specs=vmem,
        scratch_shapes=[pltpu.VMEM(a.shape, a.dtype) for a in operands] + [
            pltpu.VMEM((2 * ROWS, SLOTS), bf16),
            pltpu.VMEM((SLOTS, LANES), bf16),
            pltpu.VMEM((SLOTS, LANES), bf16),
            pltpu.VMEM((ROWS, CELLS), f32),
            pltpu.VMEM((HALF_PLANES, 256, 256), f32),
            pltpu.VMEM((HALF_PLANES, 2, BLOCKS, STRIP, LANES), f32),
            pltpu.VMEM((BLOCKS, STRIP, LANES), f32),
            pltpu.VMEM((TAYLOR, 256, LANES), f32),
            pltpu.VMEM((TAYLOR + 1, 32, 8, LANES), f32),
            pltpu.VMEM((8, 4, LANES), f32),
            pltpu.VMEM((8, 4, LANES), f32),
            pltpu.VMEM((8, LANES), f32),
            dma((4,)), dma((4,)), dma, dma, dma((11,)),
        ],
        compiler_params=pltpu.CompilerParams(
            vmem_limit_bytes=55220 * 1024, collective_id=0, has_side_effects=True
        ),
        name="strip_image",
    )(offsets, *operands)


def solve_taylor(moments, images):
    entry_00, entry_01, entry_02 = (moments[0], moments[1], moments[2])
    entry_11, entry_12, entry_22 = (moments[2], moments[3], moments[4])
    minor_00 = entry_11 * entry_22 - entry_12 * entry_12
    minor_01 = entry_02 * entry_12 - entry_01 * entry_22
    minor_02 = entry_01 * entry_12 - entry_02 * entry_11
    minor_11 = entry_00 * entry_22 - entry_02 * entry_02
    minor_12 = entry_01 * entry_02 - entry_00 * entry_12
    minor_22 = entry_00 * entry_11 - entry_01 * entry_01
    determinant = entry_00 * minor_00 + entry_01 * minor_01 + entry_02 * minor_02
    first = minor_00 * images[0] + minor_01 * images[1] + minor_02 * images[2]
    second = minor_01 * images[0] + minor_11 * images[1] + minor_12 * images[2]
    third = minor_02 * images[0] + minor_12 * images[1] + minor_22 * images[2]
    return (first, second, third), determinant


MESH_ID = pl.DeviceIdType.MESH


def body(vis_value, vis_weight, kernel, tile_index, plane_index, chan_index, chan_offset, counts):
    scaled = device_image(
        counts, chan_offset, vis_value[0, 0], vis_weight[0], kernel[0, 0],
        tile_index[0], plane_index[0], chan_index[0],
    )
    return scaled[0] / scaled[1]


def solution(mesh):
    split = Mesh(mesh.devices.reshape(2, 2, 4, 4, 4), ("chan_0", "chan_1", "bl_0", "bl_1", "bl_2"))
    return jax.shard_map(
        body,
        mesh=split,
        in_specs=(
            P(CHAN, BL, None, None),
            P(CHAN, BL, None),
            P(CHAN, BL, None, None),
            P(CHAN, BL, None),
            P(CHAN, BL, None),
            P(CHAN, BL, None),
            P(CHAN, None),
            P(CHAN, BL),
        ),
        out_specs=P(None, CHAN_BL),
        check_vma=False,
    )
```

```python
import functools
import math

import jax
import jax.numpy as jnp
import numpy as np
from jax import lax
from jax.experimental import pallas as pl
from jax.experimental.pallas import tpu as pltpu
from jax.sharding import Mesh
from jax.sharding import PartitionSpec as P

NPIX = 4096
TILE = 8
TAYLOR = 3
MOMENTS = 5
STRIP = 8
SLOTS = 2048
HALF_PLANES = 4
WIDE = TILE + 1
ROWS = TAYLOR * WIDE * 2 * STRIP
SPAN = WIDE * 2 * STRIP
CELLS = HALF_PLANES * NPIX // TILE
BLOCKS = 32
LANES = 128
CHUNK = 256
CHAN_BL = ("chan_0", "chan_1", "bl_0", "bl_1", "bl_2")
CHAN = ("chan_0", "chan_1")
BL = ("bl_0", "bl_1", "bl_2")
f32 = jnp.float32
bf16 = jnp.bfloat16


def split_pair(table):
    high = table.astype(np.float32).astype(bf16)
    low = (table - high.astype(np.float64)).astype(np.float32).astype(bf16)
    return high, low


def tap_table():
    a = np.arange(TILE)[None, :]
    l = np.arange(STRIP)[:, None] - STRIP // 2
    angle = 2.0 * math.pi * ((a - NPIX // 2) * l % NPIX) / NPIX
    table = np.zeros((2, TILE, STRIP, TILE, TILE))
    for e in range(TILE):
        table[0, e, :, :, e] = np.cos(angle)
        table[1, e, :, :, e] = np.sin(angle)
    high, low = split_pair(table.reshape(2 * TILE * STRIP, TILE * TILE))
    ones = np.zeros((16, 2 * TILE * TILE), np.float32)
    ones[0, :TILE * TILE] = 1.0
    return np.concatenate([np.concatenate([high, low], axis=1), ones.astype(bf16)], axis=0)


def line_table():
    n = np.arange(LANES)
    angle = 2.0 * math.pi * (n[:, None] * n[None, :] % LANES) / LANES
    sign = 1.0 - 2.0 * (n % 2)
    c, s = np.cos(angle) * sign, np.sin(angle) * sign
    return np.concatenate(split_pair(np.block([[c, s], [-s, c]])), axis=0)


def twist_table():
    mq = np.arange(LANES)
    rows = [2.0 * math.pi * 8 * vb * mq / NPIX for vb in range(4)]
    for e in range(TILE):
        for mr in range(4):
            rows.append(2.0 * math.pi * e * (mq + LANES * mr) / NPIX + math.pi * e)
    angle = np.stack(rows)
    return np.concatenate([np.cos(angle), np.sin(angle)], axis=0).astype(np.float32)


def screen_table():
    cell = 0.5 / NPIX
    l = np.arange(STRIP)[None, :, None] - STRIP // 2
    m = (np.arange(BLOCKS)[:, None, None] - BLOCKS // 2) * LANES + np.arange(LANES)[None, None, :]
    radius = (l * cell) ** 2 + (m * cell) ** 2
    s = -radius / (1.0 + np.sqrt(1.0 - radius))
    angle = 2.0 * math.pi * 20.0 * s
    return np.stack([np.cos(angle), np.sin(angle)]).astype(np.float32)


def unit_circle(index):
    quarter = ((index + 64) >> 7) & 3
    x = (((index + 64) & 127) - 64).astype(f32) * (2.0 * math.pi / 512.0)
    x2 = x * x
    s = x * (1.0 + x2 * (-1.0 / 6 + x2 * (1.0 / 120 + x2 * (-1.0 / 5040 + x2 * (1.0 / 362880)))))
    c = 1.0 + x2 * (-0.5 + x2 * (1.0 / 24 + x2 * (-1.0 / 720 + x2 * (1.0 / 40320))))
    odd = (quarter & 1) == 1
    cos = jnp.where(odd, s, c)
    sin = jnp.where(odd, c, s)
    cos = jnp.where((quarter == 1) | (quarter == 2), -cos, cos)
    sin = jnp.where(quarter >= 2, -sin, sin)
    return cos, sin


def cmul(a, b):
    return a[0] * b[0] - a[1] * b[1], a[0] * b[1] + a[1] * b[0]


def cadd(a, b):
    return a[0] + b[0], a[1] + b[1]


def csub(a, b):
    return a[0] - b[0], a[1] - b[1]


def turn(a):
    return -a[1], a[0]


def four_point(x):
    a, b = cadd(x[0], x[2]), csub(x[0], x[2])
    c, d = cadd(x[1], x[3]), turn(csub(x[1], x[3]))
    return [cadd(a, c), cadd(b, d), csub(a, c), csub(b, d)]


def eight_point(x):
    even, odd = four_point(x[0::2]), four_point(x[1::2])
    r = math.sqrt(0.5)
    odd = [
        odd[0],
        ((odd[1][0] - odd[1][1]) * r, (odd[1][0] + odd[1][1]) * r),
        turn(odd[2]),
        ((-odd[3][0] - odd[3][1]) * r, (odd[3][0] - odd[3][1]) * r),
    ]
    return [cadd(e, o) for e, o in zip(even, odd)] + [csub(e, o) for e, o in zip(even, odd)]


def image_kernel(*refs):
    offset_ref = refs[0]
    (
        count_ref, vis_ref, weight_ref, kernel_ref, tile_ref, plane_ref, chan_ref,
        tap_ref, line_ref, twist_ref, screen_ref,
    ) = refs[13:24]
    fetches = [pltpu.make_async_copy(refs[1 + i], refs[13 + i], refs[-1].at[i]) for i in range(11)]
    for i in FETCH_ORDER:
        fetches[i].start()
    out_ref = refs[12]
    image_body(
        fetches, count_ref, offset_ref, vis_ref, weight_ref, kernel_ref, tile_ref, plane_ref, chan_ref,
        tap_ref, line_ref, twist_ref, screen_ref, out_ref, *refs[24:-1]
    )


START_X = (0.0, 0.8, 1.7, 1.8)
START_Z = (0, 1, 2, 3, 7, 4, 5, 6)
PLANE_ORDER = sorted(range(32), key=lambda t: START_X[t // 4 % 4] + START_X[t % 4] + 1.2 * (t // 16))
LINE_ORDER = tuple(z % 2 * 4 + z // 2 for z in START_Z)


def plane_peer(me, j):
    there = (me + j) % 32
    return there, {"chan_1": there // 16, "bl_0": there // 4 % 4, "bl_1": there % 4}


FETCH_ORDER = (7, 3, 0, 1, 2, 4, 5, 6, 8, 9, 10)


def image_body(
    fetches, count_ref, offset_ref, vis_ref, weight_ref, kernel_ref, tile_ref, plane_ref, chan_ref,
    tap_ref, line_ref, twist_ref, screen_ref, out_ref, updates, bank_of, lane_hot, hot, grid, lines, screens, image,
    own, plane_in, plane_sum, line_in, moment_own, plane_send, plane_recv, line_send, line_recv,
):
    barrier = pltpu.get_barrier_semaphore()
    signal = functools.partial(pl.semaphore_signal, barrier, inc=1, device_id_type=MESH_ID)
    me = lax.axis_index("chan_1") * 16 + lax.axis_index("bl_0") * 4 + lax.axis_index("bl_1")
    for j in range(1, 32):
        signal(device_id=plane_peer(me, j)[1])
    deep = lax.axis_index("chan_0") * 4 + lax.axis_index("bl_2")
    for j in range(1, 8):
        there = (deep + j) % 8
        signal(device_id={"bl_2": there % 4, "chan_0": there // 4})

    for i in (7, 3):
        fetches[i].wait()
    for i in (0, 1, 2, 4, 5, 6):
        fetches[i].wait()
    count = jnp.broadcast_to(count_ref[0:1, 0:1], (1, CHUNK))
    offsets = [jnp.broadcast_to(offset_ref[0:1, c:c + 1], (1, CHUNK)) for c in range(16)]

    def one_chunk(step, sums):
        at = pl.ds(pl.multiple_of(step * CHUNK, CHUNK), CHUNK)
        chunk_kernel = kernel_ref[:, at]
        taps = jnp.dot(tap_ref[...], jnp.concatenate([chunk_kernel, chunk_kernel], axis=0), preferred_element_type=f32)
        slot = step * CHUNK + lax.broadcasted_iota(jnp.int32, (1, CHUNK), 1)
        weight = jnp.where(slot < count, weight_ref[:, at].astype(f32), 0.0)
        chan = chan_ref[:, at]
        coord = jnp.zeros((1, CHUNK), f32)
        for c in range(16):
            coord = jnp.where(chan == c, offsets[c], coord)
        tile = tile_ref[:, at]
        plane = plane_ref[:, at]
        direct = plane >= HALF_PLANES
        tile_v = tile & 511
        tile_v = jnp.where(direct, tile_v, 511 - tile_v)
        half = jnp.where(direct, plane - HALF_PLANES, HALF_PLANES - 1 - plane)
        across = lambda row: jnp.transpose(jnp.broadcast_to(row.astype(f32), (LANES, CHUNK)))
        bank_of[at, :] = across(half * 4 + (tile_v & 3)).astype(bf16)
        lane = lax.broadcasted_iota(jnp.int32, (CHUNK, LANES), 1).astype(f32)
        lane_hot[at, :] = jnp.where(across(tile_v >> 2) == lane, 1.0, 0.0).astype(bf16)
        weighted = weight * taps[128:129]
        new_sums = []
        power = weighted
        for m in range(MOMENTS):
            new_sums.append(sums[m] + power)
            power = power * coord
        vis = vis_ref[:, at].astype(f32)
        base = (weight * vis[0:1], weight * vis[1:2])
        row = lax.broadcasted_iota(jnp.int32, (STRIP, CHUNK), 0) - STRIP // 2
        phase = unit_circle(((tile >> 9) * row) & 511)
        turned = cmul(phase, base)
        mirror = jnp.where(direct, 1.0, -1.0)
        flipped = (turned[0] * mirror, turned[1] * mirror)
        direct_rows = jnp.broadcast_to(direct, (STRIP, CHUNK))
        coord_rows = jnp.broadcast_to(coord, (STRIP, CHUNK))
        parts = []
        for e in range(TILE):
            r = slice(e * STRIP, (e + 1) * STRIP)
            i = slice(64 + e * STRIP, 64 + (e + 1) * STRIP)
            tap_r, tap_i = taps[r], taps[i]
            parts.append(
                (turned[0] * tap_r - turned[1] * tap_i, flipped[0] * tap_i + flipped[1] * tap_r)
            )
        zero = jnp.zeros((STRIP, CHUNK), f32)
        for e in range(WIDE):
            there = parts[e] if e < TILE else (zero, zero)
            back = parts[TILE - e] if e > 0 else (zero, zero)
            both = jnp.concatenate(
                [jnp.where(direct_rows, there[0], back[0]), jnp.where(direct_rows, there[1], back[1])], axis=0
            )
            for k in range(TAYLOR):
                if k > 0:
                    both = both * jnp.concatenate([coord_rows, coord_rows], axis=0)
                high = both.astype(bf16)
                low = (both - high.astype(f32)).astype(bf16)
                first = 2 * k * SPAN + e * 16
                updates[first:first + 16, at] = high
                updates[first + SPAN:first + SPAN + 16, at] = low
        return tuple(new_sums)

    sums = lax.fori_loop(
        0, SLOTS // CHUNK, one_chunk, tuple(jnp.zeros((1, CHUNK), f32) for _ in range(MOMENTS)),
        unroll=True,
    )
    lane = lax.broadcasted_iota(jnp.int32, (STRIP, LANES), 1)
    moment_row = jnp.zeros((STRIP, LANES), f32)
    for m in range(MOMENTS):
        total = jnp.sum(sums[m], axis=1, keepdims=True)
        moment_row = jnp.where(lane == m, jnp.broadcast_to(total, (STRIP, LANES)), moment_row)
    moment_own[...] = moment_row

    def spread(k):
        for step in range(CELLS // CHUNK):
            if k == 0:
                banks = bank_of[...]
                halves = [
                    jnp.where(banks == jnp.asarray(step * 2 + half, bf16), lane_hot[...], jnp.zeros((), bf16))
                    for half in range(CHUNK // LANES)
                ]
                one_hot = jnp.concatenate(halves, axis=1)
                hot[step] = one_hot
            else:
                one_hot = hot[step]
            both = jnp.dot(updates[2 * SPAN * k:2 * SPAN * (k + 1)], one_hot, preferred_element_type=f32)
            grid[SPAN * k:SPAN * (k + 1), step * CHUNK:(step + 1) * CHUNK] = both[:SPAN] + both[SPAN:]

    def tables():
        for i in (8, 9, 10):
            fetches[i].wait()
        for b in range(BLOCKS):
            one = (screen_ref[0, b], screen_ref[1, b])
            two = cmul(one, one)
            for q in range(HALF_PLANES):
                screens[q, 0, b] = one[0]
                screens[q, 1, b] = one[1]
                if q < HALF_PLANES - 1:
                    one = cmul(one, two)

    def piece(k, e, part, q, vb):
        first = ((k * WIDE + e) * 2 + part) * STRIP
        at = pl.ds(pl.multiple_of(q * 512 + vb * LANES, LANES), LANES)
        return grid[first:first + STRIP, at]

    def one_term(k):
        for q in range(HALF_PLANES):
            residues = []
            for vb in range(4):
                halves = []
                for part in range(2):
                    spill = piece(k, TILE, part, q, (vb - 1) % 4)
                    if vb == 0:
                        spill = pltpu.roll(spill, 1, 1)
                    column = [piece(k, 0, part, q, vb) + spill]
                    column += [piece(k, e, part, q, vb) for e in range(1, TILE)]
                    halves.append(jnp.concatenate(column, axis=0))
                residues.append(jnp.concatenate(halves, axis=1))
            whole = jnp.concatenate(residues, axis=0)
            high = whole.astype(bf16)
            low = (whole - high.astype(f32)).astype(bf16)
            lines[q] = (
                jnp.dot(high, line_ref[0:256], preferred_element_type=f32)
                + jnp.dot(low, line_ref[0:256], preferred_element_type=f32)
                + jnp.dot(high, line_ref[256:512], preferred_element_type=f32)
            )
        for q in range(HALF_PLANES):
            quarters = [[], [], [], []]
            for e in range(TILE):
                x = []
                for vb in range(4):
                    first = (vb * TILE + e) * STRIP
                    value = (lines[q, first:first + STRIP, 0:LANES], lines[q, first:first + STRIP, LANES:2 * LANES])
                    if vb > 0:
                        value = cmul(value, (twist_ref[vb:vb + 1], twist_ref[36 + vb:37 + vb]))
                    x.append(value)
                for mr, value in enumerate(four_point(x)):
                    if e > 0:
                        t = 4 + e * 4 + mr
                        value = cmul(value, (twist_ref[t:t + 1], twist_ref[36 + t:37 + t]))
                    quarters[mr].append(value)
            for mr in range(4):
                for mh, value in enumerate(eight_point(quarters[mr])):
                    b = 4 * mh + mr
                    add = value[0] * screens[q, 0, b] - value[1] * screens[q, 1, b]
                    if q < HALF_PLANES - 1:
                        image[b] = image[b] + add if q > 0 else add
                    else:
                        total = image[b] + add
                        first = b // 4 * 8 + b % 4
                        own[k, pl.ds(first, 4, stride=64), :] = total[0:4]
                        own[k, pl.ds(first + 4, 4, stride=64), :] = total[4:8]

    low_z = lax.axis_index("chan_0")
    core = lax.axis_index("chan_1")
    me = core * 16 + lax.axis_index("bl_0") * 4 + lax.axis_index("bl_1")
    deep = low_z * 4 + lax.axis_index("bl_2")

    def together(source, target, send, recv):
        return pltpu.make_async_remote_copy(
            src_ref=source, dst_ref=target, send_sem=send, recv_sem=recv,
            device_id={"chan_1": 1 - core}, device_id_type=MESH_ID,
        )

    def send_plane(k):
        for there in PLANE_ORDER:
            copy = pltpu.make_async_remote_copy(
                src_ref=own.at[k, there * 8:there * 8 + 8] if k < TAYLOR else moment_own,
                dst_ref=plane_in.at[k, (me - there) % 32], send_sem=plane_send.at[k], recv_sem=plane_recv.at[k],
                device_id={"chan_1": there // 16, "bl_0": there // 4 % 4, "bl_1": there % 4}, device_id_type=MESH_ID,
            )
            pl.when(me != there)(copy.start)

    for k in range(TAYLOR):
        spread(k)
        if k == 0:
            tables()
        one_term(k)
        if k == 0:
            pl.semaphore_wait(barrier, 38)
            send_plane(TAYLOR)
        send_plane(k)

    for k in (TAYLOR, 0, 1, 2):
        total = own[k, pl.ds(pl.multiple_of(me * 8, 8), 8)] if k < TAYLOR else moment_own[...]
        together(plane_in.at[3, 1:32], plane_in.at[k, 1:32], plane_send.at[k], plane_recv.at[k]).wait()
        for j in range(1, 32):
            total = total + plane_in[k, j]
        for r in range(8):
            plane_sum[r, k:k + 1] = total[r:r + 1]

    for there in LINE_ORDER:
        copy = pltpu.make_async_remote_copy(
            src_ref=plane_sum.at[there], dst_ref=line_in.at[(deep - there) % 8], send_sem=line_send, recv_sem=line_recv,
            device_id={"bl_2": there % 4, "chan_0": there // 4}, device_id_type=MESH_ID,
        )
        pl.when(deep != there)(copy.start)
    total = plane_sum[deep]
    together(plane_sum.at[0:7], line_in.at[1:8], line_send, line_recv).wait()
    for j in range(1, 8):
        total = total + line_in[j]
    moments = [total[TAYLOR:TAYLOR + 1, m:m + 1] for m in range(MOMENTS)]
    images = [total[k:k + 1] for k in range(TAYLOR)]
    rows, determinant = solve_taylor(moments, images)
    for k in range(TAYLOR):
        out_ref[0, k:k + 1] = rows[k]
        out_ref[1, k:k + 1] = jnp.broadcast_to(determinant, (1, LANES))


def device_image(counts, offsets, vis, weight, kernel, tile, plane, chan):
    vmem = pl.BlockSpec(memory_space=pltpu.VMEM)
    dma = pltpu.SemaphoreType.DMA
    operands = (
        counts, vis, weight, kernel, tile, plane, chan,
        jnp.asarray(tap_table()), jnp.asarray(line_table()), jnp.asarray(twist_table()), jnp.asarray(screen_table()),
    )
    return pl.pallas_call(
        image_kernel,
        out_shape=jax.ShapeDtypeStruct((2, TAYLOR, LANES), f32),
        in_specs=[vmem] + [pl.BlockSpec(memory_space=pltpu.HBM)] * 11,
        out_specs=vmem,
        scratch_shapes=[pltpu.VMEM(a.shape, a.dtype) for a in operands] + [
            pltpu.VMEM((2 * ROWS, SLOTS), bf16),
            pltpu.VMEM((SLOTS, LANES), bf16),
            pltpu.VMEM((SLOTS, LANES), bf16),
            pltpu.VMEM((CELLS // CHUNK, SLOTS, CHUNK), bf16),
            pltpu.VMEM((ROWS, CELLS), f32),
            pltpu.VMEM((HALF_PLANES, 256, 256), f32),
            pltpu.VMEM((HALF_PLANES, 2, BLOCKS, STRIP, LANES), f32),
            pltpu.VMEM((BLOCKS, STRIP, LANES), f32),
            pltpu.VMEM((TAYLOR, 256, LANES), f32),
            pltpu.VMEM((TAYLOR + 1, 32, 8, LANES), f32),
            pltpu.VMEM((8, 4, LANES), f32),
            pltpu.VMEM((8, 4, LANES), f32),
            pltpu.VMEM((8, LANES), f32),
            dma((4,)), dma((4,)), dma, dma, dma((11,)),
        ],
        compiler_params=pltpu.CompilerParams(
            vmem_limit_bytes=55220 * 1024, collective_id=0, has_side_effects=True
        ),
        name="strip_image",
    )(offsets, *operands)


def solve_taylor(moments, images):
    entry_00, entry_01, entry_02 = (moments[0], moments[1], moments[2])
    entry_11, entry_12, entry_22 = (moments[2], moments[3], moments[4])
    minor_00 = entry_11 * entry_22 - entry_12 * entry_12
    minor_01 = entry_02 * entry_12 - entry_01 * entry_22
    minor_02 = entry_01 * entry_12 - entry_02 * entry_11
    minor_11 = entry_00 * entry_22 - entry_02 * entry_02
    minor_12 = entry_01 * entry_02 - entry_00 * entry_12
    minor_22 = entry_00 * entry_11 - entry_01 * entry_01
    determinant = entry_00 * minor_00 + entry_01 * minor_01 + entry_02 * minor_02
    first = minor_00 * images[0] + minor_01 * images[1] + minor_02 * images[2]
    second = minor_01 * images[0] + minor_11 * images[1] + minor_12 * images[2]
    third = minor_02 * images[0] + minor_12 * images[1] + minor_22 * images[2]
    return (first, second, third), determinant


MESH_ID = pl.DeviceIdType.MESH


def body(vis_value, vis_weight, kernel, tile_index, plane_index, chan_index, chan_offset, counts):
    scaled = device_image(
        counts, chan_offset, vis_value[0, 0], vis_weight[0], kernel[0, 0],
        tile_index[0], plane_index[0], chan_index[0],
    )
    return scaled[0] / scaled[1]


def solution(mesh):
    split = Mesh(mesh.devices.reshape(2, 2, 4, 4, 4), ("chan_0", "chan_1", "bl_0", "bl_1", "bl_2"))
    return jax.shard_map(
        body,
        mesh=split,
        in_specs=(
            P(CHAN, BL, None, None),
            P(CHAN, BL, None),
            P(CHAN, BL, None, None),
            P(CHAN, BL, None),
            P(CHAN, BL, None),
            P(CHAN, BL, None),
            P(CHAN, None),
            P(CHAN, BL),
        ),
        out_specs=P(None, CHAN_BL),
        check_vma=False,
    )
```

```python
import functools
import math

import jax
import jax.numpy as jnp
import numpy as np
from jax import lax
from jax.experimental import pallas as pl
from jax.experimental.pallas import tpu as pltpu
from jax.sharding import Mesh
from jax.sharding import PartitionSpec as P

NPIX = 4096
TILE = 8
TAYLOR = 3
MOMENTS = 5
STRIP = 8
SLOTS = 2048
HALF_PLANES = 4
WIDE = TILE + 1
ROWS = TAYLOR * WIDE * 2 * STRIP
SPAN = WIDE * 2 * STRIP
CELLS = HALF_PLANES * NPIX // TILE
BLOCKS = 32
LANES = 128
CHUNK = 256
CHAN_BL = ("chan_0", "chan_1", "bl_0", "bl_1", "bl_2")
CHAN = ("chan_0", "chan_1")
BL = ("bl_0", "bl_1", "bl_2")
f32 = jnp.float32
bf16 = jnp.bfloat16


def split_pair(table):
    high = table.astype(np.float32).astype(bf16)
    low = (table - high.astype(np.float64)).astype(np.float32).astype(bf16)
    return high, low


def tap_table():
    a = np.arange(TILE)[None, :]
    l = np.arange(STRIP)[:, None] - STRIP // 2
    angle = 2.0 * math.pi * ((a - NPIX // 2) * l % NPIX) / NPIX
    table = np.zeros((2, TILE, STRIP, TILE, TILE))
    for e in range(TILE):
        table[0, e, :, :, e] = np.cos(angle)
        table[1, e, :, :, e] = np.sin(angle)
    high, low = split_pair(table.reshape(2 * TILE * STRIP, TILE * TILE))
    ones = np.zeros((16, 2 * TILE * TILE), np.float32)
    ones[0, :TILE * TILE] = 1.0
    return np.concatenate([np.concatenate([high, low], axis=1), ones.astype(bf16)], axis=0)


def line_table():
    n = np.arange(LANES)
    angle = 2.0 * math.pi * (n[:, None] * n[None, :] % LANES) / LANES
    sign = 1.0 - 2.0 * (n % 2)
    c, s = np.cos(angle) * sign, np.sin(angle) * sign
    return np.concatenate(split_pair(np.block([[c, s], [-s, c]])), axis=0)


def twist_table():
    mq = np.arange(LANES)
    rows = [2.0 * math.pi * 8 * vb * mq / NPIX for vb in range(4)]
    for e in range(TILE):
        for mr in range(4):
            rows.append(2.0 * math.pi * e * (mq + LANES * mr) / NPIX + math.pi * e)
    angle = np.stack(rows)
    return np.concatenate([np.cos(angle), np.sin(angle)], axis=0).astype(np.float32)


def screen_table():
    cell = 0.5 / NPIX
    l = np.arange(STRIP)[None, :, None] - STRIP // 2
    m = (np.arange(BLOCKS)[:, None, None] - BLOCKS // 2) * LANES + np.arange(LANES)[None, None, :]
    radius = (l * cell) ** 2 + (m * cell) ** 2
    s = -radius / (1.0 + np.sqrt(1.0 - radius))
    angle = 2.0 * math.pi * 20.0 * s
    return np.stack([np.cos(angle), np.sin(angle)]).astype(np.float32)


def unit_circle(index):
    quarter = ((index + 64) >> 7) & 3
    x = (((index + 64) & 127) - 64).astype(f32) * (2.0 * math.pi / 512.0)
    x2 = x * x
    s = x * (1.0 + x2 * (-1.0 / 6 + x2 * (1.0 / 120 + x2 * (-1.0 / 5040 + x2 * (1.0 / 362880)))))
    c = 1.0 + x2 * (-0.5 + x2 * (1.0 / 24 + x2 * (-1.0 / 720 + x2 * (1.0 / 40320))))
    odd = (quarter & 1) == 1
    cos = jnp.where(odd, s, c)
    sin = jnp.where(odd, c, s)
    cos = jnp.where((quarter == 1) | (quarter == 2), -cos, cos)
    sin = jnp.where(quarter >= 2, -sin, sin)
    return cos, sin


def cmul(a, b):
    return a[0] * b[0] - a[1] * b[1], a[0] * b[1] + a[1] * b[0]


def cadd(a, b):
    return a[0] + b[0], a[1] + b[1]


def csub(a, b):
    return a[0] - b[0], a[1] - b[1]


def turn(a):
    return -a[1], a[0]


def four_point(x):
    a, b = cadd(x[0], x[2]), csub(x[0], x[2])
    c, d = cadd(x[1], x[3]), turn(csub(x[1], x[3]))
    return [cadd(a, c), cadd(b, d), csub(a, c), csub(b, d)]


def eight_point(x):
    even, odd = four_point(x[0::2]), four_point(x[1::2])
    r = math.sqrt(0.5)
    odd = [
        odd[0],
        ((odd[1][0] - odd[1][1]) * r, (odd[1][0] + odd[1][1]) * r),
        turn(odd[2]),
        ((-odd[3][0] - odd[3][1]) * r, (odd[3][0] - odd[3][1]) * r),
    ]
    return [cadd(e, o) for e, o in zip(even, odd)] + [csub(e, o) for e, o in zip(even, odd)]


def image_kernel(*refs):
    offset_ref = refs[0]
    (
        count_ref, vis_ref, weight_ref, kernel_ref, tile_ref, plane_ref, chan_ref,
        tap_ref, line_ref, twist_ref, screen_ref,
    ) = refs[13:24]
    fetches = [pltpu.make_async_copy(refs[1 + i], refs[13 + i], refs[-1].at[i]) for i in range(11)]
    for i in FETCH_ORDER:
        fetches[i].start()
    out_ref = refs[12]
    image_body(
        fetches, count_ref, offset_ref, vis_ref, weight_ref, kernel_ref, tile_ref, plane_ref, chan_ref,
        tap_ref, line_ref, twist_ref, screen_ref, out_ref, *refs[24:-1]
    )


START_X = (0.0, 0.8, 1.7, 1.8)
START_Z = (0, 1, 2, 3, 7, 4, 5, 6)
PLANE_ORDER = sorted(range(32), key=lambda t: START_X[t // 4 % 4] + START_X[t % 4] + 1.2 * (t // 16))
LINE_ORDER = tuple(z % 2 * 4 + z // 2 for z in START_Z)


def plane_peer(me, j):
    there = (me + j) % 32
    return there, {"chan_1": there // 16, "bl_0": there // 4 % 4, "bl_1": there % 4}


FETCH_ORDER = (7, 3, 0, 1, 2, 4, 5, 6, 8, 9, 10)


def image_body(
    fetches, count_ref, offset_ref, vis_ref, weight_ref, kernel_ref, tile_ref, plane_ref, chan_ref,
    tap_ref, line_ref, twist_ref, screen_ref, out_ref, updates, bank_of, lane_hot, hot, grid, lines, screens, image,
    own, plane_in, plane_sum, line_in, moment_own, plane_send, plane_recv, line_send, line_recv,
):
    barrier = pltpu.get_barrier_semaphore()
    signal = functools.partial(pl.semaphore_signal, barrier, inc=1, device_id_type=MESH_ID)
    me = lax.axis_index("chan_1") * 16 + lax.axis_index("bl_0") * 4 + lax.axis_index("bl_1")
    for j in range(1, 32):
        signal(device_id=plane_peer(me, j)[1])
    deep = lax.axis_index("chan_0") * 4 + lax.axis_index("bl_2")
    for j in range(1, 8):
        there = (deep + j) % 8
        signal(device_id={"bl_2": there % 4, "chan_0": there // 4})

    for i in (7, 3):
        fetches[i].wait()
    for i in (0, 1, 2, 4, 5, 6):
        fetches[i].wait()
    count = jnp.broadcast_to(count_ref[0:1, 0:1], (1, CHUNK))
    offsets = [jnp.broadcast_to(offset_ref[0:1, c:c + 1], (1, CHUNK)) for c in range(16)]

    def one_chunk(step, sums):
        at = pl.ds(pl.multiple_of(step * CHUNK, CHUNK), CHUNK)
        chunk_kernel = kernel_ref[:, at]
        taps = jnp.dot(tap_ref[...], jnp.concatenate([chunk_kernel, chunk_kernel], axis=0), preferred_element_type=f32)
        slot = step * CHUNK + lax.broadcasted_iota(jnp.int32, (1, CHUNK), 1)
        weight = jnp.where(slot < count, weight_ref[:, at].astype(f32), 0.0)
        chan = chan_ref[:, at]
        coord = jnp.zeros((1, CHUNK), f32)
        for c in range(16):
            coord = jnp.where(chan == c, offsets[c], coord)
        tile = tile_ref[:, at]
        plane = plane_ref[:, at]
        direct = plane >= HALF_PLANES
        tile_v = tile & 511
        tile_v = jnp.where(direct, tile_v, 511 - tile_v)
        half = jnp.where(direct, plane - HALF_PLANES, HALF_PLANES - 1 - plane)
        across = lambda row: jnp.transpose(jnp.broadcast_to(row.astype(f32), (LANES, CHUNK)))
        bank_of[at, :] = across(half * 4 + (tile_v & 3)).astype(bf16)
        lane = lax.broadcasted_iota(jnp.int32, (CHUNK, LANES), 1).astype(f32)
        lane_hot[at, :] = jnp.where(across(tile_v >> 2) == lane, 1.0, 0.0).astype(bf16)
        weighted = weight * taps[128:129]
        new_sums = []
        power = weighted
        for m in range(MOMENTS):
            new_sums.append(sums[m] + power)
            power = power * coord
        vis = vis_ref[:, at].astype(f32)
        base = (weight * vis[0:1], weight * vis[1:2])
        row = lax.broadcasted_iota(jnp.int32, (STRIP, CHUNK), 0) - STRIP // 2
        phase = unit_circle(((tile >> 9) * row) & 511)
        turned = cmul(phase, base)
        mirror = jnp.where(direct, 1.0, -1.0)
        flipped = (turned[0] * mirror, turned[1] * mirror)
        direct_rows = jnp.broadcast_to(direct, (STRIP, CHUNK))
        coord_rows = jnp.broadcast_to(coord, (STRIP, CHUNK))
        parts = []
        for e in range(TILE):
            r = slice(e * STRIP, (e + 1) * STRIP)
            i = slice(64 + e * STRIP, 64 + (e + 1) * STRIP)
            tap_r, tap_i = taps[r], taps[i]
            parts.append(
                (turned[0] * tap_r - turned[1] * tap_i, flipped[0] * tap_i + flipped[1] * tap_r)
            )
        zero = jnp.zeros((STRIP, CHUNK), f32)
        for e in range(WIDE):
            there = parts[e] if e < TILE else (zero, zero)
            back = parts[TILE - e] if e > 0 else (zero, zero)
            both = jnp.concatenate(
                [jnp.where(direct_rows, there[0], back[0]), jnp.where(direct_rows, there[1], back[1])], axis=0
            )
            for k in range(TAYLOR):
                if k > 0:
                    both = both * jnp.concatenate([coord_rows, coord_rows], axis=0)
                high = both.astype(bf16)
                low = (both - high.astype(f32)).astype(bf16)
                first = 2 * k * SPAN + e * 16
                updates[first:first + 16, at] = high
                updates[first + SPAN:first + SPAN + 16, at] = low
        return tuple(new_sums)

    sums = lax.fori_loop(
        0, SLOTS // CHUNK, one_chunk, tuple(jnp.zeros((1, CHUNK), f32) for _ in range(MOMENTS)),
        unroll=True,
    )
    lane = lax.broadcasted_iota(jnp.int32, (STRIP, LANES), 1)
    moment_row = jnp.zeros((STRIP, LANES), f32)
    for m in range(MOMENTS):
        total = jnp.sum(sums[m], axis=1, keepdims=True)
        moment_row = jnp.where(lane == m, jnp.broadcast_to(total, (STRIP, LANES)), moment_row)
    moment_own[...] = moment_row

    def spread(k):
        for step in range(CELLS // CHUNK):
            if k == 0:
                banks = bank_of[...]
                halves = [
                    jnp.where(banks == jnp.asarray(step * 2 + half, bf16), lane_hot[...], jnp.zeros((), bf16))
                    for half in range(CHUNK // LANES)
                ]
                one_hot = jnp.concatenate(halves, axis=1)
                hot[step] = one_hot
            else:
                one_hot = hot[step]
            both = jnp.dot(updates[2 * SPAN * k:2 * SPAN * (k + 1)], one_hot, preferred_element_type=f32)
            grid[SPAN * k:SPAN * (k + 1), step * CHUNK:(step + 1) * CHUNK] = both[:SPAN] + both[SPAN:]

    for i in (8, 9, 10):
        fetches[i].wait()
    for b in range(BLOCKS):
        one = (screen_ref[0, b], screen_ref[1, b])
        two = cmul(one, one)
        for q in range(HALF_PLANES):
            screens[q, 0, b] = one[0]
            screens[q, 1, b] = one[1]
            if q < HALF_PLANES - 1:
                one = cmul(one, two)

    def piece(k, e, part, q, vb):
        first = ((k * WIDE + e) * 2 + part) * STRIP
        at = pl.ds(pl.multiple_of(q * 512 + vb * LANES, LANES), LANES)
        return grid[first:first + STRIP, at]

    def one_term(k):
        for q in range(HALF_PLANES):
            residues = []
            for vb in range(4):
                halves = []
                for part in range(2):
                    spill = piece(k, TILE, part, q, (vb - 1) % 4)
                    if vb == 0:
                        spill = pltpu.roll(spill, 1, 1)
                    column = [piece(k, 0, part, q, vb) + spill]
                    column += [piece(k, e, part, q, vb) for e in range(1, TILE)]
                    halves.append(jnp.concatenate(column, axis=0))
                residues.append(jnp.concatenate(halves, axis=1))
            whole = jnp.concatenate(residues, axis=0)
            high = whole.astype(bf16)
            low = (whole - high.astype(f32)).astype(bf16)
            lines[q] = (
                jnp.dot(high, line_ref[0:256], preferred_element_type=f32)
                + jnp.dot(low, line_ref[0:256], preferred_element_type=f32)
                + jnp.dot(high, line_ref[256:512], preferred_element_type=f32)
            )
        for q in range(HALF_PLANES):
            quarters = [[], [], [], []]
            for e in range(TILE):
                x = []
                for vb in range(4):
                    first = (vb * TILE + e) * STRIP
                    value = (lines[q, first:first + STRIP, 0:LANES], lines[q, first:first + STRIP, LANES:2 * LANES])
                    if vb > 0:
                        value = cmul(value, (twist_ref[vb:vb + 1], twist_ref[36 + vb:37 + vb]))
                    x.append(value)
                for mr, value in enumerate(four_point(x)):
                    if e > 0:
                        t = 4 + e * 4 + mr
                        value = cmul(value, (twist_ref[t:t + 1], twist_ref[36 + t:37 + t]))
                    quarters[mr].append(value)
            for mr in range(4):
                for mh, value in enumerate(eight_point(quarters[mr])):
                    b = 4 * mh + mr
                    add = value[0] * screens[q, 0, b] - value[1] * screens[q, 1, b]
                    if q < HALF_PLANES - 1:
                        image[b] = image[b] + add if q > 0 else add
                    else:
                        total = image[b] + add
                        first = b // 4 * 8 + b % 4
                        own[k, pl.ds(first, 4, stride=64), :] = total[0:4]
                        own[k, pl.ds(first + 4, 4, stride=64), :] = total[4:8]

    low_z = lax.axis_index("chan_0")
    core = lax.axis_index("chan_1")
    me = core * 16 + lax.axis_index("bl_0") * 4 + lax.axis_index("bl_1")
    deep = low_z * 4 + lax.axis_index("bl_2")

    def together(source, target, send, recv):
        return pltpu.make_async_remote_copy(
            src_ref=source, dst_ref=target, send_sem=send, recv_sem=recv,
            device_id={"chan_1": 1 - core}, device_id_type=MESH_ID,
        )

    def send_plane(k):
        for there in PLANE_ORDER:
            copy = pltpu.make_async_remote_copy(
                src_ref=own.at[k, there * 8:there * 8 + 8] if k < TAYLOR else moment_own,
                dst_ref=plane_in.at[k, (me - there) % 32], send_sem=plane_send.at[k], recv_sem=plane_recv.at[k],
                device_id={"chan_1": there // 16, "bl_0": there // 4 % 4, "bl_1": there % 4}, device_id_type=MESH_ID,
            )
            pl.when(me != there)(copy.start)

    for k in range(TAYLOR):
        spread(k)
        one_term(k)
        if k == 0:
            pl.semaphore_wait(barrier, 38)
            send_plane(TAYLOR)
        send_plane(k)

    for k in (TAYLOR, 0, 1, 2):
        total = own[k, pl.ds(pl.multiple_of(me * 8, 8), 8)] if k < TAYLOR else moment_own[...]
        together(plane_in.at[3, 1:32], plane_in.at[k, 1:32], plane_send.at[k], plane_recv.at[k]).wait()
        for j in range(1, 32):
            total = total + plane_in[k, j]
        for r in range(8):
            plane_sum[r, k:k + 1] = total[r:r + 1]

    for there in LINE_ORDER:
        copy = pltpu.make_async_remote_copy(
            src_ref=plane_sum.at[there], dst_ref=line_in.at[(deep - there) % 8], send_sem=line_send, recv_sem=line_recv,
            device_id={"bl_2": there % 4, "chan_0": there // 4}, device_id_type=MESH_ID,
        )
        pl.when(deep != there)(copy.start)
    total = plane_sum[deep]
    together(plane_sum.at[0:7], line_in.at[1:8], line_send, line_recv).wait()
    for j in range(1, 8):
        total = total + line_in[j]
    moments = [total[TAYLOR:TAYLOR + 1, m:m + 1] for m in range(MOMENTS)]
    images = [total[k:k + 1] for k in range(TAYLOR)]
    rows, determinant = solve_taylor(moments, images)
    for k in range(TAYLOR):
        out_ref[0, k:k + 1] = rows[k]
        out_ref[1, k:k + 1] = jnp.broadcast_to(determinant, (1, LANES))


def device_image(counts, offsets, vis, weight, kernel, tile, plane, chan):
    vmem = pl.BlockSpec(memory_space=pltpu.VMEM)
    dma = pltpu.SemaphoreType.DMA
    operands = (
        counts, vis, weight, kernel, tile, plane, chan,
        jnp.asarray(tap_table()), jnp.asarray(line_table()), jnp.asarray(twist_table()), jnp.asarray(screen_table()),
    )
    return pl.pallas_call(
        image_kernel,
        out_shape=jax.ShapeDtypeStruct((2, TAYLOR, LANES), f32),
        in_specs=[vmem] + [pl.BlockSpec(memory_space=pltpu.HBM)] * 11,
        out_specs=vmem,
        scratch_shapes=[pltpu.VMEM(a.shape, a.dtype) for a in operands] + [
            pltpu.VMEM((2 * ROWS, SLOTS), bf16),
            pltpu.VMEM((SLOTS, LANES), bf16),
            pltpu.VMEM((SLOTS, LANES), bf16),
            pltpu.VMEM((CELLS // CHUNK, SLOTS, CHUNK), bf16),
            pltpu.VMEM((ROWS, CELLS), f32),
            pltpu.VMEM((HALF_PLANES, 256, 256), f32),
            pltpu.VMEM((HALF_PLANES, 2, BLOCKS, STRIP, LANES), f32),
            pltpu.VMEM((BLOCKS, STRIP, LANES), f32),
            pltpu.VMEM((TAYLOR, 256, LANES), f32),
            pltpu.VMEM((TAYLOR + 1, 32, 8, LANES), f32),
            pltpu.VMEM((8, 4, LANES), f32),
            pltpu.VMEM((8, 4, LANES), f32),
            pltpu.VMEM((8, LANES), f32),
            dma((4,)), dma((4,)), dma, dma, dma((11,)),
        ],
        compiler_params=pltpu.CompilerParams(
            vmem_limit_bytes=55220 * 1024, collective_id=0, has_side_effects=True
        ),
        name="strip_image",
    )(offsets, *operands)


def solve_taylor(moments, images):
    entry_00, entry_01, entry_02 = (moments[0], moments[1], moments[2])
    entry_11, entry_12, entry_22 = (moments[2], moments[3], moments[4])
    minor_00 = entry_11 * entry_22 - entry_12 * entry_12
    minor_01 = entry_02 * entry_12 - entry_01 * entry_22
    minor_02 = entry_01 * entry_12 - entry_02 * entry_11
    minor_11 = entry_00 * entry_22 - entry_02 * entry_02
    minor_12 = entry_01 * entry_02 - entry_00 * entry_12
    minor_22 = entry_00 * entry_11 - entry_01 * entry_01
    determinant = entry_00 * minor_00 + entry_01 * minor_01 + entry_02 * minor_02
    first = minor_00 * images[0] + minor_01 * images[1] + minor_02 * images[2]
    second = minor_01 * images[0] + minor_11 * images[1] + minor_12 * images[2]
    third = minor_02 * images[0] + minor_12 * images[1] + minor_22 * images[2]
    return (first, second, third), determinant


MESH_ID = pl.DeviceIdType.MESH


def body(vis_value, vis_weight, kernel, tile_index, plane_index, chan_index, chan_offset, counts):
    scaled = device_image(
        counts, chan_offset, vis_value[0, 0], vis_weight[0], kernel[0, 0],
        tile_index[0], plane_index[0], chan_index[0],
    )
    return scaled[0] / scaled[1]


def solution(mesh):
    split = Mesh(mesh.devices.reshape(2, 2, 4, 4, 4), ("chan_0", "chan_1", "bl_0", "bl_1", "bl_2"))
    return jax.shard_map(
        body,
        mesh=split,
        in_specs=(
            P(CHAN, BL, None, None),
            P(CHAN, BL, None),
            P(CHAN, BL, None, None),
            P(CHAN, BL, None),
            P(CHAN, BL, None),
            P(CHAN, BL, None),
            P(CHAN, None),
            P(CHAN, BL),
        ),
        out_specs=P(None, CHAN_BL),
        check_vma=False,
    )
```

```python
import functools
import math

import jax
import jax.numpy as jnp
import numpy as np
from jax import lax
from jax.experimental import pallas as pl
from jax.experimental.pallas import tpu as pltpu
from jax.sharding import Mesh
from jax.sharding import PartitionSpec as P

NPIX = 4096
TILE = 8
TAYLOR = 3
MOMENTS = 5
STRIP = 8
SLOTS = 2048
HALF_PLANES = 4
WIDE = TILE + 1
ROWS = TAYLOR * WIDE * 2 * STRIP
SPAN = WIDE * 2 * STRIP
CELLS = HALF_PLANES * NPIX // TILE
BLOCKS = 32
LANES = 128
CHUNK = 256
CHAN_BL = ("chan_0", "chan_1", "bl_0", "bl_1", "bl_2")
CHAN = ("chan_0", "chan_1")
BL = ("bl_0", "bl_1", "bl_2")
f32 = jnp.float32
bf16 = jnp.bfloat16


def split_pair(table):
    high = table.astype(np.float32).astype(bf16)
    low = (table - high.astype(np.float64)).astype(np.float32).astype(bf16)
    return high, low


def tap_table():
    a = np.arange(TILE)[None, :]
    l = np.arange(STRIP)[:, None] - STRIP // 2
    angle = 2.0 * math.pi * ((a - NPIX // 2) * l % NPIX) / NPIX
    table = np.zeros((2, TILE, STRIP, TILE, TILE))
    for e in range(TILE):
        table[0, e, :, :, e] = np.cos(angle)
        table[1, e, :, :, e] = np.sin(angle)
    high, low = split_pair(table.reshape(2 * TILE * STRIP, TILE * TILE))
    ones = np.zeros((16, 2 * TILE * TILE), np.float32)
    ones[0, :TILE * TILE] = 1.0
    return np.concatenate([np.concatenate([high, low], axis=1), ones.astype(bf16)], axis=0)


def line_table():
    n = np.arange(LANES)
    angle = 2.0 * math.pi * (n[:, None] * n[None, :] % LANES) / LANES
    sign = 1.0 - 2.0 * (n % 2)
    c, s = np.cos(angle) * sign, np.sin(angle) * sign
    return np.concatenate(split_pair(np.block([[c, s], [-s, c]])), axis=0)


def twist_table():
    mq = np.arange(LANES)
    rows = [2.0 * math.pi * 8 * vb * mq / NPIX for vb in range(4)]
    for e in range(TILE):
        for mr in range(4):
            rows.append(2.0 * math.pi * e * (mq + LANES * mr) / NPIX + math.pi * e)
    angle = np.stack(rows)
    return np.concatenate([np.cos(angle), np.sin(angle)], axis=0).astype(np.float32)


def screen_table():
    cell = 0.5 / NPIX
    l = np.arange(STRIP)[None, :, None] - STRIP // 2
    m = (np.arange(BLOCKS)[:, None, None] - BLOCKS // 2) * LANES + np.arange(LANES)[None, None, :]
    radius = (l * cell) ** 2 + (m * cell) ** 2
    s = -radius / (1.0 + np.sqrt(1.0 - radius))
    angle = 2.0 * math.pi * 20.0 * s
    return np.stack([np.cos(angle), np.sin(angle)]).astype(np.float32)


def unit_circle(index):
    quarter = ((index + 64) >> 7) & 3
    x = (((index + 64) & 127) - 64).astype(f32) * (2.0 * math.pi / 512.0)
    x2 = x * x
    s = x * (1.0 + x2 * (-1.0 / 6 + x2 * (1.0 / 120 + x2 * (-1.0 / 5040 + x2 * (1.0 / 362880)))))
    c = 1.0 + x2 * (-0.5 + x2 * (1.0 / 24 + x2 * (-1.0 / 720 + x2 * (1.0 / 40320))))
    odd = (quarter & 1) == 1
    cos = jnp.where(odd, s, c)
    sin = jnp.where(odd, c, s)
    cos = jnp.where((quarter == 1) | (quarter == 2), -cos, cos)
    sin = jnp.where(quarter >= 2, -sin, sin)
    return cos, sin


def cmul(a, b):
    return a[0] * b[0] - a[1] * b[1], a[0] * b[1] + a[1] * b[0]


def cadd(a, b):
    return a[0] + b[0], a[1] + b[1]


def csub(a, b):
    return a[0] - b[0], a[1] - b[1]


def turn(a):
    return -a[1], a[0]


def four_point(x):
    a, b = cadd(x[0], x[2]), csub(x[0], x[2])
    c, d = cadd(x[1], x[3]), turn(csub(x[1], x[3]))
    return [cadd(a, c), cadd(b, d), csub(a, c), csub(b, d)]


def eight_point(x):
    even, odd = four_point(x[0::2]), four_point(x[1::2])
    r = math.sqrt(0.5)
    odd = [
        odd[0],
        ((odd[1][0] - odd[1][1]) * r, (odd[1][0] + odd[1][1]) * r),
        turn(odd[2]),
        ((-odd[3][0] - odd[3][1]) * r, (odd[3][0] - odd[3][1]) * r),
    ]
    return [cadd(e, o) for e, o in zip(even, odd)] + [csub(e, o) for e, o in zip(even, odd)]


def image_kernel(*refs):
    offset_ref = refs[0]
    (
        count_ref, vis_ref, weight_ref, kernel_ref, tile_ref, plane_ref, chan_ref,
        tap_ref, line_ref, twist_ref, screen_ref,
    ) = refs[13:24]
    fetches = [pltpu.make_async_copy(refs[1 + i], refs[13 + i], refs[-1].at[i]) for i in range(11)]
    for i in FETCH_ORDER:
        fetches[i].start()
    out_ref = refs[12]
    image_body(
        fetches, count_ref, offset_ref, vis_ref, weight_ref, kernel_ref, tile_ref, plane_ref, chan_ref,
        tap_ref, line_ref, twist_ref, screen_ref, out_ref, *refs[24:-1]
    )


START_X = (0.0, 0.8, 1.7, 1.8)
START_Z = (0, 1, 2, 3, 7, 4, 5, 6)
PLANE_ORDER = sorted(range(32), key=lambda t: START_X[t // 4 % 4] + START_X[t % 4] + 1.2 * (t // 16))
LINE_ORDER = tuple(z % 2 * 4 + z // 2 for z in START_Z)


def tree_sum(values):
    while len(values) > 1:
        values = [a + b for a, b in zip(values[0::2], values[1::2])]
    return values[0]


def plane_peer(me, j):
    there = (me + j) % 32
    return there, {"chan_1": there // 16, "bl_0": there // 4 % 4, "bl_1": there % 4}


FETCH_ORDER = (7, 3, 0, 1, 2, 4, 5, 6, 8, 9, 10)


def image_body(
    fetches, count_ref, offset_ref, vis_ref, weight_ref, kernel_ref, tile_ref, plane_ref, chan_ref,
    tap_ref, line_ref, twist_ref, screen_ref, out_ref, updates, bank_of, lane_hot, hot, grid, lines, screens, image,
    own, plane_in, plane_sum, line_in, moment_own, plane_send, plane_recv, line_send, line_recv,
):
    barrier = pltpu.get_barrier_semaphore()
    signal = functools.partial(pl.semaphore_signal, barrier, inc=1, device_id_type=MESH_ID)
    me = lax.axis_index("chan_1") * 16 + lax.axis_index("bl_0") * 4 + lax.axis_index("bl_1")
    for j in range(1, 32):
        signal(device_id=plane_peer(me, j)[1])
    deep = lax.axis_index("chan_0") * 4 + lax.axis_index("bl_2")
    for j in range(1, 8):
        there = (deep + j) % 8
        signal(device_id={"bl_2": there % 4, "chan_0": there // 4})

    for i in (7, 3):
        fetches[i].wait()
    for i in (0, 1, 2, 4, 5, 6):
        fetches[i].wait()
    count = jnp.broadcast_to(count_ref[0:1, 0:1], (1, CHUNK))
    offsets = [jnp.broadcast_to(offset_ref[0:1, c:c + 1], (1, CHUNK)) for c in range(16)]

    def one_chunk(step, sums):
        at = pl.ds(pl.multiple_of(step * CHUNK, CHUNK), CHUNK)
        chunk_kernel = kernel_ref[:, at]
        taps = jnp.dot(tap_ref[...], jnp.concatenate([chunk_kernel, chunk_kernel], axis=0), preferred_element_type=f32)
        slot = step * CHUNK + lax.broadcasted_iota(jnp.int32, (1, CHUNK), 1)
        weight = jnp.where(slot < count, weight_ref[:, at].astype(f32), 0.0)
        chan = chan_ref[:, at]
        coord = jnp.zeros((1, CHUNK), f32)
        for c in range(16):
            coord = jnp.where(chan == c, offsets[c], coord)
        tile = tile_ref[:, at]
        plane = plane_ref[:, at]
        direct = plane >= HALF_PLANES
        tile_v = tile & 511
        tile_v = jnp.where(direct, tile_v, 511 - tile_v)
        half = jnp.where(direct, plane - HALF_PLANES, HALF_PLANES - 1 - plane)
        across = lambda row: jnp.transpose(jnp.broadcast_to(row.astype(f32), (LANES, CHUNK)))
        bank_of[at, :] = across(half * 4 + (tile_v & 3)).astype(bf16)
        lane = lax.broadcasted_iota(jnp.int32, (CHUNK, LANES), 1).astype(f32)
        lane_hot[at, :] = jnp.where(across(tile_v >> 2) == lane, 1.0, 0.0).astype(bf16)
        weighted = weight * taps[128:129]
        new_sums = []
        power = weighted
        for m in range(MOMENTS):
            new_sums.append(sums[m] + power)
            power = power * coord
        vis = vis_ref[:, at].astype(f32)
        base = (weight * vis[0:1], weight * vis[1:2])
        row = lax.broadcasted_iota(jnp.int32, (STRIP, CHUNK), 0) - STRIP // 2
        phase = unit_circle(((tile >> 9) * row) & 511)
        turned = cmul(phase, base)
        mirror = jnp.where(direct, 1.0, -1.0)
        flipped = (turned[0] * mirror, turned[1] * mirror)
        direct_rows = jnp.broadcast_to(direct, (STRIP, CHUNK))
        coord_rows = jnp.broadcast_to(coord, (STRIP, CHUNK))
        parts = []
        for e in range(TILE):
            r = slice(e * STRIP, (e + 1) * STRIP)
            i = slice(64 + e * STRIP, 64 + (e + 1) * STRIP)
            tap_r, tap_i = taps[r], taps[i]
            parts.append(
                (turned[0] * tap_r - turned[1] * tap_i, flipped[0] * tap_i + flipped[1] * tap_r)
            )
        zero = jnp.zeros((STRIP, CHUNK), f32)
        for e in range(WIDE):
            there = parts[e] if e < TILE else (zero, zero)
            back = parts[TILE - e] if e > 0 else (zero, zero)
            both = jnp.concatenate(
                [jnp.where(direct_rows, there[0], back[0]), jnp.where(direct_rows, there[1], back[1])], axis=0
            )
            for k in range(TAYLOR):
                if k > 0:
                    both = both * jnp.concatenate([coord_rows, coord_rows], axis=0)
                high = both.astype(bf16)
                low = (both - high.astype(f32)).astype(bf16)
                first = 2 * k * SPAN + e * 16
                updates[first:first + 16, at] = high
                updates[first + SPAN:first + SPAN + 16, at] = low
        return tuple(new_sums)

    sums = lax.fori_loop(
        0, SLOTS // CHUNK, one_chunk, tuple(jnp.zeros((1, CHUNK), f32) for _ in range(MOMENTS)),
        unroll=True,
    )
    lane = lax.broadcasted_iota(jnp.int32, (STRIP, LANES), 1)
    moment_row = jnp.zeros((STRIP, LANES), f32)
    for m in range(MOMENTS):
        total = jnp.sum(sums[m], axis=1, keepdims=True)
        moment_row = jnp.where(lane == m, jnp.broadcast_to(total, (STRIP, LANES)), moment_row)
    moment_own[...] = moment_row

    def spread(k):
        for step in range(CELLS // CHUNK):
            if k == 0:
                banks = bank_of[...]
                halves = [
                    jnp.where(banks == jnp.asarray(step * 2 + half, bf16), lane_hot[...], jnp.zeros((), bf16))
                    for half in range(CHUNK // LANES)
                ]
                one_hot = jnp.concatenate(halves, axis=1)
                hot[step] = one_hot
            else:
                one_hot = hot[step]
            both = jnp.dot(updates[2 * SPAN * k:2 * SPAN * (k + 1)], one_hot, preferred_element_type=f32)
            grid[SPAN * k:SPAN * (k + 1), step * CHUNK:(step + 1) * CHUNK] = both[:SPAN] + both[SPAN:]

    for i in (8, 9, 10):
        fetches[i].wait()
    for b in range(BLOCKS):
        one = (screen_ref[0, b], screen_ref[1, b])
        two = cmul(one, one)
        for q in range(HALF_PLANES):
            screens[q, 0, b] = one[0]
            screens[q, 1, b] = one[1]
            if q < HALF_PLANES - 1:
                one = cmul(one, two)

    def piece(k, e, part, q, vb):
        first = ((k * WIDE + e) * 2 + part) * STRIP
        at = pl.ds(pl.multiple_of(q * 512 + vb * LANES, LANES), LANES)
        return grid[first:first + STRIP, at]

    def one_term(k):
        for q in range(HALF_PLANES):
            residues = []
            for vb in range(4):
                halves = []
                for part in range(2):
                    spill = piece(k, TILE, part, q, (vb - 1) % 4)
                    if vb == 0:
                        spill = pltpu.roll(spill, 1, 1)
                    column = [piece(k, 0, part, q, vb) + spill]
                    column += [piece(k, e, part, q, vb) for e in range(1, TILE)]
                    halves.append(jnp.concatenate(column, axis=0))
                residues.append(jnp.concatenate(halves, axis=1))
            whole = jnp.concatenate(residues, axis=0)
            high = whole.astype(bf16)
            low = (whole - high.astype(f32)).astype(bf16)
            lines[q] = (
                jnp.dot(high, line_ref[0:256], preferred_element_type=f32)
                + jnp.dot(low, line_ref[0:256], preferred_element_type=f32)
                + jnp.dot(high, line_ref[256:512], preferred_element_type=f32)
            )
        for q in range(HALF_PLANES):
            quarters = [[], [], [], []]
            for e in range(TILE):
                x = []
                for vb in range(4):
                    first = (vb * TILE + e) * STRIP
                    value = (lines[q, first:first + STRIP, 0:LANES], lines[q, first:first + STRIP, LANES:2 * LANES])
                    if vb > 0:
                        value = cmul(value, (twist_ref[vb:vb + 1], twist_ref[36 + vb:37 + vb]))
                    x.append(value)
                for mr, value in enumerate(four_point(x)):
                    if e > 0:
                        t = 4 + e * 4 + mr
                        value = cmul(value, (twist_ref[t:t + 1], twist_ref[36 + t:37 + t]))
                    quarters[mr].append(value)
            for mr in range(4):
                for mh, value in enumerate(eight_point(quarters[mr])):
                    b = 4 * mh + mr
                    add = value[0] * screens[q, 0, b] - value[1] * screens[q, 1, b]
                    if q < HALF_PLANES - 1:
                        image[b] = image[b] + add if q > 0 else add
                    else:
                        total = image[b] + add
                        first = b // 4 * 8 + b % 4
                        own[k, pl.ds(first, 4, stride=64), :] = total[0:4]
                        own[k, pl.ds(first + 4, 4, stride=64), :] = total[4:8]

    low_z = lax.axis_index("chan_0")
    core = lax.axis_index("chan_1")
    me = core * 16 + lax.axis_index("bl_0") * 4 + lax.axis_index("bl_1")
    deep = low_z * 4 + lax.axis_index("bl_2")

    def together(source, target, send, recv):
        return pltpu.make_async_remote_copy(
            src_ref=source, dst_ref=target, send_sem=send, recv_sem=recv,
            device_id={"chan_1": 1 - core}, device_id_type=MESH_ID,
        )

    def send_plane(k):
        for there in PLANE_ORDER:
            copy = pltpu.make_async_remote_copy(
                src_ref=own.at[k, there * 8:there * 8 + 8] if k < TAYLOR else moment_own,
                dst_ref=plane_in.at[k, (me - there) % 32], send_sem=plane_send.at[k], recv_sem=plane_recv.at[k],
                device_id={"chan_1": there // 16, "bl_0": there // 4 % 4, "bl_1": there % 4}, device_id_type=MESH_ID,
            )
            pl.when(me != there)(copy.start)

    for k in range(TAYLOR):
        spread(k)
        one_term(k)
        if k == 0:
            pl.semaphore_wait(barrier, 38)
            send_plane(TAYLOR)
        send_plane(k)

    for k in (TAYLOR, 0, 1, 2):
        total = own[k, pl.ds(pl.multiple_of(me * 8, 8), 8)] if k < TAYLOR else moment_own[...]
        together(plane_in.at[3, 1:32], plane_in.at[k, 1:32], plane_send.at[k], plane_recv.at[k]).wait()
        total = tree_sum([total] + [plane_in[k, j] for j in range(1, 32)])
        for r in range(8):
            plane_sum[r, k:k + 1] = total[r:r + 1]

    for there in LINE_ORDER:
        copy = pltpu.make_async_remote_copy(
            src_ref=plane_sum.at[there], dst_ref=line_in.at[(deep - there) % 8], send_sem=line_send, recv_sem=line_recv,
            device_id={"bl_2": there % 4, "chan_0": there // 4}, device_id_type=MESH_ID,
        )
        pl.when(deep != there)(copy.start)
    total = plane_sum[deep]
    together(plane_sum.at[0:7], line_in.at[1:8], line_send, line_recv).wait()
    total = tree_sum([total] + [line_in[j] for j in range(1, 8)])
    moments = [total[TAYLOR:TAYLOR + 1, m:m + 1] for m in range(MOMENTS)]
    images = [total[k:k + 1] for k in range(TAYLOR)]
    rows, determinant = solve_taylor(moments, images)
    for k in range(TAYLOR):
        out_ref[0, k:k + 1] = rows[k]
        out_ref[1, k:k + 1] = jnp.broadcast_to(determinant, (1, LANES))


def device_image(counts, offsets, vis, weight, kernel, tile, plane, chan):
    vmem = pl.BlockSpec(memory_space=pltpu.VMEM)
    dma = pltpu.SemaphoreType.DMA
    operands = (
        counts, vis, weight, kernel, tile, plane, chan,
        jnp.asarray(tap_table()), jnp.asarray(line_table()), jnp.asarray(twist_table()), jnp.asarray(screen_table()),
    )
    return pl.pallas_call(
        image_kernel,
        out_shape=jax.ShapeDtypeStruct((2, TAYLOR, LANES), f32),
        in_specs=[vmem] + [pl.BlockSpec(memory_space=pltpu.HBM)] * 11,
        out_specs=vmem,
        scratch_shapes=[pltpu.VMEM(a.shape, a.dtype) for a in operands] + [
            pltpu.VMEM((2 * ROWS, SLOTS), bf16),
            pltpu.VMEM((SLOTS, LANES), bf16),
            pltpu.VMEM((SLOTS, LANES), bf16),
            pltpu.VMEM((CELLS // CHUNK, SLOTS, CHUNK), bf16),
            pltpu.VMEM((ROWS, CELLS), f32),
            pltpu.VMEM((HALF_PLANES, 256, 256), f32),
            pltpu.VMEM((HALF_PLANES, 2, BLOCKS, STRIP, LANES), f32),
            pltpu.VMEM((BLOCKS, STRIP, LANES), f32),
            pltpu.VMEM((TAYLOR, 256, LANES), f32),
            pltpu.VMEM((TAYLOR + 1, 32, 8, LANES), f32),
            pltpu.VMEM((8, 4, LANES), f32),
            pltpu.VMEM((8, 4, LANES), f32),
            pltpu.VMEM((8, LANES), f32),
            dma((4,)), dma((4,)), dma, dma, dma((11,)),
        ],
        compiler_params=pltpu.CompilerParams(
            vmem_limit_bytes=55220 * 1024, collective_id=0, has_side_effects=True
        ),
        name="strip_image",
    )(offsets, *operands)


def solve_taylor(moments, images):
    entry_00, entry_01, entry_02 = (moments[0], moments[1], moments[2])
    entry_11, entry_12, entry_22 = (moments[2], moments[3], moments[4])
    minor_00 = entry_11 * entry_22 - entry_12 * entry_12
    minor_01 = entry_02 * entry_12 - entry_01 * entry_22
    minor_02 = entry_01 * entry_12 - entry_02 * entry_11
    minor_11 = entry_00 * entry_22 - entry_02 * entry_02
    minor_12 = entry_01 * entry_02 - entry_00 * entry_12
    minor_22 = entry_00 * entry_11 - entry_01 * entry_01
    determinant = entry_00 * minor_00 + entry_01 * minor_01 + entry_02 * minor_02
    first = minor_00 * images[0] + minor_01 * images[1] + minor_02 * images[2]
    second = minor_01 * images[0] + minor_11 * images[1] + minor_12 * images[2]
    third = minor_02 * images[0] + minor_12 * images[1] + minor_22 * images[2]
    return (first, second, third), determinant


MESH_ID = pl.DeviceIdType.MESH


def body(vis_value, vis_weight, kernel, tile_index, plane_index, chan_index, chan_offset, counts):
    scaled = device_image(
        counts, chan_offset, vis_value[0, 0], vis_weight[0], kernel[0, 0],
        tile_index[0], plane_index[0], chan_index[0],
    )
    return scaled[0] / scaled[1]


def solution(mesh):
    split = Mesh(mesh.devices.reshape(2, 2, 4, 4, 4), ("chan_0", "chan_1", "bl_0", "bl_1", "bl_2"))
    return jax.shard_map(
        body,
        mesh=split,
        in_specs=(
            P(CHAN, BL, None, None),
            P(CHAN, BL, None),
            P(CHAN, BL, None, None),
            P(CHAN, BL, None),
            P(CHAN, BL, None),
            P(CHAN, BL, None),
            P(CHAN, None),
            P(CHAN, BL),
        ),
        out_specs=P(None, CHAN_BL),
        check_vma=False,
    )
```
